32 devices in a mesh: fsdp: 2 (over y), ctx: 4 (over x, core), tp: 4 (over z).
Axes of the slice: x: 2, y: 2, z: 4, core: 2. Of those that a mesh axis runs over, the one named last changes fastest.
Arguments:
- inputs: bfloat16 [6, 1536, 1024], P('fsdp', ('ctx', 'tp')), may hold values from -6 to 6
- teacher: bfloat16 [6, 1536, 1024], P('fsdp', ('ctx', 'tp')), may hold values from -6 to 6
- clips_dev: int32 [2], replicated, may hold values from 1 to 3, as said below
- ffn1_gain: float32 [1024], replicated, may hold values from 0.5 to 1.5
- ffn1_shift: float32 [1024], replicated, may hold values from -0.625 to 0.625
- ffn1_in: bfloat16 [1024, 4096], P(('fsdp', 'ctx'), 'tp'), may hold values from -0.1875 to 0.1875
- ffn1_in_bias: float32 [4096], replicated, may hold values from -0.625 to 0.625
- ffn1_out: bfloat16 [1024, 4096], P(('fsdp', 'ctx'), 'tp'), may hold values from -0.1875 to 0.1875
- ffn1_out_bias: float32 [1024], replicated, may hold values from -0.625 to 0.625
- attn_gain: float32 [1024], replicated, may hold values from 0.5 to 1.5
- attn_shift: float32 [1024], replicated, may hold values from -0.625 to 0.625
- query_weight: bfloat16 [1024, 1024], P(('fsdp', 'ctx'), 'tp'), may hold values from -0.1875 to 0.1875
- query_bias: float32 [1024], replicated, may hold values from -0.625 to 0.625
- key_weight: bfloat16 [1024, 1024], P(('fsdp', 'ctx'), 'tp'), may hold values from -0.1875 to 0.1875
- value_weight: bfloat16 [1024, 1024], P(('fsdp', 'ctx'), 'tp'), may hold values from -0.1875 to 0.1875
- value_bias: float32 [1024], replicated, may hold values from -0.625 to 0.625
- attn_out_weight: bfloat16 [1024, 1024], P(('fsdp', 'ctx'), 'tp'), may hold values from -0.75 to 0.75
- attn_out_bias: float32 [1024], replicated, may hold values from -0.625 to 0.625
- rel_table: bfloat16 [73, 64], replicated, may hold values from -6 to 6
- conv_gain: float32 [1024], replicated, may hold values from 0.5 to 1.5
- conv_shift: float32 [1024], replicated, may hold values from -0.625 to 0.625
- conv_value_weight: bfloat16 [1024, 1024], P(('fsdp', 'ctx'), 'tp'), may hold values from -0.1875 to 0.1875
- conv_gate_weight: bfloat16 [1024, 1024], P(('fsdp', 'ctx'), 'tp'), may hold values from -0.1875 to 0.1875
- conv_depth: float32 [31, 1024], replicated, may hold values from -1 to 1
- conv_inner_gain: float32 [1024], replicated, may hold values from 0.5 to 1.5
- conv_inner_shift: float32 [1024], replicated, may hold values from -0.625 to 0.625
- conv_out_weight: bfloat16 [1024, 1024], P(('fsdp', 'ctx'), 'tp'), may hold values from -0.1875 to 0.1875
- ffn2_gain: float32 [1024], replicated, may hold values from 0.5 to 1.5
- ffn2_shift: float32 [1024], replicated, may hold values from -0.625 to 0.625
- ffn2_in: bfloat16 [1024, 4096], P(('fsdp', 'ctx'), 'tp'), may hold values from -0.1875 to 0.1875
- ffn2_in_bias: float32 [4096], replicated, may hold values from -0.625 to 0.625
- ffn2_out: bfloat16 [1024, 4096], P(('fsdp', 'ctx'), 'tp'), may hold values from -0.1875 to 0.1875
- ffn2_out_bias: float32 [1024], replicated, may hold values from -0.625 to 0.625
- final_gain: float32 [1024], replicated, may hold values from 0.5 to 1.5
- final_shift: float32 [1024], replicated, may hold values from -0.625 to 0.625
Outputs:
- layer_out: bfloat16 [6, 1536, 1024], P('fsdp', ('ctx', 'tp'))
- loss: float32 [], replicated
- input_grad: float32 [6, 1536, 1024], P('fsdp', ('ctx', 'tp'))
- grad_ffn1_gain: float32 [1024], replicated
- grad_ffn1_shift: float32 [1024], replicated
- grad_ffn1_in: float32 [1024, 4096], P(('fsdp', 'ctx'), 'tp')
- grad_ffn1_in_bias: float32 [4096], replicated
- grad_ffn1_out: float32 [1024, 4096], P(('fsdp', 'ctx'), 'tp')
- grad_ffn1_out_bias: float32 [1024], replicated
- grad_attn_gain: float32 [1024], replicated
- grad_attn_shift: float32 [1024], replicated
- grad_query_weight: float32 [1024, 1024], P(('fsdp', 'ctx'), 'tp')
- grad_query_bias: float32 [1024], replicated
- grad_key_weight: float32 [1024, 1024], P(('fsdp', 'ctx'), 'tp')
- grad_value_weight: float32 [1024, 1024], P(('fsdp', 'ctx'), 'tp')
- grad_value_bias: float32 [1024], replicated
- grad_attn_out_weight: float32 [1024, 1024], P(('fsdp', 'ctx'), 'tp')
- grad_attn_out_bias: float32 [1024], replicated
- grad_rel_table: float32 [73, 64], replicated
- grad_conv_gain: float32 [1024], replicated
- grad_conv_shift: float32 [1024], replicated
- grad_conv_value_weight: float32 [1024, 1024], P(('fsdp', 'ctx'), 'tp')
- grad_conv_gate_weight: float32 [1024, 1024], P(('fsdp', 'ctx'), 'tp')
- grad_conv_depth: float32 [31, 1024], replicated
- grad_conv_inner_gain: float32 [1024], replicated
- grad_conv_inner_shift: float32 [1024], replicated
- grad_conv_out_weight: float32 [1024, 1024], P(('fsdp', 'ctx'), 'tp')
- grad_ffn2_gain: float32 [1024], replicated
- grad_ffn2_shift: float32 [1024], replicated
- grad_ffn2_in: float32 [1024, 4096], P(('fsdp', 'ctx'), 'tp')
- grad_ffn2_in_bias: float32 [4096], replicated
- grad_ffn2_out: float32 [1024, 4096], P(('fsdp', 'ctx'), 'tp')
- grad_ffn2_out_bias: float32 [1024], replicated
- grad_final_gain: float32 [1024], replicated
- grad_final_shift: float32 [1024], replicated
The draws below stay inside these ranges and needn't reach their ends.
Inputs may be any that keep to these rules, and one draw needn't show every extreme that they name: clips_dev[f] counts the clips of fsdp index f, which fill its first slots; some index holds 3, some other index fewer.
All inputs are finite; a program needn't handle non-finite values.
Results may differ from the reference program's by a relative error of at most 0.028.
Values may be sent and summed in bfloat16 or wider, within the bound.
A program may use at most 384 MiB of HBM per device.

```python
import math
import jax
import jax.numpy as jnp
from jax import lax

D = 1024
HEADS = 16
FF = 4096
KERNEL = 31
LEFT = 64
RIGHT = 8
HEAD = 64
SEQ = 1536
CAP = 3
SLOTS = 6
N_FSDP = 2


def draw_clips_dev(key, part):
    key_counts, key_pick, key_other, key_low = jax.random.split(key, 4)
    counts = jax.random.randint(key_counts, (N_FSDP,), 1, CAP + 1)
    chosen = jax.random.randint(key_pick, (), 0, N_FSDP)
    other = (chosen + 1 + jax.random.randint(key_other, (), 0, N_FSDP - 1)) % N_FSDP
    fewer = jax.random.randint(key_low, (), 1, CAP)
    positions = jnp.arange(N_FSDP)
    counts = jnp.where(positions == other, fewer, counts)
    return jnp.where(positions == chosen, CAP, counts).astype(jnp.int32)


def block_scale(key, extent, cuts, smallest, top_value):
    def one(dim, blocks):
        steps = jax.random.uniform(jax.random.fold_in(jax.random.fold_in(key, 6), dim), (blocks,), jnp.float32, smallest / len(cuts), top_value / len(cuts))
        return jnp.repeat(jnp.exp(steps), extent[dim] // blocks).reshape((-1,) + (1,) * (len(extent) - dim - 1))

    level = one(*cuts[0])
    for cut in cuts[1:]:
        level = level * one(*cut)
    return level


def normal_values(own_key, shape, width, most, pieces=(), kind=jnp.bfloat16):
    values = width * jax.random.normal(own_key, shape, jnp.float32)
    if pieces:
        values = values * block_scale(own_key, shape, pieces, -0.22, 0.18)
    return jnp.clip(values, -most, most).astype(kind)


def setup_inputs(seed: int = 0) -> dict:
    key_list = jax.random.split(jax.random.key(seed), 36)
    return {
        "inputs": normal_values(key_list[0], (SLOTS, SEQ, D), 1.0, 6.0, ((0, 2), (1, 16))),
        "teacher": normal_values(key_list[1], (SLOTS, SEQ, D), 1.0, 6.0, ((0, 2), (1, 16))),
        "clips_dev": draw_clips_dev(jax.random.fold_in(key_list[35], 71), 0),
        "ffn1_gain": jnp.clip(1.0 + 0.1 * jax.random.normal(key_list[3], (D,), jnp.float32), 0.5, 1.5),
        "ffn1_shift": normal_values(key_list[4], (D,), 0.1, 0.625, (), jnp.float32),
        "ffn1_in": normal_values(key_list[5], (D, FF), D ** -0.5, 0.1875, ((0, 8), (1, 4))),
        "ffn1_in_bias": normal_values(key_list[6], (FF,), 0.1, 0.625, (), jnp.float32),
        "ffn1_out": normal_values(key_list[7], (D, FF), (FF // 4) ** -0.5, 0.1875, ((0, 8), (1, 4))),
        "ffn1_out_bias": normal_values(key_list[8], (D,), 0.1, 0.625, (), jnp.float32),
        "attn_gain": jnp.clip(1.0 + 0.1 * jax.random.normal(key_list[9], (D,), jnp.float32), 0.5, 1.5),
        "attn_shift": normal_values(key_list[10], (D,), 0.1, 0.625, (), jnp.float32),
        "query_weight": normal_values(key_list[11], (D, D), D ** -0.5, 0.1875, ((0, 8), (1, 4))),
        "query_bias": normal_values(key_list[12], (D,), 0.1, 0.625, (), jnp.float32),
        "key_weight": normal_values(key_list[13], (D, D), D ** -0.5, 0.1875, ((0, 8), (1, 4))),
        "value_weight": normal_values(key_list[14], (D, D), D ** -0.5, 0.1875, ((0, 8), (1, 4))),
        "value_bias": normal_values(key_list[15], (D,), 0.1, 0.625, (), jnp.float32),
        "attn_out_weight": normal_values(key_list[16], (D, D), (D // 16) ** -0.5, 0.75, ((0, 8), (1, 4))),
        "attn_out_bias": normal_values(key_list[17], (D,), 0.1, 0.625, (), jnp.float32),
        "rel_table": normal_values(key_list[18], (LEFT + RIGHT + 1, HEAD), 1.0, 6.0),
        "conv_gain": jnp.clip(1.0 + 0.1 * jax.random.normal(key_list[19], (D,), jnp.float32), 0.5, 1.5),
        "conv_shift": normal_values(key_list[20], (D,), 0.1, 0.625, (), jnp.float32),
        "conv_value_weight": normal_values(key_list[21], (D, D), D ** -0.5, 0.1875, ((0, 8), (1, 4))),
        "conv_gate_weight": normal_values(key_list[22], (D, D), D ** -0.5, 0.1875, ((0, 8), (1, 4))),
        "conv_depth": normal_values(key_list[23], (KERNEL, D), KERNEL ** -0.5, 1.0, (), jnp.float32),
        "conv_inner_gain": jnp.clip(1.0 + 0.1 * jax.random.normal(key_list[24], (D,), jnp.float32), 0.5, 1.5),
        "conv_inner_shift": normal_values(key_list[25], (D,), 0.1, 0.625, (), jnp.float32),
        "conv_out_weight": normal_values(key_list[26], (D, D), D ** -0.5, 0.1875, ((0, 8), (1, 4))),
        "ffn2_gain": jnp.clip(1.0 + 0.1 * jax.random.normal(key_list[27], (D,), jnp.float32), 0.5, 1.5),
        "ffn2_shift": normal_values(key_list[28], (D,), 0.1, 0.625, (), jnp.float32),
        "ffn2_in": normal_values(key_list[29], (D, FF), D ** -0.5, 0.1875, ((0, 8), (1, 4))),
        "ffn2_in_bias": normal_values(key_list[30], (FF,), 0.1, 0.625, (), jnp.float32),
        "ffn2_out": normal_values(key_list[31], (D, FF), (FF // 4) ** -0.5, 0.1875, ((0, 8), (1, 4))),
        "ffn2_out_bias": normal_values(key_list[32], (D,), 0.1, 0.625, (), jnp.float32),
        "final_gain": jnp.clip(1.0 + 0.1 * jax.random.normal(key_list[33], (D,), jnp.float32), 0.5, 1.5),
        "final_shift": normal_values(key_list[34], (D,), 0.1, 0.625, (), jnp.float32),
    }


@jax.custom_vjp
def low(v):
    return lax.optimization_barrier(v.astype(jnp.bfloat16)).astype(jnp.float32)

@jax.custom_vjp
def low_back(v):
    return v

def low_keep(v):
    return (low(v), None)

def low_pass(kept, grad):
    return (grad,)

def back_keep(v):
    return (v, None)

def back_low(kept, grad):
    return (low(grad),)
low.defvjp(low_keep, low_pass)
low_back.defvjp(back_keep, back_low)
epsilon = 1e-05
highest_precision = lax.Precision.HIGHEST

def layer_norm(stream, norm_gain, norm_shift):
    centred = stream - lax.optimization_barrier(jnp.mean(stream, axis=-1, keepdims=True))
    spread = lax.optimization_barrier(jnp.mean(centred * centred, axis=-1, keepdims=True))
    return centred * lax.rsqrt(spread + epsilon) * norm_gain + norm_shift

def project_in(left_reach, right_reach):
    return jnp.einsum('zub,bx->zux', left_reach, right_reach, precision=highest_precision)

def project_out(left_reach, right_reach):
    return jnp.einsum('anp,op->ano', left_reach, right_reach, precision=highest_precision)

def feed_forward(stream, norm_gain, norm_shift, weight_in, bias_in, weight_out, bias_out):
    normed = low(layer_norm(stream, norm_gain, norm_shift))
    hidden_pre = low_back(project_in(normed, weight_in) + bias_in)
    active = low(jax.nn.silu(hidden_pre))
    branch = low_back(project_out(active, weight_out) + bias_out)
    return stream + 0.5 * branch

def attend_clip(operands, rel_table):
    query_heads, key_heads, value_heads = operands
    positions = jnp.arange(SEQ, dtype=jnp.int32)
    offsets = jnp.clip(positions[None, :] - positions[:, None], -LEFT, RIGHT) + LEFT
    rel_scores = jnp.einsum('lhe,re->hlr', query_heads, rel_table, precision=highest_precision)
    index_map = jnp.broadcast_to(offsets[None, :, :], (HEADS, SEQ, SEQ))
    bias_entries = jnp.take_along_axis(rel_scores, index_map, axis=2)
    dots = jnp.einsum('lhe,mhe->hlm', query_heads, key_heads, precision=highest_precision)
    scores = low_back((dots + bias_entries) * (1.0 / math.sqrt(HEAD)))
    attn_probs = jnp.exp(scores - jax.nn.logsumexp(scores, axis=-1, keepdims=True))
    return jnp.einsum('hlm,mhe->lhe', low(attn_probs), value_heads, precision=highest_precision)

def attention(stream, norm_gain, norm_shift, query_weight, query_bias, key_weight, value_weight, value_bias, out_weight, out_bias, rel_table):
    normed = low(layer_norm(stream, norm_gain, norm_shift))
    queries = low(low_back(project_in(normed, query_weight) + query_bias))
    keys_all = low(low_back(project_in(normed, key_weight)))
    values_all = low(low_back(project_in(normed, value_weight) + value_bias))
    head_shape = (SLOTS, SEQ, HEADS, HEAD)

    def one_clip(operands):
        return attend_clip(operands, rel_table)
    mixed_heads = lax.map(jax.checkpoint(one_clip), (queries.reshape(head_shape), keys_all.reshape(head_shape), values_all.reshape(head_shape)))
    mixed_token_rows = low(low_back(mixed_heads.reshape(SLOTS, SEQ, D)))
    branch = low_back(project_out(mixed_token_rows, out_weight) + out_bias)
    return stream + branch

def conv_module(stream, norm_gain, norm_shift, value_weight, gate_weight, depth_kernel, inner_gain, inner_offset, out_weight):
    normed = low(layer_norm(stream, norm_gain, norm_shift))
    part_value = low_back(project_in(normed, value_weight))
    part_gate = low_back(project_in(normed, gate_weight))
    gated_rows = low(part_value * jax.nn.sigmoid(part_gate))
    padded = jnp.pad(gated_rows, ((0, 0), (KERNEL - 1, 0), (0, 0)))
    convolved = depth_kernel[0] * padded[:, 0:SEQ, :]
    for tap_index in range(1, KERNEL):
        convolved = convolved + depth_kernel[tap_index] * padded[:, tap_index:tap_index + SEQ, :]
    active = low(jax.nn.silu(layer_norm(convolved, inner_gain, inner_offset)))
    branch = low_back(project_out(active, out_weight))
    return stream + branch

def layer_forward(stream, weights):
    ffn1_gain, ffn1_shift, ffn1_in, ffn1_in_bias, ffn1_out, ffn1_out_bias, attn_gain, attn_shift, query_weight, query_bias, key_weight, value_weight, value_bias, attn_out_weight, attn_out_bias, rel_table, conv_gain, conv_shift, conv_value_weight, conv_gate_weight, conv_depth, conv_inner_gain, conv_inner_shift, conv_out_weight, ffn2_gain, ffn2_shift, ffn2_in, ffn2_in_bias, ffn2_out, ffn2_out_bias, final_gain, final_shift = weights
    after_ffn1 = feed_forward(stream, ffn1_gain, ffn1_shift, ffn1_in, ffn1_in_bias, ffn1_out, ffn1_out_bias)
    after_attn = attention(after_ffn1, attn_gain, attn_shift, query_weight, query_bias, key_weight, value_weight, value_bias, attn_out_weight, attn_out_bias, rel_table)
    after_conv = conv_module(after_attn, conv_gain, conv_shift, conv_value_weight, conv_gate_weight, conv_depth, conv_inner_gain, conv_inner_shift, conv_out_weight)
    after_ffn2 = feed_forward(after_conv, ffn2_gain, ffn2_shift, ffn2_in, ffn2_in_bias, ffn2_out, ffn2_out_bias)
    return layer_norm(after_ffn2, final_gain, final_shift)

def reference(inputs, teacher, clips_dev, ffn1_gain, ffn1_shift, ffn1_in, ffn1_in_bias, ffn1_out, ffn1_out_bias, attn_gain, attn_shift, query_weight, query_bias, key_weight, value_weight, value_bias, attn_out_weight, attn_out_bias, rel_table, conv_gain, conv_shift, conv_value_weight, conv_gate_weight, conv_depth, conv_inner_gain, conv_inner_shift, conv_out_weight, ffn2_gain, ffn2_shift, ffn2_in, ffn2_in_bias, ffn2_out, ffn2_out_bias, final_gain, final_shift):
    params = (ffn1_gain, ffn1_shift, ffn1_in, ffn1_in_bias, ffn1_out, ffn1_out_bias, attn_gain, attn_shift, query_weight, query_bias, key_weight, value_weight, value_bias, attn_out_weight, attn_out_bias, rel_table, conv_gain, conv_shift, conv_value_weight, conv_gate_weight, conv_depth, conv_inner_gain, conv_inner_shift, conv_out_weight, ffn2_gain, ffn2_shift, ffn2_in, ffn2_in_bias, ffn2_out, ffn2_out_bias, final_gain, final_shift)
    floats = tuple((member.astype(jnp.float32) for member in params))
    live_slots = (jnp.arange(CAP, dtype=jnp.int32)[None, :] < clips_dev[:, None]).reshape(SLOTS).astype(jnp.float32)
    target = teacher.astype(jnp.float32)

    def objective(stream, *weights):
        final_out = layer_forward(stream, weights)
        misfit = (final_out - target) * live_slots[:, None, None]
        return (jnp.sum(misfit * misfit), final_out)
    sse_total, pullback, final_out = jax.vjp(objective, inputs.astype(jnp.float32), *floats, has_aux=True)
    grads = pullback(jnp.ones_like(sse_total))
    token_count = (jnp.sum(clips_dev) * SEQ).astype(jnp.float32)
    loss = sse_total / token_count
    return (final_out.astype(jnp.bfloat16), loss, grads[0], grads[1], grads[2], grads[3], grads[4], grads[5], grads[6], grads[7], grads[8], grads[9], grads[10], grads[11], grads[12], grads[13], grads[14], grads[15], grads[16], grads[17], grads[18], grads[19], grads[20], grads[21], grads[22], grads[23], grads[24], grads[25], grads[26], grads[27], grads[28], grads[29], grads[30], grads[31], grads[32])
```

```python
import math

import jax
import jax.numpy as jnp
from jax import lax
from jax.sharding import PartitionSpec as P

D = 1024
LEFT = 64
HEAD = 64
SEQ = 1536


epsilon = 1e-05


def from_behind(shard, axis, by):
    devices = lax.axis_size(axis)
    pairs = [(i, i + by) for i in range(devices) if 0 <= i + by < devices]
    return lax.ppermute(shard, axis, pairs)


def norm_forward(stream, norm_gain, norm_shift):
    centred = stream - jnp.mean(stream, axis=-1, keepdims=True)
    inverse = lax.rsqrt(jnp.mean(centred * centred, axis=-1, keepdims=True) + epsilon)
    standard = centred * inverse
    return (standard * norm_gain + norm_shift, standard, inverse)


def norm_backward(grad_out, standard, inverse, norm_gain):
    grad_standard = grad_out * norm_gain
    mean_first = jnp.mean(grad_standard, axis=-1, keepdims=True)
    mean_second = jnp.mean(grad_standard * standard, axis=-1, keepdims=True)
    grad_in = inverse * (grad_standard - mean_first - standard * mean_second)
    return (grad_in, jnp.sum(grad_out * standard, axis=(0, 1)), jnp.sum(grad_out, axis=(0, 1)))


def silu_slope(hidden_pre):
    gate_sig = jax.nn.sigmoid(hidden_pre)
    return gate_sig * (1.0 + hidden_pre * (1.0 - gate_sig))


def rows_in(left_reach, right_reach):
    return jnp.einsum("zub,bx->zux", left_reach, right_reach, preferred_element_type=jnp.float32)


def rows_out(left_reach, right_reach):
    return jnp.einsum("anp,op->ano", left_reach, right_reach, preferred_element_type=jnp.float32)


def weight_sum(left_reach, right_reach):
    return jnp.einsum("zbt,zbm->tm", left_reach, right_reach, preferred_element_type=jnp.float32)


def widen(normed):
    return lax.all_gather(normed.astype(jnp.bfloat16), "tp", axis=1, tiled=True)


def narrow(partial_rows):
    return lax.psum_scatter(
        partial_rows.astype(jnp.bfloat16), "tp", scatter_dimension=1, tiled=True
    ).astype(jnp.float32)


def widen_grad(grad_branch):
    return lax.all_gather(grad_branch, "tp", axis=1, tiled=True)


def narrow_grad(partial_rows):
    return lax.psum_scatter(
        partial_rows.astype(jnp.bfloat16), "tp", scatter_dimension=1, tiled=True
    ).astype(jnp.float32)


def local_cut(full_array, tp_rank, size_local):
    return lax.dynamic_slice_in_dim(
        full_array, tp_rank * size_local, size_local, full_array.ndim - 1
    )


def local_put(local_array, tp_rank, full_size):
    shape_full = local_array.shape[:-1] + (full_size,)
    return lax.dynamic_update_slice_in_dim(
        jnp.zeros(shape_full, jnp.float32),
        local_array,
        tp_rank * local_array.shape[-1],
        local_array.ndim - 1,
    )


def band_bias(rel_scores, query_start, key_count):
    lead = rel_scores.shape[:3]
    row_count = lead[2]
    extent = key_count + row_count
    left_edge = jnp.broadcast_to(rel_scores[..., :1], lead + (key_count,))
    right_edge = jnp.broadcast_to(rel_scores[..., -1:], lead + (key_count + row_count,))
    extended = jnp.concatenate([left_edge, rel_scores, right_edge], axis=3)
    start = key_count + LEFT - (row_count - 1) - query_start
    skewed = lax.dynamic_slice_in_dim(extended, start, extent, 3)
    flat = skewed.reshape(lead[:2] + (row_count * extent,))
    sheared = flat[..., row_count - 1 : row_count - 1 + row_count * (extent - 1)]
    return sheared.reshape(lead[:2] + (row_count, extent - 1))[..., :key_count]


def attention_logits(query_heads, key_heads, rel_table, query_start):
    rel_scores = jnp.einsum(
        "slhe,re->shlr", query_heads, rel_table, preferred_element_type=jnp.float32
    )
    bias_entries = band_bias(rel_scores, query_start, key_heads.shape[1])
    dots = jnp.einsum("slhe,smhe->shlm", query_heads, key_heads, preferred_element_type=jnp.float32)
    return ((dots + bias_entries) * (1.0 / math.sqrt(HEAD)), rel_scores)


def ffn_forward(stream, norm_gain, norm_shift, weight_in, bias_in, weight_out, bias_out):
    normed, standard, inverse = norm_forward(stream, norm_gain, norm_shift)
    wide_rows = widen(normed)
    hidden_pre = rows_in(wide_rows, weight_in) + bias_in
    active = jax.nn.silu(hidden_pre).astype(jnp.bfloat16)
    branch = narrow(rows_out(active, weight_out)) + bias_out
    return (stream + 0.5 * branch, (standard, inverse, wide_rows, hidden_pre))


def ffn_backward(grad_stream, saved, norm_gain, weight_in, weight_out):
    standard, inverse, wide_rows, hidden_pre = saved
    grad_branch = (0.5 * grad_stream).astype(jnp.bfloat16)
    out_bias_grad = jnp.sum(grad_branch.astype(jnp.float32), axis=(0, 1))
    wide_grad = widen_grad(grad_branch)
    active = jax.nn.silu(hidden_pre).astype(jnp.bfloat16)
    out_grad = weight_sum(wide_grad, active)
    grad_pre = (rows_in(wide_grad, weight_out) * silu_slope(hidden_pre)).astype(jnp.bfloat16)
    in_bias_grad = jnp.sum(grad_pre.astype(jnp.float32), axis=(0, 1))
    in_grad = weight_sum(wide_rows, grad_pre)
    grad_normed = narrow_grad(rows_out(grad_pre, weight_in))
    grad_in, gain_grad, shift_grad = norm_backward(grad_normed, standard, inverse, norm_gain)
    return (
        grad_stream + grad_in,
        (gain_grad, shift_grad, in_grad, in_bias_grad, out_grad, out_bias_grad),
    )


def attn_forward(stream, norm_gain, norm_shift, weights, biases, rel_table, ctx_rank):
    query_w, key_w, value_w, out_w = weights
    query_b, value_b, out_b = biases
    normed, standard, inverse = norm_forward(stream, norm_gain, norm_shift)
    wide_rows = widen(normed)
    queries = (rows_in(wide_rows, query_w) + query_b).astype(jnp.bfloat16)
    keys_local = rows_in(wide_rows, key_w).astype(jnp.bfloat16)
    values_local = (rows_in(wide_rows, value_w) + value_b).astype(jnp.bfloat16)
    keys_all, values_all = (
        lax.all_gather(keys_local, "ctx", axis=1, tiled=True),
        lax.all_gather(values_local, "ctx", axis=1, tiled=True),
    )
    slot_count, row_count, width_local = queries.shape
    key_count = keys_all.shape[1]
    head_count = width_local // HEAD
    query_heads = queries.reshape(slot_count, row_count, head_count, HEAD)
    key_heads = keys_all.reshape(slot_count, key_count, head_count, HEAD)
    value_heads = values_all.reshape(slot_count, key_count, head_count, HEAD)
    scores, rel_scores = attention_logits(query_heads, key_heads, rel_table, ctx_rank * row_count)
    row_max = jnp.max(scores, axis=-1, keepdims=True)
    log_total = row_max + jnp.log(jnp.sum(jnp.exp(scores - row_max), axis=-1, keepdims=True))
    attn_probs = jnp.exp(scores - log_total).astype(jnp.bfloat16)
    mixed_heads = jnp.einsum(
        "shlm,smhe->slhe", attn_probs, value_heads, preferred_element_type=jnp.float32
    )
    mixed_token_rows = mixed_heads.astype(jnp.bfloat16).reshape(slot_count, row_count, width_local)
    branch = narrow(rows_out(mixed_token_rows, out_w)) + out_b
    return (
        stream + branch,
        (standard, inverse, wide_rows, queries, keys_all, values_all, mixed_token_rows, log_total),
    )


def attn_backward(grad_stream, saved, norm_gain, weights, rel_table, ctx_rank):
    query_w, key_w, value_w, out_w = weights
    standard, inverse, wide_rows, queries, keys_all, values_all, mixed_token_rows, log_total = saved
    grad_branch = grad_stream.astype(jnp.bfloat16)
    out_bias_grad = jnp.sum(grad_branch.astype(jnp.float32), axis=(0, 1))
    wide_grad = widen_grad(grad_branch)
    out_grad = weight_sum(wide_grad, mixed_token_rows)
    grad_mixed = rows_in(wide_grad, out_w).astype(jnp.bfloat16)
    slot_count, row_count, width_local = queries.shape
    key_count = keys_all.shape[1]
    head_count = width_local // HEAD
    query_heads = queries.reshape(slot_count, row_count, head_count, HEAD)
    key_heads = keys_all.reshape(slot_count, key_count, head_count, HEAD)
    value_heads = values_all.reshape(slot_count, key_count, head_count, HEAD)
    grad_heads = grad_mixed.reshape(slot_count, row_count, head_count, HEAD)
    query_start = ctx_rank * row_count
    rel_scores = jnp.einsum(
        "slhe,re->shlr", query_heads, rel_table, preferred_element_type=jnp.float32
    )
    bias_entries, pick_back = jax.vjp(
        lambda table_scores: band_bias(table_scores, query_start, key_count), rel_scores
    )
    dots = jnp.einsum("slhe,smhe->shlm", query_heads, key_heads, preferred_element_type=jnp.float32)
    scale_factor = 1.0 / math.sqrt(HEAD)
    scores = (dots + bias_entries) * scale_factor
    attn_probs = jnp.exp(scores - log_total)
    grad_probs = jnp.einsum(
        "slhe,smhe->shlm", grad_heads, value_heads, preferred_element_type=jnp.float32
    )
    row_dot = jnp.sum(attn_probs * grad_probs, axis=-1, keepdims=True)
    grad_scores = (attn_probs * (grad_probs - row_dot)).astype(jnp.bfloat16)
    value_terms = jnp.einsum(
        "shlm,slhe->smhe",
        attn_probs.astype(jnp.bfloat16),
        grad_heads,
        preferred_element_type=jnp.float32,
    )
    key_terms = (
        jnp.einsum("shlm,slhe->smhe", grad_scores, query_heads, preferred_element_type=jnp.float32)
        * scale_factor
    )
    key_grad, value_grad = (
        lax.psum_scatter(
            key_terms.reshape(slot_count, key_count, width_local).astype(jnp.bfloat16),
            "ctx",
            scatter_dimension=1,
            tiled=True,
        ).astype(jnp.float32),
        lax.psum_scatter(
            value_terms.reshape(slot_count, key_count, width_local).astype(jnp.bfloat16),
            "ctx",
            scatter_dimension=1,
            tiled=True,
        ).astype(jnp.float32),
    )
    rel_grad = pick_back(grad_scores.astype(jnp.float32) * scale_factor)[0]
    query_grad = (
        jnp.einsum("shlm,smhe->slhe", grad_scores, key_heads, preferred_element_type=jnp.float32)
        * scale_factor
    )
    query_grad = query_grad + jnp.einsum(
        "shlr,re->slhe", rel_grad, rel_table.astype(jnp.float32), precision=lax.Precision.HIGHEST
    )
    table_grad = jnp.einsum(
        "shlr,slhe->re", rel_grad, query_heads.astype(jnp.float32), precision=lax.Precision.HIGHEST
    )
    query_low = query_grad.reshape(slot_count, row_count, width_local).astype(jnp.bfloat16)
    key_low = key_grad.astype(jnp.bfloat16)
    value_low = value_grad.astype(jnp.bfloat16)
    query_bias_grad = jnp.sum(query_low.astype(jnp.float32), axis=(0, 1))
    value_bias_grad = jnp.sum(value_low.astype(jnp.float32), axis=(0, 1))
    query_w_grad = weight_sum(wide_rows, query_low)
    key_w_grad = weight_sum(wide_rows, key_low)
    value_w_grad = weight_sum(wide_rows, value_low)
    grad_normed = narrow_grad(
        rows_out(query_low, query_w) + rows_out(key_low, key_w) + rows_out(value_low, value_w)
    )
    grad_in, gain_grad, shift_grad = norm_backward(grad_normed, standard, inverse, norm_gain)
    return (
        grad_stream + grad_in,
        (
            gain_grad,
            shift_grad,
            query_w_grad,
            query_bias_grad,
            key_w_grad,
            value_w_grad,
            value_bias_grad,
            out_grad,
            out_bias_grad,
            table_grad,
        ),
    )


def conv_forward(stream, norm_gain, norm_shift, weights, depth_local, inner_gain, inner_offset):
    value_w, gate_w, out_w = weights
    normed, standard, inverse = norm_forward(stream, norm_gain, norm_shift)
    wide_rows = widen(normed)
    part_value = rows_in(wide_rows, value_w)
    part_gate = rows_in(wide_rows, gate_w)
    gated_rows = (part_value * jax.nn.sigmoid(part_gate)).astype(jnp.bfloat16)
    row_count = gated_rows.shape[1]
    reach_rows = depth_local.shape[0] - 1
    halo_rows = from_behind(gated_rows[:, row_count - reach_rows :, :], "ctx", 1)
    padded = jnp.concatenate([halo_rows, gated_rows], axis=1)
    padded_float = padded.astype(jnp.float32)
    convolved = depth_local[0] * padded_float[:, 0:row_count, :]
    for tap_index in range(1, depth_local.shape[0]):
        convolved = (
            convolved
            + depth_local[tap_index] * padded_float[:, tap_index : tap_index + row_count, :]
        )
    row_sums = lax.psum(
        (jnp.sum(convolved, axis=-1), jnp.sum(convolved * convolved, axis=-1)), "tp"
    )
    row_mean = (row_sums[0] / D)[..., None]
    row_var = (row_sums[1] / D)[..., None] - row_mean * row_mean
    inner_inverse = lax.rsqrt(row_var + epsilon)
    inner_standard = (convolved - row_mean) * inner_inverse
    inner_pre = inner_standard * inner_gain + inner_offset
    active = jax.nn.silu(inner_pre).astype(jnp.bfloat16)
    branch = narrow(rows_out(active, out_w))
    return (
        stream + branch,
        (
            standard,
            inverse,
            wide_rows,
            part_value,
            part_gate,
            padded,
            inner_standard,
            inner_inverse,
            inner_pre,
        ),
    )


def conv_backward(grad_stream, saved, norm_gain, weights, depth_local, inner_gain):
    value_w, gate_w, out_w = weights
    (
        standard,
        inverse,
        wide_rows,
        part_value,
        part_gate,
        padded,
        inner_standard,
        inner_inverse,
        inner_pre,
    ) = saved
    grad_branch = grad_stream.astype(jnp.bfloat16)
    wide_grad = widen_grad(grad_branch)
    active = jax.nn.silu(inner_pre).astype(jnp.bfloat16)
    out_grad = weight_sum(wide_grad, active)
    grad_inner = rows_in(wide_grad, out_w) * silu_slope(inner_pre)
    inner_gain_grad = jnp.sum(grad_inner * inner_standard, axis=(0, 1))
    inner_shift_grad = jnp.sum(grad_inner, axis=(0, 1))
    grad_standard = grad_inner * inner_gain
    row_sums = lax.psum(
        (jnp.sum(grad_standard, axis=-1), jnp.sum(grad_standard * inner_standard, axis=-1)), "tp"
    )
    grad_conv = inner_inverse * (
        grad_standard - (row_sums[0] / D)[..., None] - inner_standard * (row_sums[1] / D)[..., None]
    )
    row_count = grad_conv.shape[1]
    tap_count = depth_local.shape[0]
    reach_rows = tap_count - 1
    padded_float = padded.astype(jnp.float32)
    depth_grad = jnp.stack(
        [
            jnp.sum(grad_conv * padded_float[:, tap_index : tap_index + row_count, :], axis=(0, 1))
            for tap_index in range(tap_count)
        ]
    )
    grad_padded = jnp.zeros(padded.shape, jnp.float32)
    for tap_index in range(tap_count):
        grad_padded = grad_padded.at[:, tap_index : tap_index + row_count, :].add(
            depth_local[tap_index] * grad_conv
        )
    back_halo = from_behind(grad_padded[:, :reach_rows, :].astype(jnp.bfloat16), "ctx", -1).astype(
        jnp.float32
    )
    grad_gated = grad_padded[:, reach_rows:, :] + jnp.pad(
        back_halo, ((0, 0), (row_count - reach_rows, 0), (0, 0))
    )
    gate_sig = jax.nn.sigmoid(part_gate)
    grad_value = (grad_gated * gate_sig).astype(jnp.bfloat16)
    grad_gate = (grad_gated * part_value * gate_sig * (1.0 - gate_sig)).astype(jnp.bfloat16)
    value_w_grad = weight_sum(wide_rows, grad_value)
    gate_w_grad = weight_sum(wide_rows, grad_gate)
    grad_normed = narrow_grad(rows_out(grad_value, value_w) + rows_out(grad_gate, gate_w))
    grad_in, gain_grad, shift_grad = norm_backward(grad_normed, standard, inverse, norm_gain)
    return (
        grad_stream + grad_in,
        (
            gain_grad,
            shift_grad,
            value_w_grad,
            gate_w_grad,
            depth_grad,
            inner_gain_grad,
            inner_shift_grad,
            out_grad,
        ),
    )


def gather_rows(shard):
    return lax.all_gather(shard, ("fsdp", "ctx"), axis=0, tiled=True)


def scatter_sum(*grads):
    joined = jnp.concatenate([grad.astype(jnp.bfloat16) for grad in grads], axis=1)
    part = lax.psum_scatter(joined, ("fsdp", "ctx"), scatter_dimension=0, tiled=True)
    pieces = []
    start = 0
    for grad in grads:
        pieces.append(part[:, start : start + grad.shape[1]].astype(jnp.float32))
        start += grad.shape[1]
    return tuple(pieces)


def sum_small(whole_parts, split_parts, tp_rank):
    tp_count = lax.axis_size("tp")
    split = jnp.concatenate([part.reshape(-1) for part in split_parts])
    spread = lax.dynamic_update_slice(
        jnp.zeros((tp_count, split.shape[0]), jnp.float32), split[None], (tp_rank, 0)
    )
    flat = jnp.concatenate([part.reshape(-1) for part in whole_parts] + [spread.reshape(-1)])
    count = flat.shape[0]
    flat = jnp.pad(flat, (0, -count % 1024)).reshape(-1, 128)
    total = lax.psum(flat, ("fsdp", "ctx", "tp")).reshape(-1)
    whole = []
    start = 0
    for part in whole_parts:
        whole.append(total[start : start + part.size].reshape(part.shape))
        start += part.size
    spread = total[start : start + tp_count * split.shape[0]].reshape(tp_count, -1)
    pieces = []
    start = 0
    for part in split_parts:
        piece = spread[:, start : start + part.size]
        if part.ndim == 1:
            pieces.append(piece.reshape(-1))
        else:
            piece = piece.reshape((tp_count,) + part.shape)
            pieces.append(piece.transpose(1, 0, 2).reshape(part.shape[0], -1))
        start += part.size
    w, p = whole, pieces
    return (
        w[0], w[1], p[0], w[2], w[3], w[4], p[1], p[2], w[5], w[6], w[7], w[8],
        p[3], p[4], p[5], w[9], w[10], p[6], w[11], w[12], w[13], w[14],
    )


def body(
    inputs,
    teacher,
    clips_dev,
    ffn1_gain,
    ffn1_shift,
    ffn1_in,
    ffn1_in_bias,
    ffn1_out,
    ffn1_out_bias,
    attn_gain,
    attn_shift,
    query_weight,
    query_bias,
    key_weight,
    value_weight,
    value_bias,
    attn_out_weight,
    attn_out_bias,
    rel_table,
    conv_gain,
    conv_shift,
    conv_value_weight,
    conv_gate_weight,
    conv_depth,
    conv_inner_gain,
    conv_inner_shift,
    conv_out_weight,
    ffn2_gain,
    ffn2_shift,
    ffn2_in,
    ffn2_in_bias,
    ffn2_out,
    ffn2_out_bias,
    final_gain,
    final_shift,
):
    ffn1_in_all = gather_rows(ffn1_in)
    ffn1_out_all = gather_rows(ffn1_out)
    attn_all = gather_rows(
        jnp.concatenate([query_weight, key_weight, value_weight, attn_out_weight], axis=1)
    )
    conv_all = gather_rows(
        jnp.concatenate([conv_value_weight, conv_gate_weight, conv_out_weight], axis=1)
    )
    ffn2_in_all = gather_rows(ffn2_in)
    ffn2_out_all = gather_rows(ffn2_out)
    width = query_weight.shape[1]
    gathered = (
        ffn1_in_all,
        ffn1_out_all,
        attn_all[:, :width],
        attn_all[:, width : 2 * width],
        attn_all[:, 2 * width : 3 * width],
        attn_all[:, 3 * width :],
        conv_all[:, :width],
        conv_all[:, width : 2 * width],
        conv_all[:, 2 * width :],
        ffn2_in_all,
        ffn2_out_all,
    )
    tp_rank = lax.axis_index("tp")
    ctx_rank = lax.axis_index("ctx")
    hidden_local = gathered[0].shape[1]
    width_local = gathered[2].shape[1]
    ffn1_bias_local = local_cut(ffn1_in_bias, tp_rank, hidden_local)
    ffn2_bias_local = local_cut(ffn2_in_bias, tp_rank, hidden_local)
    query_bias_local = local_cut(query_bias, tp_rank, width_local)
    value_bias_local = local_cut(value_bias, tp_rank, width_local)
    depth_local = local_cut(conv_depth, tp_rank, width_local)
    inner_gain_local = local_cut(conv_inner_gain, tp_rank, width_local)
    inner_shift_local = local_cut(conv_inner_shift, tp_rank, width_local)
    stream_zero = inputs.astype(jnp.float32)
    stream_one, saved_one = ffn_forward(
        stream_zero, ffn1_gain, ffn1_shift, gathered[0], ffn1_bias_local, gathered[1], ffn1_out_bias
    )
    stream_two, saved_two = attn_forward(
        stream_one,
        attn_gain,
        attn_shift,
        (gathered[2], gathered[3], gathered[4], gathered[5]),
        (query_bias_local, value_bias_local, attn_out_bias),
        rel_table,
        ctx_rank,
    )
    stream_three, saved_three = conv_forward(
        stream_two,
        conv_gain,
        conv_shift,
        (gathered[6], gathered[7], gathered[8]),
        depth_local,
        inner_gain_local,
        inner_shift_local,
    )
    stream_four, saved_four = ffn_forward(
        stream_three,
        ffn2_gain,
        ffn2_shift,
        gathered[9],
        ffn2_bias_local,
        gathered[10],
        ffn2_out_bias,
    )
    final_out, final_standard, final_inverse = norm_forward(stream_four, final_gain, final_shift)
    live_slots = (
        jnp.arange(final_out.shape[0], dtype=jnp.int32) < clips_dev[lax.axis_index("fsdp")]
    ).astype(jnp.float32)
    misfit = (final_out - teacher.astype(jnp.float32)) * live_slots[:, None, None]
    sse_local = jnp.sum(misfit * misfit)
    gradient_fourth, final_gain_grad, final_shift_grad = norm_backward(
        2.0 * misfit, final_standard, final_inverse, final_gain
    )
    back_weights = gathered
    grad_three, ffn2_grads = ffn_backward(
        gradient_fourth, saved_four, ffn2_gain, back_weights[9], back_weights[10]
    )
    grad_two, conv_grads = conv_backward(
        grad_three,
        saved_three,
        conv_gain,
        (back_weights[6], back_weights[7], back_weights[8]),
        depth_local,
        inner_gain_local,
    )
    grad_one, attn_grads = attn_backward(
        grad_two,
        saved_two,
        attn_gain,
        (back_weights[2], back_weights[3], back_weights[4], back_weights[5]),
        rel_table,
        ctx_rank,
    )
    grad_zero, ffn1_grads = ffn_backward(
        grad_one, saved_one, ffn1_gain, back_weights[0], back_weights[1]
    )
    ffn2_parts = scatter_sum(ffn2_grads[2], ffn2_grads[4])
    conv_parts = scatter_sum(conv_grads[2], conv_grads[3], conv_grads[7])
    attn_parts = scatter_sum(attn_grads[2], attn_grads[4], attn_grads[5], attn_grads[7])
    ffn1_parts = scatter_sum(ffn1_grads[2], ffn1_grads[4])
    weight_parts = ffn1_parts + attn_parts + conv_parts + ffn2_parts
    shared = sum_small(
        (
            ffn1_grads[0],
            ffn1_grads[1],
            ffn1_grads[5],
            attn_grads[0],
            attn_grads[1],
            attn_grads[8],
            attn_grads[9],
            conv_grads[0],
            conv_grads[1],
            ffn2_grads[0],
            ffn2_grads[1],
            ffn2_grads[5],
            final_gain_grad,
            final_shift_grad,
            sse_local,
        ),
        (
            ffn1_grads[3],
            attn_grads[3],
            attn_grads[6],
            conv_grads[4],
            conv_grads[5],
            conv_grads[6],
            ffn2_grads[3],
        ),
        tp_rank,
    )
    token_count = (jnp.sum(clips_dev) * SEQ).astype(jnp.float32)
    loss = shared[21] / token_count
    return (
        final_out.astype(jnp.bfloat16),
        loss,
        grad_zero,
        shared[0],
        shared[1],
        weight_parts[0],
        shared[2],
        weight_parts[1],
        shared[3],
        shared[4],
        shared[5],
        weight_parts[2],
        shared[6],
        weight_parts[3],
        weight_parts[4],
        shared[7],
        weight_parts[5],
        shared[8],
        shared[9],
        shared[10],
        shared[11],
        weight_parts[6],
        weight_parts[7],
        shared[12],
        shared[13],
        shared[14],
        weight_parts[8],
        shared[15],
        shared[16],
        weight_parts[9],
        shared[17],
        weight_parts[10],
        shared[18],
        shared[19],
        shared[20],
    )


def solution(mesh):
    in_specs = (
        P("fsdp", ("ctx", "tp"), None),
        P("fsdp", ("ctx", "tp"), None),
        P(),
        P(),
        P(),
        P(("fsdp", "ctx"), "tp"),
        P(),
        P(("fsdp", "ctx"), "tp"),
        P(),
        P(),
        P(),
        P(("fsdp", "ctx"), "tp"),
        P(),
        P(("fsdp", "ctx"), "tp"),
        P(("fsdp", "ctx"), "tp"),
        P(),
        P(("fsdp", "ctx"), "tp"),
        P(),
        P(),
        P(),
        P(),
        P(("fsdp", "ctx"), "tp"),
        P(("fsdp", "ctx"), "tp"),
        P(),
        P(),
        P(),
        P(("fsdp", "ctx"), "tp"),
        P(),
        P(),
        P(("fsdp", "ctx"), "tp"),
        P(),
        P(("fsdp", "ctx"), "tp"),
        P(),
        P(),
        P(),
    )
    out_specs = (
        P("fsdp", ("ctx", "tp"), None),
        P(),
        P("fsdp", ("ctx", "tp"), None),
        P(),
        P(),
        P(("fsdp", "ctx"), "tp"),
        P(),
        P(("fsdp", "ctx"), "tp"),
        P(),
        P(),
        P(),
        P(("fsdp", "ctx"), "tp"),
        P(),
        P(("fsdp", "ctx"), "tp"),
        P(("fsdp", "ctx"), "tp"),
        P(),
        P(("fsdp", "ctx"), "tp"),
        P(),
        P(),
        P(),
        P(),
        P(("fsdp", "ctx"), "tp"),
        P(("fsdp", "ctx"), "tp"),
        P(),
        P(),
        P(),
        P(("fsdp", "ctx"), "tp"),
        P(),
        P(),
        P(("fsdp", "ctx"), "tp"),
        P(),
        P(("fsdp", "ctx"), "tp"),
        P(),
        P(),
        P(),
    )
    return jax.shard_map(body, mesh=mesh, in_specs=in_specs, out_specs=out_specs, check_vma=False)
```

```python
import functools
import math

import jax
import jax.numpy as jnp
from jax import lax
from jax.experimental import pallas as pl
from jax.experimental.pallas import tpu as pltpu
from jax.sharding import PartitionSpec as P

D = 1024
LEFT = 64
HEAD = 64
SEQ = 1536


epsilon = 1e-05


def from_behind(shard, axis, by):
    devices = lax.axis_size(axis)
    pairs = [(i, i + by) for i in range(devices) if 0 <= i + by < devices]
    return lax.ppermute(shard, axis, pairs)


def norm_forward(stream, norm_gain, norm_shift):
    centred = stream - jnp.mean(stream, axis=-1, keepdims=True)
    inverse = lax.rsqrt(jnp.mean(centred * centred, axis=-1, keepdims=True) + epsilon)
    standard = centred * inverse
    return (standard * norm_gain + norm_shift, standard, inverse)


def norm_backward(grad_out, standard, inverse, norm_gain):
    grad_standard = grad_out * norm_gain
    mean_first = jnp.mean(grad_standard, axis=-1, keepdims=True)
    mean_second = jnp.mean(grad_standard * standard, axis=-1, keepdims=True)
    grad_in = inverse * (grad_standard - mean_first - standard * mean_second)
    return (grad_in, jnp.sum(grad_out * standard, axis=(0, 1)), jnp.sum(grad_out, axis=(0, 1)))


def silu_slope(hidden_pre):
    gate_sig = jax.nn.sigmoid(hidden_pre)
    return gate_sig * (1.0 + hidden_pre * (1.0 - gate_sig))


def rows_in(left_reach, right_reach):
    return jnp.einsum("zub,bx->zux", left_reach, right_reach, preferred_element_type=jnp.float32)


def rows_out(left_reach, right_reach):
    return jnp.einsum("anp,op->ano", left_reach, right_reach, preferred_element_type=jnp.float32)


def weight_sum(left_reach, right_reach):
    return jnp.einsum("zbt,zbm->tm", left_reach, right_reach, preferred_element_type=jnp.float32)


def widen(normed):
    return lax.all_gather(normed.astype(jnp.bfloat16), "tp", axis=1, tiled=True)


def narrow(partial_rows):
    return lax.psum_scatter(
        partial_rows.astype(jnp.bfloat16), "tp", scatter_dimension=1, tiled=True
    ).astype(jnp.float32)


def widen_grad(grad_branch):
    return lax.all_gather(grad_branch, "tp", axis=1, tiled=True)


def narrow_grad(partial_rows):
    return lax.psum_scatter(
        partial_rows.astype(jnp.bfloat16), "tp", scatter_dimension=1, tiled=True
    ).astype(jnp.float32)


def local_cut(full_array, tp_rank, size_local):
    return lax.dynamic_slice_in_dim(
        full_array, tp_rank * size_local, size_local, full_array.ndim - 1
    )


def local_put(local_array, tp_rank, full_size):
    shape_full = local_array.shape[:-1] + (full_size,)
    return lax.dynamic_update_slice_in_dim(
        jnp.zeros(shape_full, jnp.float32),
        local_array,
        tp_rank * local_array.shape[-1],
        local_array.ndim - 1,
    )


BAND = 384


def wide_table(rel_table):
    before = jnp.broadcast_to(rel_table[:1], (LEFT, HEAD))
    after = jnp.broadcast_to(rel_table[-1:], (BAND - LEFT - rel_table.shape[0], HEAD))
    return jnp.concatenate([before, rel_table, after], axis=0)


def dot_t(left, right):
    return lax.dot_general(left, right, (((1,), (1,)), ((), ())), preferred_element_type=jnp.float32)


def dot_n(left, right):
    return lax.dot_general(left, right, (((1,), (0,)), ((), ())), preferred_element_type=jnp.float32)


def scaled_scores(query_block, keys, table, place, rows_at, reach):
    rows = query_block.shape[0]
    key_count = keys.shape[0]
    near = dot_t(query_block, table)
    left, right = near[:, :1], near[:, BAND - 1 :]
    row = lax.broadcasted_iota(jnp.int32, (rows, key_count), 0)
    col = lax.broadcasted_iota(jnp.int32, (rows, key_count), 1)
    place[:, 128 : 128 + key_count] = dot_t(query_block, keys) + jnp.where(
        col < row + rows_at, left, right
    )
    rolled = pltpu.roll(near, 0, 1, stride=1, stride_axis=0)
    apart = band_distance(rows)
    band = jnp.where(apart <= -LEFT, left, jnp.where(apart >= reach, right, rolled))
    window = pl.ds(pl.multiple_of(rows_at, 128), BAND)
    place[:, window] += band - jnp.where(apart < 0, left, right)
    return place[:, 128 : 128 + key_count]


def band_distance(rows):
    row = lax.broadcasted_iota(jnp.int32, (rows, BAND), 0)
    col = lax.broadcasted_iota(jnp.int32, (rows, BAND), 1)
    return col - 128 - row


def attend_kernel(reach, start_ref, query_ref, key_ref, value_ref, table_ref, mixed_ref, total_ref, place):
    rows = query_ref.shape[1]
    rows_at = start_ref[0] + pl.program_id(2) * rows
    table = table_ref[...]
    for half in range(query_ref.shape[2] // HEAD):
        lanes = slice(half * HEAD, (half + 1) * HEAD)
        query_block = query_ref[0, :, lanes] * jnp.bfloat16(1.0 / math.sqrt(HEAD))
        scores = scaled_scores(query_block, key_ref[0, :, lanes], table, place, rows_at, reach)
        top = jnp.max(scores, axis=-1, keepdims=True)
        powers = jnp.exp(scores - top)
        row_sum = jnp.sum(powers, axis=-1, keepdims=True)
        probs = (powers * (1.0 / row_sum)).astype(jnp.bfloat16)
        mixed_ref[0, :, lanes] = dot_n(probs, value_ref[0, :, lanes]).astype(jnp.bfloat16)
        total_ref[0, :, lanes] = jnp.broadcast_to(top + jnp.log(row_sum), (rows, HEAD))


def attend_back_kernel(
    reach, start_ref, query_ref, key_ref, value_ref, table_ref, total_ref, grad_ref,
    query_grad_ref, key_grad_ref, value_grad_ref, table_grad_ref, place, key_sum, value_sum,
):
    rows = query_ref.shape[1]
    key_count = key_ref.shape[1]
    block = pl.program_id(2)
    rows_at = start_ref[0] + block * rows
    table = table_ref[...]
    scale = jnp.bfloat16(1.0 / math.sqrt(HEAD))

    @pl.when(block == 0)
    def _():
        key_sum[...] = jnp.zeros_like(key_sum)
        value_sum[...] = jnp.zeros_like(value_sum)

    @pl.when((block == 0) & (pl.program_id(0) == 0) & (pl.program_id(1) == 0))
    def _():
        table_grad_ref[...] = jnp.zeros_like(table_grad_ref)

    for half in range(query_ref.shape[2] // HEAD):
        lanes = slice(half * HEAD, (half + 1) * HEAD)
        query_block = query_ref[0, :, lanes] * scale
        keys = key_ref[0, :, lanes]
        grad_block = grad_ref[0, :, lanes]
        scores = scaled_scores(query_block, keys, table, place, rows_at, reach)
        probs = jnp.exp(scores - total_ref[0, :, half * HEAD : half * HEAD + 1])
        grad_probs = dot_t(grad_block, value_ref[0, :, lanes])
        row_dot = jnp.sum(probs * grad_probs, axis=-1, keepdims=True)
        grad_scores = (probs * (grad_probs - row_dot)).astype(jnp.bfloat16)
        value_sum[lanes, :] += dot_n(grad_block.T, probs.astype(jnp.bfloat16))
        key_sum[lanes, :] += dot_n(query_block.T, grad_scores)
        wide = grad_scores.astype(jnp.float32)
        place[:, 128 : 128 + key_count] = wide
        apart_all = (
            lax.broadcasted_iota(jnp.int32, wide.shape, 1)
            - lax.broadcasted_iota(jnp.int32, wide.shape, 0)
            - rows_at
        )
        far_left = jnp.sum(jnp.where(apart_all <= -LEFT, wide, 0.0), axis=-1, keepdims=True)
        far_right = jnp.sum(jnp.where(apart_all >= reach, wide, 0.0), axis=-1, keepdims=True)
        window = place[:, pl.ds(pl.multiple_of(rows_at, 128), BAND)]
        window_col = lax.broadcasted_iota(jnp.int32, window.shape, 1) + rows_at - 128
        apart = band_distance(rows)
        inside = (apart > -LEFT) & (apart < reach) & (window_col >= 0) & (window_col < key_count)
        turned = jnp.where(inside, window, 0.0)
        row = lax.broadcasted_iota(jnp.int32, turned.shape, 0)
        for bit in range((rows - 1).bit_length()):
            moved = pltpu.roll(turned, BAND - (1 << bit), 1)
            turned = jnp.where(((row >> bit) & 1) == 1, moved, turned)
        lane = lax.broadcasted_iota(jnp.int32, turned.shape, 1)
        by_row = jnp.where(lane == LEFT, far_left, jnp.where(lane == 2 * LEFT + reach, far_right, turned))
        coarse = by_row.astype(jnp.bfloat16)
        fine = (by_row - coarse.astype(jnp.float32)).astype(jnp.bfloat16)
        query_grad = dot_n(grad_scores, keys) + dot_n(coarse, table) + dot_n(fine, table)
        query_grad_ref[0, :, lanes] = (query_grad * (1.0 / math.sqrt(HEAD))).astype(jnp.bfloat16)
        query_turned = query_block.T
        table_grad_ref[...] += dot_n(query_turned, coarse) + dot_n(query_turned, fine)

    @pl.when(block == pl.num_programs(2) - 1)
    def _():
        key_grad_ref[0] = key_sum[...].T.astype(jnp.bfloat16)
        value_grad_ref[0] = value_sum[...].T.astype(jnp.bfloat16)


def attend_specs(queries, keys):
    slots, rows, width = queries.shape
    lanes = 2 * HEAD
    block = 128
    grid = (slots, width // lanes, rows // block)
    by_query = pl.BlockSpec((1, block, lanes), lambda s, p, b, *_: (s, b, p))
    by_key = pl.BlockSpec((1, keys.shape[1], lanes), lambda s, p, b, *_: (s, 0, p))
    table = pl.BlockSpec((BAND, HEAD), lambda s, p, b, *_: (0, 0))
    place = pltpu.VMEM((block, keys.shape[1] + 256), jnp.float32)
    flops = slots * rows * keys.shape[1] * width * 4
    return grid, by_query, by_key, table, place, flops


def attend(queries, keys, values, table, reach, query_start):
    grid, by_query, by_key, by_table, place, flops = attend_specs(queries, keys)
    return pl.pallas_call(
        functools.partial(attend_kernel, reach),
        out_shape=(
            jax.ShapeDtypeStruct(queries.shape, jnp.bfloat16),
            jax.ShapeDtypeStruct(queries.shape, jnp.float32),
        ),
        grid_spec=pltpu.PrefetchScalarGridSpec(
            num_scalar_prefetch=1,
            grid=grid,
            in_specs=[by_query, by_key, by_key, by_table],
            out_specs=(by_query, by_query),
            scratch_shapes=[place],
        ),
        cost_estimate=pl.CostEstimate(flops=2 * flops, bytes_accessed=8 << 20, transcendentals=flops >> 8),
        name="attend",
    )(query_start.reshape(1), queries, keys, values, table)


def attend_back(queries, keys, values, table, totals, grad_mixed, reach, query_start):
    grid, by_query, by_key, by_table, place, flops = attend_specs(queries, keys)
    turned = pltpu.VMEM((2 * HEAD, keys.shape[1]), jnp.float32)
    return pl.pallas_call(
        functools.partial(attend_back_kernel, reach),
        out_shape=(
            jax.ShapeDtypeStruct(queries.shape, jnp.bfloat16),
            jax.ShapeDtypeStruct(keys.shape, jnp.bfloat16),
            jax.ShapeDtypeStruct(keys.shape, jnp.bfloat16),
            jax.ShapeDtypeStruct((HEAD, BAND), jnp.float32),
        ),
        grid_spec=pltpu.PrefetchScalarGridSpec(
            num_scalar_prefetch=1,
            grid=grid,
            in_specs=[by_query, by_key, by_key, by_table, by_query, by_query],
            out_specs=(
                by_query,
                by_key,
                by_key,
                pl.BlockSpec((HEAD, BAND), lambda s, p, b, *_: (0, 0)),
            ),
            scratch_shapes=[place, turned, turned],
        ),
        cost_estimate=pl.CostEstimate(flops=5 * flops, bytes_accessed=16 << 20, transcendentals=flops >> 8),
        name="attend_back",
    )(query_start.reshape(1), queries, keys, values, table, totals, grad_mixed)


def ffn_forward(stream, norm_gain, norm_shift, weight_in, bias_in, weight_out, bias_out):
    normed, standard, inverse = norm_forward(stream, norm_gain, norm_shift)
    wide_rows = widen(normed)
    hidden_pre = rows_in(wide_rows, weight_in) + bias_in
    active = jax.nn.silu(hidden_pre).astype(jnp.bfloat16)
    branch = narrow(rows_out(active, weight_out)) + bias_out
    return (stream + 0.5 * branch, (standard, inverse, wide_rows, hidden_pre))


def ffn_backward(grad_stream, saved, norm_gain, weight_in, weight_out):
    standard, inverse, wide_rows, hidden_pre = saved
    grad_branch = (0.5 * grad_stream).astype(jnp.bfloat16)
    out_bias_grad = jnp.sum(grad_branch.astype(jnp.float32), axis=(0, 1))
    wide_grad = widen_grad(grad_branch)
    active = jax.nn.silu(hidden_pre).astype(jnp.bfloat16)
    out_grad = weight_sum(wide_grad, active)
    grad_pre = (rows_in(wide_grad, weight_out) * silu_slope(hidden_pre)).astype(jnp.bfloat16)
    in_bias_grad = jnp.sum(grad_pre.astype(jnp.float32), axis=(0, 1))
    in_grad = weight_sum(wide_rows, grad_pre)
    grad_normed = narrow_grad(rows_out(grad_pre, weight_in))
    grad_in, gain_grad, shift_grad = norm_backward(grad_normed, standard, inverse, norm_gain)
    return (
        grad_stream + grad_in,
        (gain_grad, shift_grad, in_grad, in_bias_grad, out_grad, out_bias_grad),
    )


def attn_forward(stream, norm_gain, norm_shift, weights, biases, rel_table, ctx_rank):
    query_w, key_w, value_w, out_w = weights
    query_b, value_b, out_b = biases
    normed, standard, inverse = norm_forward(stream, norm_gain, norm_shift)
    wide_rows = widen(normed)
    queries = (rows_in(wide_rows, query_w) + query_b).astype(jnp.bfloat16)
    keys_local = rows_in(wide_rows, key_w).astype(jnp.bfloat16)
    values_local = (rows_in(wide_rows, value_w) + value_b).astype(jnp.bfloat16)
    keys_all, values_all = (
        lax.all_gather(keys_local, "ctx", axis=1, tiled=True),
        lax.all_gather(values_local, "ctx", axis=1, tiled=True),
    )
    reach = rel_table.shape[0] - 1 - LEFT
    mixed_token_rows, log_total = attend(
        queries, keys_all, values_all, wide_table(rel_table), reach, ctx_rank * queries.shape[1]
    )
    branch = narrow(rows_out(mixed_token_rows, out_w)) + out_b
    return (
        stream + branch,
        (standard, inverse, wide_rows, queries, keys_all, values_all, mixed_token_rows, log_total),
    )


def attn_backward(grad_stream, saved, norm_gain, weights, rel_table, ctx_rank):
    query_w, key_w, value_w, out_w = weights
    standard, inverse, wide_rows, queries, keys_all, values_all, mixed_token_rows, log_total = saved
    grad_branch = grad_stream.astype(jnp.bfloat16)
    out_bias_grad = jnp.sum(grad_branch.astype(jnp.float32), axis=(0, 1))
    wide_grad = widen_grad(grad_branch)
    out_grad = weight_sum(wide_grad, mixed_token_rows)
    grad_mixed = rows_in(wide_grad, out_w).astype(jnp.bfloat16)
    reach = rel_table.shape[0] - 1 - LEFT
    query_low, key_terms, value_terms, table_turned = attend_back(
        queries,
        keys_all,
        values_all,
        wide_table(rel_table),
        log_total,
        grad_mixed,
        reach,
        ctx_rank * queries.shape[1],
    )
    table_grad = table_turned[:, LEFT : LEFT + rel_table.shape[0]].T
    key_grad, value_grad = (
        lax.psum_scatter(key_terms, "ctx", scatter_dimension=1, tiled=True),
        lax.psum_scatter(value_terms, "ctx", scatter_dimension=1, tiled=True),
    )
    key_low = key_grad.astype(jnp.bfloat16)
    value_low = value_grad.astype(jnp.bfloat16)
    query_bias_grad = jnp.sum(query_low.astype(jnp.float32), axis=(0, 1))
    value_bias_grad = jnp.sum(value_low.astype(jnp.float32), axis=(0, 1))
    query_w_grad = weight_sum(wide_rows, query_low)
    key_w_grad = weight_sum(wide_rows, key_low)
    value_w_grad = weight_sum(wide_rows, value_low)
    grad_normed = narrow_grad(
        rows_out(query_low, query_w) + rows_out(key_low, key_w) + rows_out(value_low, value_w)
    )
    grad_in, gain_grad, shift_grad = norm_backward(grad_normed, standard, inverse, norm_gain)
    return (
        grad_stream + grad_in,
        (
            gain_grad,
            shift_grad,
            query_w_grad,
            query_bias_grad,
            key_w_grad,
            value_w_grad,
            value_bias_grad,
            out_grad,
            out_bias_grad,
            table_grad,
        ),
    )


def conv_forward(stream, norm_gain, norm_shift, weights, depth_local, inner_gain, inner_offset):
    value_w, gate_w, out_w = weights
    normed, standard, inverse = norm_forward(stream, norm_gain, norm_shift)
    wide_rows = widen(normed)
    part_value = rows_in(wide_rows, value_w)
    part_gate = rows_in(wide_rows, gate_w)
    gated_rows = (part_value * jax.nn.sigmoid(part_gate)).astype(jnp.bfloat16)
    row_count = gated_rows.shape[1]
    reach_rows = depth_local.shape[0] - 1
    halo_rows = from_behind(gated_rows[:, row_count - reach_rows :, :], "ctx", 1)
    padded = jnp.concatenate([halo_rows, gated_rows], axis=1)
    padded_float = padded.astype(jnp.float32)
    convolved = depth_local[0] * padded_float[:, 0:row_count, :]
    for tap_index in range(1, depth_local.shape[0]):
        convolved = (
            convolved
            + depth_local[tap_index] * padded_float[:, tap_index : tap_index + row_count, :]
        )
    row_sums = lax.psum(
        (jnp.sum(convolved, axis=-1), jnp.sum(convolved * convolved, axis=-1)), "tp"
    )
    row_mean = (row_sums[0] / D)[..., None]
    row_var = (row_sums[1] / D)[..., None] - row_mean * row_mean
    inner_inverse = lax.rsqrt(row_var + epsilon)
    inner_standard = (convolved - row_mean) * inner_inverse
    inner_pre = inner_standard * inner_gain + inner_offset
    active = jax.nn.silu(inner_pre).astype(jnp.bfloat16)
    branch = narrow(rows_out(active, out_w))
    return (
        stream + branch,
        (
            standard,
            inverse,
            wide_rows,
            part_value,
            part_gate,
            padded,
            inner_standard,
            inner_inverse,
            inner_pre,
        ),
    )


def conv_backward(grad_stream, saved, norm_gain, weights, depth_local, inner_gain):
    value_w, gate_w, out_w = weights
    (
        standard,
        inverse,
        wide_rows,
        part_value,
        part_gate,
        padded,
        inner_standard,
        inner_inverse,
        inner_pre,
    ) = saved
    grad_branch = grad_stream.astype(jnp.bfloat16)
    wide_grad = widen_grad(grad_branch)
    active = jax.nn.silu(inner_pre).astype(jnp.bfloat16)
    out_grad = weight_sum(wide_grad, active)
    grad_inner = rows_in(wide_grad, out_w) * silu_slope(inner_pre)
    inner_gain_grad = jnp.sum(grad_inner * inner_standard, axis=(0, 1))
    inner_shift_grad = jnp.sum(grad_inner, axis=(0, 1))
    grad_standard = grad_inner * inner_gain
    row_sums = lax.psum(
        (jnp.sum(grad_standard, axis=-1), jnp.sum(grad_standard * inner_standard, axis=-1)), "tp"
    )
    grad_conv = inner_inverse * (
        grad_standard - (row_sums[0] / D)[..., None] - inner_standard * (row_sums[1] / D)[..., None]
    )
    row_count = grad_conv.shape[1]
    tap_count = depth_local.shape[0]
    reach_rows = tap_count - 1
    padded_float = padded.astype(jnp.float32)
    depth_grad = jnp.stack(
        [
            jnp.sum(grad_conv * padded_float[:, tap_index : tap_index + row_count, :], axis=(0, 1))
            for tap_index in range(tap_count)
        ]
    )
    grad_padded = jnp.zeros(padded.shape, jnp.float32)
    for tap_index in range(tap_count):
        grad_padded = grad_padded.at[:, tap_index : tap_index + row_count, :].add(
            depth_local[tap_index] * grad_conv
        )
    back_halo = from_behind(grad_padded[:, :reach_rows, :].astype(jnp.bfloat16), "ctx", -1).astype(
        jnp.float32
    )
    grad_gated = grad_padded[:, reach_rows:, :] + jnp.pad(
        back_halo, ((0, 0), (row_count - reach_rows, 0), (0, 0))
    )
    gate_sig = jax.nn.sigmoid(part_gate)
    grad_value = (grad_gated * gate_sig).astype(jnp.bfloat16)
    grad_gate = (grad_gated * part_value * gate_sig * (1.0 - gate_sig)).astype(jnp.bfloat16)
    value_w_grad = weight_sum(wide_rows, grad_value)
    gate_w_grad = weight_sum(wide_rows, grad_gate)
    grad_normed = narrow_grad(rows_out(grad_value, value_w) + rows_out(grad_gate, gate_w))
    grad_in, gain_grad, shift_grad = norm_backward(grad_normed, standard, inverse, norm_gain)
    return (
        grad_stream + grad_in,
        (
            gain_grad,
            shift_grad,
            value_w_grad,
            gate_w_grad,
            depth_grad,
            inner_gain_grad,
            inner_shift_grad,
            out_grad,
        ),
    )


def gather_rows(shard):
    return lax.all_gather(shard, ("fsdp", "ctx"), axis=0, tiled=True)


def scatter_sum(*grads):
    joined = jnp.concatenate([grad.astype(jnp.bfloat16) for grad in grads], axis=1)
    part = lax.psum_scatter(joined, ("fsdp", "ctx"), scatter_dimension=0, tiled=True)
    pieces = []
    start = 0
    for grad in grads:
        pieces.append(part[:, start : start + grad.shape[1]].astype(jnp.float32))
        start += grad.shape[1]
    return tuple(pieces)


def sum_small(whole_parts, split_parts, tp_rank):
    tp_count = lax.axis_size("tp")
    split = jnp.concatenate([part.reshape(-1) for part in split_parts])
    spread = lax.dynamic_update_slice(
        jnp.zeros((tp_count, split.shape[0]), jnp.float32), split[None], (tp_rank, 0)
    )
    flat = jnp.concatenate([part.reshape(-1) for part in whole_parts] + [spread.reshape(-1)])
    count = flat.shape[0]
    flat = jnp.pad(flat, (0, -count % 1024)).reshape(-1, 128)
    total = lax.psum(flat, ("fsdp", "ctx", "tp")).reshape(-1)
    whole = []
    start = 0
    for part in whole_parts:
        whole.append(total[start : start + part.size].reshape(part.shape))
        start += part.size
    spread = total[start : start + tp_count * split.shape[0]].reshape(tp_count, -1)
    pieces = []
    start = 0
    for part in split_parts:
        piece = spread[:, start : start + part.size]
        if part.ndim == 1:
            pieces.append(piece.reshape(-1))
        else:
            piece = piece.reshape((tp_count,) + part.shape)
            pieces.append(piece.transpose(1, 0, 2).reshape(part.shape[0], -1))
        start += part.size
    w, p = whole, pieces
    return (
        w[0], w[1], p[0], w[2], w[3], w[4], p[1], p[2], w[5], w[6], w[7], w[8],
        p[3], p[4], p[5], w[9], w[10], p[6], w[11], w[12], w[13], w[14],
    )


def body(
    inputs,
    teacher,
    clips_dev,
    ffn1_gain,
    ffn1_shift,
    ffn1_in,
    ffn1_in_bias,
    ffn1_out,
    ffn1_out_bias,
    attn_gain,
    attn_shift,
    query_weight,
    query_bias,
    key_weight,
    value_weight,
    value_bias,
    attn_out_weight,
    attn_out_bias,
    rel_table,
    conv_gain,
    conv_shift,
    conv_value_weight,
    conv_gate_weight,
    conv_depth,
    conv_inner_gain,
    conv_inner_shift,
    conv_out_weight,
    ffn2_gain,
    ffn2_shift,
    ffn2_in,
    ffn2_in_bias,
    ffn2_out,
    ffn2_out_bias,
    final_gain,
    final_shift,
):
    ffn1_in_all = gather_rows(ffn1_in)
    ffn1_out_all = gather_rows(ffn1_out)
    attn_all = gather_rows(
        jnp.concatenate([query_weight, key_weight, value_weight, attn_out_weight], axis=1)
    )
    conv_all = gather_rows(
        jnp.concatenate([conv_value_weight, conv_gate_weight, conv_out_weight], axis=1)
    )
    ffn2_in_all = gather_rows(ffn2_in)
    ffn2_out_all = gather_rows(ffn2_out)
    width = query_weight.shape[1]
    gathered = (
        ffn1_in_all,
        ffn1_out_all,
        attn_all[:, :width],
        attn_all[:, width : 2 * width],
        attn_all[:, 2 * width : 3 * width],
        attn_all[:, 3 * width :],
        conv_all[:, :width],
        conv_all[:, width : 2 * width],
        conv_all[:, 2 * width :],
        ffn2_in_all,
        ffn2_out_all,
    )
    tp_rank = lax.axis_index("tp")
    ctx_rank = lax.axis_index("ctx")
    hidden_local = gathered[0].shape[1]
    width_local = gathered[2].shape[1]
    ffn1_bias_local = local_cut(ffn1_in_bias, tp_rank, hidden_local)
    ffn2_bias_local = local_cut(ffn2_in_bias, tp_rank, hidden_local)
    query_bias_local = local_cut(query_bias, tp_rank, width_local)
    value_bias_local = local_cut(value_bias, tp_rank, width_local)
    depth_local = local_cut(conv_depth, tp_rank, width_local)
    inner_gain_local = local_cut(conv_inner_gain, tp_rank, width_local)
    inner_shift_local = local_cut(conv_inner_shift, tp_rank, width_local)
    stream_zero = inputs.astype(jnp.float32)
    stream_one, saved_one = ffn_forward(
        stream_zero, ffn1_gain, ffn1_shift, gathered[0], ffn1_bias_local, gathered[1], ffn1_out_bias
    )
    stream_two, saved_two = attn_forward(
        stream_one,
        attn_gain,
        attn_shift,
        (gathered[2], gathered[3], gathered[4], gathered[5]),
        (query_bias_local, value_bias_local, attn_out_bias),
        rel_table,
        ctx_rank,
    )
    stream_three, saved_three = conv_forward(
        stream_two,
        conv_gain,
        conv_shift,
        (gathered[6], gathered[7], gathered[8]),
        depth_local,
        inner_gain_local,
        inner_shift_local,
    )
    stream_four, saved_four = ffn_forward(
        stream_three,
        ffn2_gain,
        ffn2_shift,
        gathered[9],
        ffn2_bias_local,
        gathered[10],
        ffn2_out_bias,
    )
    final_out, final_standard, final_inverse = norm_forward(stream_four, final_gain, final_shift)
    live_slots = (
        jnp.arange(final_out.shape[0], dtype=jnp.int32) < clips_dev[lax.axis_index("fsdp")]
    ).astype(jnp.float32)
    misfit = (final_out - teacher.astype(jnp.float32)) * live_slots[:, None, None]
    sse_local = jnp.sum(misfit * misfit)
    gradient_fourth, final_gain_grad, final_shift_grad = norm_backward(
        2.0 * misfit, final_standard, final_inverse, final_gain
    )
    back_weights = gathered
    grad_three, ffn2_grads = ffn_backward(
        gradient_fourth, saved_four, ffn2_gain, back_weights[9], back_weights[10]
    )
    grad_two, conv_grads = conv_backward(
        grad_three,
        saved_three,
        conv_gain,
        (back_weights[6], back_weights[7], back_weights[8]),
        depth_local,
        inner_gain_local,
    )
    grad_one, attn_grads = attn_backward(
        grad_two,
        saved_two,
        attn_gain,
        (back_weights[2], back_weights[3], back_weights[4], back_weights[5]),
        rel_table,
        ctx_rank,
    )
    grad_zero, ffn1_grads = ffn_backward(
        grad_one, saved_one, ffn1_gain, back_weights[0], back_weights[1]
    )
    ffn2_parts = scatter_sum(ffn2_grads[2], ffn2_grads[4])
    conv_parts = scatter_sum(conv_grads[2], conv_grads[3], conv_grads[7])
    attn_parts = scatter_sum(attn_grads[2], attn_grads[4], attn_grads[5], attn_grads[7])
    ffn1_parts = scatter_sum(ffn1_grads[2], ffn1_grads[4])
    weight_parts = ffn1_parts + attn_parts + conv_parts + ffn2_parts
    shared = sum_small(
        (
            ffn1_grads[0],
            ffn1_grads[1],
            ffn1_grads[5],
            attn_grads[0],
            attn_grads[1],
            attn_grads[8],
            attn_grads[9],
            conv_grads[0],
            conv_grads[1],
            ffn2_grads[0],
            ffn2_grads[1],
            ffn2_grads[5],
            final_gain_grad,
            final_shift_grad,
            sse_local,
        ),
        (
            ffn1_grads[3],
            attn_grads[3],
            attn_grads[6],
            conv_grads[4],
            conv_grads[5],
            conv_grads[6],
            ffn2_grads[3],
        ),
        tp_rank,
    )
    token_count = (jnp.sum(clips_dev) * SEQ).astype(jnp.float32)
    loss = shared[21] / token_count
    return (
        final_out.astype(jnp.bfloat16),
        loss,
        grad_zero,
        shared[0],
        shared[1],
        weight_parts[0],
        shared[2],
        weight_parts[1],
        shared[3],
        shared[4],
        shared[5],
        weight_parts[2],
        shared[6],
        weight_parts[3],
        weight_parts[4],
        shared[7],
        weight_parts[5],
        shared[8],
        shared[9],
        shared[10],
        shared[11],
        weight_parts[6],
        weight_parts[7],
        shared[12],
        shared[13],
        shared[14],
        weight_parts[8],
        shared[15],
        shared[16],
        weight_parts[9],
        shared[17],
        weight_parts[10],
        shared[18],
        shared[19],
        shared[20],
    )


def solution(mesh):
    in_specs = (
        P("fsdp", ("ctx", "tp"), None),
        P("fsdp", ("ctx", "tp"), None),
        P(),
        P(),
        P(),
        P(("fsdp", "ctx"), "tp"),
        P(),
        P(("fsdp", "ctx"), "tp"),
        P(),
        P(),
        P(),
        P(("fsdp", "ctx"), "tp"),
        P(),
        P(("fsdp", "ctx"), "tp"),
        P(("fsdp", "ctx"), "tp"),
        P(),
        P(("fsdp", "ctx"), "tp"),
        P(),
        P(),
        P(),
        P(),
        P(("fsdp", "ctx"), "tp"),
        P(("fsdp", "ctx"), "tp"),
        P(),
        P(),
        P(),
        P(("fsdp", "ctx"), "tp"),
        P(),
        P(),
        P(("fsdp", "ctx"), "tp"),
        P(),
        P(("fsdp", "ctx"), "tp"),
        P(),
        P(),
        P(),
    )
    out_specs = (
        P("fsdp", ("ctx", "tp"), None),
        P(),
        P("fsdp", ("ctx", "tp"), None),
        P(),
        P(),
        P(("fsdp", "ctx"), "tp"),
        P(),
        P(("fsdp", "ctx"), "tp"),
        P(),
        P(),
        P(),
        P(("fsdp", "ctx"), "tp"),
        P(),
        P(("fsdp", "ctx"), "tp"),
        P(("fsdp", "ctx"), "tp"),
        P(),
        P(("fsdp", "ctx"), "tp"),
        P(),
        P(),
        P(),
        P(),
        P(("fsdp", "ctx"), "tp"),
        P(("fsdp", "ctx"), "tp"),
        P(),
        P(),
        P(),
        P(("fsdp", "ctx"), "tp"),
        P(),
        P(),
        P(("fsdp", "ctx"), "tp"),
        P(),
        P(("fsdp", "ctx"), "tp"),
        P(),
        P(),
        P(),
    )
    return jax.shard_map(body, mesh=mesh, in_specs=in_specs, out_specs=out_specs, check_vma=False)
```

```python
import functools
import math

import jax
import jax.numpy as jnp
from jax import lax
from jax.experimental import pallas as pl
from jax.experimental.pallas import tpu as pltpu
from jax.sharding import PartitionSpec as P

D = 1024
LEFT = 64
HEAD = 64
SEQ = 1536


epsilon = 1e-05


def from_behind(shard, axis, by):
    devices = lax.axis_size(axis)
    pairs = [(i, i + by) for i in range(devices) if 0 <= i + by < devices]
    return lax.ppermute(shard, axis, pairs)


def norm_forward(stream, norm_gain, norm_shift):
    centred = stream - jnp.mean(stream, axis=-1, keepdims=True)
    inverse = lax.rsqrt(jnp.mean(centred * centred, axis=-1, keepdims=True) + epsilon)
    standard = centred * inverse
    return (standard * norm_gain + norm_shift, standard, inverse)


def norm_backward(grad_out, standard, inverse, norm_gain):
    grad_standard = grad_out * norm_gain
    mean_first = jnp.mean(grad_standard, axis=-1, keepdims=True)
    mean_second = jnp.mean(grad_standard * standard, axis=-1, keepdims=True)
    grad_in = inverse * (grad_standard - mean_first - standard * mean_second)
    return (grad_in, jnp.sum(grad_out * standard, axis=(0, 1)), jnp.sum(grad_out, axis=(0, 1)))


def silu_slope(hidden_pre):
    gate_sig = jax.nn.sigmoid(hidden_pre)
    return gate_sig * (1.0 + hidden_pre * (1.0 - gate_sig))


def rows_in(left_reach, right_reach):
    return jnp.einsum("zub,bx->zux", left_reach, right_reach, preferred_element_type=jnp.float32)


def rows_out(left_reach, right_reach):
    return jnp.einsum("anp,op->ano", left_reach, right_reach, preferred_element_type=jnp.float32)


def weight_sum(left_reach, right_reach):
    return jnp.einsum("zbt,zbm->tm", left_reach, right_reach, preferred_element_type=jnp.float32)


def together(*values):
    return lax.optimization_barrier(values)


def widen(normed):
    return lax.all_gather(normed.astype(jnp.bfloat16), "tp", axis=1, tiled=True)


def narrow(partial_rows):
    return lax.psum_scatter(
        partial_rows.astype(jnp.bfloat16), "tp", scatter_dimension=1, tiled=True
    ).astype(jnp.float32)


def widen_grad(grad_branch):
    return lax.all_gather(grad_branch, "tp", axis=1, tiled=True)


def narrow_grad(partial_rows):
    return lax.psum_scatter(
        partial_rows.astype(jnp.bfloat16), "tp", scatter_dimension=1, tiled=True
    ).astype(jnp.float32)


def local_cut(full_array, tp_rank, size_local):
    return lax.dynamic_slice_in_dim(
        full_array, tp_rank * size_local, size_local, full_array.ndim - 1
    )


def local_put(local_array, tp_rank, full_size):
    shape_full = local_array.shape[:-1] + (full_size,)
    return lax.dynamic_update_slice_in_dim(
        jnp.zeros(shape_full, jnp.float32),
        local_array,
        tp_rank * local_array.shape[-1],
        local_array.ndim - 1,
    )


BAND = 384


def wide_table(rel_table):
    before = jnp.broadcast_to(rel_table[:1], (LEFT, HEAD))
    after = jnp.broadcast_to(rel_table[-1:], (BAND - LEFT - rel_table.shape[0], HEAD))
    return jnp.concatenate([before, rel_table, after], axis=0)


def dot_t(left, right):
    return lax.dot_general(left, right, (((1,), (1,)), ((), ())), preferred_element_type=jnp.float32)


def dot_n(left, right):
    return lax.dot_general(left, right, (((1,), (0,)), ((), ())), preferred_element_type=jnp.float32)


def scaled_scores(query_block, keys, table, place, rows_at, reach):
    rows = query_block.shape[0]
    key_count = keys.shape[0]
    near = dot_t(query_block, table)
    left, right = near[:, :1], near[:, BAND - 1 :]
    row = lax.broadcasted_iota(jnp.int32, (rows, key_count), 0)
    col = lax.broadcasted_iota(jnp.int32, (rows, key_count), 1)
    place[:, 128 : 128 + key_count] = dot_t(query_block, keys) + jnp.where(
        col < row + rows_at, left, right
    )
    rolled = pltpu.roll(near, 0, 1, stride=1, stride_axis=0)
    apart = band_distance(rows)
    band = jnp.where(apart <= -LEFT, left, jnp.where(apart >= reach, right, rolled))
    window = pl.ds(pl.multiple_of(rows_at, 128), BAND)
    place[:, window] += band - jnp.where(apart < 0, left, right)
    return place[:, 128 : 128 + key_count]


def band_distance(rows):
    row = lax.broadcasted_iota(jnp.int32, (rows, BAND), 0)
    col = lax.broadcasted_iota(jnp.int32, (rows, BAND), 1)
    return col - 128 - row


def attend_kernel(reach, start_ref, query_ref, key_ref, value_ref, table_ref, mixed_ref, total_ref, place):
    rows = query_ref.shape[1]
    rows_at = start_ref[0] + pl.program_id(2) * rows
    table = table_ref[...]
    for half in range(query_ref.shape[2] // HEAD):
        lanes = slice(half * HEAD, (half + 1) * HEAD)
        query_block = query_ref[0, :, lanes] * jnp.bfloat16(1.0 / math.sqrt(HEAD))
        scores = scaled_scores(query_block, key_ref[0, :, lanes], table, place, rows_at, reach)
        top = jnp.max(scores, axis=-1, keepdims=True)
        powers = jnp.exp(scores - top)
        row_sum = jnp.sum(powers, axis=-1, keepdims=True)
        probs = (powers * (1.0 / row_sum)).astype(jnp.bfloat16)
        mixed_ref[0, :, lanes] = dot_n(probs, value_ref[0, :, lanes]).astype(jnp.bfloat16)
        total_ref[0, :, lanes] = jnp.broadcast_to(top + jnp.log(row_sum), (rows, HEAD))


def attend_back_kernel(
    reach, start_ref, query_ref, key_ref, value_ref, table_ref, total_ref, grad_ref,
    query_grad_ref, key_grad_ref, value_grad_ref, table_grad_ref, place, key_sum, value_sum,
):
    rows = query_ref.shape[1]
    key_count = key_ref.shape[1]
    block = pl.program_id(2)
    rows_at = start_ref[0] + block * rows
    table = table_ref[...]
    scale = jnp.bfloat16(1.0 / math.sqrt(HEAD))

    @pl.when(block == 0)
    def _():
        key_sum[...] = jnp.zeros_like(key_sum)
        value_sum[...] = jnp.zeros_like(value_sum)

    @pl.when((block == 0) & (pl.program_id(0) == 0) & (pl.program_id(1) == 0))
    def _():
        table_grad_ref[...] = jnp.zeros_like(table_grad_ref)

    for half in range(query_ref.shape[2] // HEAD):
        lanes = slice(half * HEAD, (half + 1) * HEAD)
        query_block = query_ref[0, :, lanes] * scale
        keys = key_ref[0, :, lanes]
        grad_block = grad_ref[0, :, lanes]
        scores = scaled_scores(query_block, keys, table, place, rows_at, reach)
        probs = jnp.exp(scores - total_ref[0, :, half * HEAD : half * HEAD + 1])
        grad_probs = dot_t(grad_block, value_ref[0, :, lanes])
        row_dot = jnp.sum(probs * grad_probs, axis=-1, keepdims=True)
        grad_scores = (probs * (grad_probs - row_dot)).astype(jnp.bfloat16)
        value_sum[lanes, :] += dot_n(grad_block.T, probs.astype(jnp.bfloat16))
        key_sum[lanes, :] += dot_n(query_block.T, grad_scores)
        wide = grad_scores.astype(jnp.float32)
        place[:, 128 : 128 + key_count] = wide
        apart_all = (
            lax.broadcasted_iota(jnp.int32, wide.shape, 1)
            - lax.broadcasted_iota(jnp.int32, wide.shape, 0)
            - rows_at
        )
        far_left = jnp.sum(jnp.where(apart_all <= -LEFT, wide, 0.0), axis=-1, keepdims=True)
        far_right = jnp.sum(jnp.where(apart_all >= reach, wide, 0.0), axis=-1, keepdims=True)
        window = place[:, pl.ds(pl.multiple_of(rows_at, 128), BAND)]
        window_col = lax.broadcasted_iota(jnp.int32, window.shape, 1) + rows_at - 128
        apart = band_distance(rows)
        inside = (apart > -LEFT) & (apart < reach) & (window_col >= 0) & (window_col < key_count)
        turned = jnp.where(inside, window, 0.0)
        row = lax.broadcasted_iota(jnp.int32, turned.shape, 0)
        for bit in range((rows - 1).bit_length()):
            moved = pltpu.roll(turned, BAND - (1 << bit), 1)
            turned = jnp.where(((row >> bit) & 1) == 1, moved, turned)
        lane = lax.broadcasted_iota(jnp.int32, turned.shape, 1)
        by_row = jnp.where(lane == LEFT, far_left, jnp.where(lane == 2 * LEFT + reach, far_right, turned))
        coarse = by_row.astype(jnp.bfloat16)
        fine = (by_row - coarse.astype(jnp.float32)).astype(jnp.bfloat16)
        query_grad = dot_n(grad_scores, keys) + dot_n(coarse, table) + dot_n(fine, table)
        query_grad_ref[0, :, lanes] = (query_grad * (1.0 / math.sqrt(HEAD))).astype(jnp.bfloat16)
        query_turned = query_block.T
        table_grad_ref[...] += dot_n(query_turned, coarse) + dot_n(query_turned, fine)

    @pl.when(block == pl.num_programs(2) - 1)
    def _():
        key_grad_ref[0] = key_sum[...].T.astype(jnp.bfloat16)
        value_grad_ref[0] = value_sum[...].T.astype(jnp.bfloat16)


def attend_specs(queries, keys):
    slots, rows, width = queries.shape
    lanes = 2 * HEAD
    block = 128
    grid = (slots, width // lanes, rows // block)
    by_query = pl.BlockSpec((1, block, lanes), lambda s, p, b, *_: (s, b, p))
    by_key = pl.BlockSpec((1, keys.shape[1], lanes), lambda s, p, b, *_: (s, 0, p))
    table = pl.BlockSpec((BAND, HEAD), lambda s, p, b, *_: (0, 0))
    place = pltpu.VMEM((block, keys.shape[1] + 256), jnp.float32)
    flops = slots * rows * keys.shape[1] * width * 4
    return grid, by_query, by_key, table, place, flops


def attend(queries, keys, values, table, reach, query_start):
    grid, by_query, by_key, by_table, place, flops = attend_specs(queries, keys)
    return pl.pallas_call(
        functools.partial(attend_kernel, reach),
        out_shape=(
            jax.ShapeDtypeStruct(queries.shape, jnp.bfloat16),
            jax.ShapeDtypeStruct(queries.shape, jnp.float32),
        ),
        grid_spec=pltpu.PrefetchScalarGridSpec(
            num_scalar_prefetch=1,
            grid=grid,
            in_specs=[by_query, by_key, by_key, by_table],
            out_specs=(by_query, by_query),
            scratch_shapes=[place],
        ),
        cost_estimate=pl.CostEstimate(flops=2 * flops, bytes_accessed=8 << 20, transcendentals=flops >> 8),
        name="attend",
    )(query_start.reshape(1), queries, keys, values, table)


def attend_back(queries, keys, values, table, totals, grad_mixed, reach, query_start):
    grid, by_query, by_key, by_table, place, flops = attend_specs(queries, keys)
    turned = pltpu.VMEM((2 * HEAD, keys.shape[1]), jnp.float32)
    return pl.pallas_call(
        functools.partial(attend_back_kernel, reach),
        out_shape=(
            jax.ShapeDtypeStruct(queries.shape, jnp.bfloat16),
            jax.ShapeDtypeStruct(keys.shape, jnp.bfloat16),
            jax.ShapeDtypeStruct(keys.shape, jnp.bfloat16),
            jax.ShapeDtypeStruct((HEAD, BAND), jnp.float32),
        ),
        grid_spec=pltpu.PrefetchScalarGridSpec(
            num_scalar_prefetch=1,
            grid=grid,
            in_specs=[by_query, by_key, by_key, by_table, by_query, by_query],
            out_specs=(
                by_query,
                by_key,
                by_key,
                pl.BlockSpec((HEAD, BAND), lambda s, p, b, *_: (0, 0)),
            ),
            scratch_shapes=[place, turned, turned],
        ),
        cost_estimate=pl.CostEstimate(flops=5 * flops, bytes_accessed=16 << 20, transcendentals=flops >> 8),
        name="attend_back",
    )(query_start.reshape(1), queries, keys, values, table, totals, grad_mixed)


def ffn_forward(stream, norm_gain, norm_shift, weight_in, bias_in, weight_out, bias_out):
    normed, standard, inverse = norm_forward(stream, norm_gain, norm_shift)
    wide_rows = widen(normed)
    hidden_pre = rows_in(wide_rows, weight_in) + bias_in
    active = jax.nn.silu(hidden_pre).astype(jnp.bfloat16)
    branch = narrow(rows_out(active, weight_out)) + bias_out
    return (stream + 0.5 * branch, (standard, inverse, wide_rows, hidden_pre))


def ffn_backward(grad_stream, saved, norm_gain, weight_in, weight_out):
    standard, inverse, wide_rows, hidden_pre = saved
    grad_branch = (0.5 * grad_stream).astype(jnp.bfloat16)
    out_bias_grad = jnp.sum(grad_branch.astype(jnp.float32), axis=(0, 1))
    wide_grad = widen_grad(grad_branch)
    active = jax.nn.silu(hidden_pre).astype(jnp.bfloat16)
    out_grad = weight_sum(wide_grad, active)
    grad_pre = (rows_in(wide_grad, weight_out) * silu_slope(hidden_pre)).astype(jnp.bfloat16)
    in_bias_grad = jnp.sum(grad_pre.astype(jnp.float32), axis=(0, 1))
    in_grad = weight_sum(wide_rows, grad_pre)
    grad_normed = narrow_grad(rows_out(grad_pre, weight_in))
    grad_normed, in_grad, out_grad = together(grad_normed, in_grad, out_grad)
    grad_in, gain_grad, shift_grad = norm_backward(grad_normed, standard, inverse, norm_gain)
    return (
        grad_stream + grad_in,
        (gain_grad, shift_grad, in_grad, in_bias_grad, out_grad, out_bias_grad),
    )


def attn_forward(stream, norm_gain, norm_shift, weights, biases, rel_table, ctx_rank, late_shard):
    query_w, key_w, value_w, out_w = weights
    query_b, value_b, out_b = biases
    normed, standard, inverse = norm_forward(stream, norm_gain, norm_shift)
    wide_rows = widen(normed)
    queries = (rows_in(wide_rows, query_w) + query_b).astype(jnp.bfloat16)
    keys_local = rows_in(wide_rows, key_w).astype(jnp.bfloat16)
    values_local = (rows_in(wide_rows, value_w) + value_b).astype(jnp.bfloat16)
    keys_all, values_all = (
        lax.all_gather(keys_local, "ctx", axis=1, tiled=True),
        lax.all_gather(values_local, "ctx", axis=1, tiled=True),
    )
    keys_all, values_all, late_shard = together(keys_all, values_all, late_shard)
    late = gather_rows(late_shard)
    reach = rel_table.shape[0] - 1 - LEFT
    mixed_token_rows, log_total = attend(
        queries, keys_all, values_all, wide_table(rel_table), reach, ctx_rank * queries.shape[1]
    )
    mixed_token_rows, late = together(mixed_token_rows, late)
    branch = narrow(rows_out(mixed_token_rows, out_w)) + out_b
    return (
        stream + branch,
        (standard, inverse, wide_rows, queries, keys_all, values_all, mixed_token_rows, log_total),
        late,
    )


def attn_backward(grad_stream, saved, norm_gain, weights, rel_table, ctx_rank, inner_grads):
    query_w, key_w, value_w, out_w = weights
    standard, inverse, wide_rows, queries, keys_all, values_all, mixed_token_rows, log_total = saved
    grad_branch = grad_stream.astype(jnp.bfloat16)
    out_bias_grad = jnp.sum(grad_branch.astype(jnp.float32), axis=(0, 1))
    inner = jnp.concatenate([grad.astype(jnp.bfloat16) for grad in inner_grads], axis=1)
    wide_grad, inner = together(widen_grad(grad_branch), inner)
    inner = lax.psum_scatter(inner, ("fsdp", "ctx"), scatter_dimension=0, tiled=True)
    grad_mixed = rows_in(wide_grad, out_w).astype(jnp.bfloat16)
    reach = rel_table.shape[0] - 1 - LEFT
    query_low, key_terms, value_terms, table_turned = attend_back(
        queries,
        keys_all,
        values_all,
        wide_table(rel_table),
        log_total,
        grad_mixed,
        reach,
        ctx_rank * queries.shape[1],
    )
    query_low, key_terms, value_terms, inner = together(query_low, key_terms, value_terms, inner)
    out_grad = weight_sum(wide_grad, mixed_token_rows)
    inner_parts = split_columns(inner, inner_grads)
    table_grad = table_turned[:, LEFT : LEFT + rel_table.shape[0]].T
    key_grad, value_grad = (
        lax.psum_scatter(key_terms, "ctx", scatter_dimension=1, tiled=True),
        lax.psum_scatter(value_terms, "ctx", scatter_dimension=1, tiled=True),
    )
    key_low = key_grad.astype(jnp.bfloat16)
    value_low = value_grad.astype(jnp.bfloat16)
    query_bias_grad = jnp.sum(query_low.astype(jnp.float32), axis=(0, 1))
    value_bias_grad = jnp.sum(value_low.astype(jnp.float32), axis=(0, 1))
    query_w_grad = weight_sum(wide_rows, query_low)
    key_w_grad = weight_sum(wide_rows, key_low)
    value_w_grad = weight_sum(wide_rows, value_low)
    grad_normed = narrow_grad(
        rows_out(query_low, query_w) + rows_out(key_low, key_w) + rows_out(value_low, value_w)
    )
    grad_normed, out_grad, query_w_grad, key_w_grad, value_w_grad = together(
        grad_normed, out_grad, query_w_grad, key_w_grad, value_w_grad
    )
    grad_in, gain_grad, shift_grad = norm_backward(grad_normed, standard, inverse, norm_gain)
    return (
        grad_stream + grad_in,
        (
            gain_grad,
            shift_grad,
            query_w_grad,
            query_bias_grad,
            key_w_grad,
            value_w_grad,
            value_bias_grad,
            out_grad,
            out_bias_grad,
            table_grad,
        ),
        inner_parts,
    )


def conv_forward(stream, norm_gain, norm_shift, weights, depth_local, inner_gain, inner_offset):
    value_w, gate_w, out_w = weights
    normed, standard, inverse = norm_forward(stream, norm_gain, norm_shift)
    wide_rows = widen(normed)
    part_value = rows_in(wide_rows, value_w)
    part_gate = rows_in(wide_rows, gate_w)
    gated_rows = (part_value * jax.nn.sigmoid(part_gate)).astype(jnp.bfloat16)
    row_count = gated_rows.shape[1]
    reach_rows = depth_local.shape[0] - 1
    halo_rows = from_behind(gated_rows[:, row_count - reach_rows :, :], "ctx", 1)
    padded = jnp.concatenate([halo_rows, gated_rows], axis=1)
    padded_float = padded.astype(jnp.float32)
    convolved = depth_local[0] * padded_float[:, 0:row_count, :]
    for tap_index in range(1, depth_local.shape[0]):
        convolved = (
            convolved
            + depth_local[tap_index] * padded_float[:, tap_index : tap_index + row_count, :]
        )
    row_sums = lax.psum(
        (jnp.sum(convolved, axis=-1), jnp.sum(convolved * convolved, axis=-1)), "tp"
    )
    row_mean = (row_sums[0] / D)[..., None]
    row_var = (row_sums[1] / D)[..., None] - row_mean * row_mean
    inner_inverse = lax.rsqrt(row_var + epsilon)
    inner_standard = (convolved - row_mean) * inner_inverse
    inner_pre = inner_standard * inner_gain + inner_offset
    active = jax.nn.silu(inner_pre).astype(jnp.bfloat16)
    branch = narrow(rows_out(active, out_w))
    return (
        stream + branch,
        (
            standard,
            inverse,
            wide_rows,
            part_value,
            part_gate,
            padded,
            inner_standard,
            inner_inverse,
            inner_pre,
        ),
    )


def taps_back_kernel(depth_ref, grad_ref, padded_ref, gated_ref, depth_grad_ref, wide):
    taps = depth_ref.shape[0]
    rows, width = gated_ref.shape[1:]
    step = 64

    @pl.when(pl.program_id(0) == 0)
    def _():
        depth_grad_ref[...] = jnp.zeros_like(depth_grad_ref)

    wide[: padded_ref.shape[1], :] = padded_ref[0].astype(jnp.float32)
    for lane in range(0, width, 128):
        lanes = slice(lane, lane + 128)
        for start in range(0, rows, step):
            own = grad_ref[0, start : start + step, lanes]
            total = jnp.zeros((step, 128), jnp.float32)
            for tap in range(taps):
                first = start + taps - 1 - tap
                total += depth_ref[tap : tap + 1, lanes] * grad_ref[0, first : first + step, lanes]
                product = own * wide[start + tap : start + tap + step, lanes]
                depth_grad_ref[8 * tap : 8 * tap + 8, lanes] += jnp.sum(
                    product.reshape(step // 8, 8, 128), axis=0
                )
            gated_ref[0, start : start + step, lanes] = total


def taps_back(grad_conv, ahead, padded, depth_local):
    slots, rows, width = grad_conv.shape
    taps = depth_local.shape[0]
    spare = -(rows + taps - 1) % 8
    reach = jnp.concatenate(
        [grad_conv, ahead, jnp.zeros((slots, spare, width), jnp.float32)], axis=1
    )
    held = jnp.pad(padded, ((0, 0), (0, spare), (0, 0)))
    by_slot = lambda count: pl.BlockSpec((1, count, width), lambda s: (s, 0, 0))
    gated, depth_sums = pl.pallas_call(
        taps_back_kernel,
        out_shape=(
            jax.ShapeDtypeStruct((slots, rows, width), jnp.float32),
            jax.ShapeDtypeStruct((8 * taps, width), jnp.float32),
        ),
        grid=(slots,),
        in_specs=[
            pl.BlockSpec((taps, width), lambda s: (0, 0)),
            by_slot(reach.shape[1]),
            by_slot(held.shape[1]),
        ],
        out_specs=(by_slot(rows), pl.BlockSpec((8 * taps, width), lambda s: (0, 0))),
        scratch_shapes=[pltpu.VMEM((held.shape[1], width), jnp.float32)],
        cost_estimate=pl.CostEstimate(
            flops=4 * taps * slots * rows * width, bytes_accessed=4 << 20, transcendentals=0
        ),
        name="taps_back",
    )(depth_local, reach, held)
    return gated, jnp.sum(depth_sums.reshape(taps, 8, width), axis=1)


def conv_backward(grad_stream, saved, norm_gain, weights, depth_local, inner_gain):
    value_w, gate_w, out_w = weights
    (
        standard,
        inverse,
        wide_rows,
        part_value,
        part_gate,
        padded,
        inner_standard,
        inner_inverse,
        inner_pre,
    ) = saved
    grad_branch = grad_stream.astype(jnp.bfloat16)
    wide_grad = widen_grad(grad_branch)
    active = jax.nn.silu(inner_pre).astype(jnp.bfloat16)
    out_grad = weight_sum(wide_grad, active)
    grad_inner = rows_in(wide_grad, out_w) * silu_slope(inner_pre)
    inner_gain_grad = jnp.sum(grad_inner * inner_standard, axis=(0, 1))
    inner_shift_grad = jnp.sum(grad_inner, axis=(0, 1))
    grad_standard = grad_inner * inner_gain
    row_sums = lax.psum(
        (jnp.sum(grad_standard, axis=-1), jnp.sum(grad_standard * inner_standard, axis=-1)), "tp"
    )
    grad_conv = inner_inverse * (
        grad_standard - (row_sums[0] / D)[..., None] - inner_standard * (row_sums[1] / D)[..., None]
    )
    row_count = grad_conv.shape[1]
    tap_count = depth_local.shape[0]
    reach_rows = tap_count - 1
    ahead = from_behind(grad_conv[:, :reach_rows, :].astype(jnp.bfloat16), "ctx", -1)
    grad_gated, depth_grad = taps_back(grad_conv, ahead.astype(jnp.float32), padded, depth_local)
    gate_sig = jax.nn.sigmoid(part_gate)
    grad_value = (grad_gated * gate_sig).astype(jnp.bfloat16)
    grad_gate = (grad_gated * part_value * gate_sig * (1.0 - gate_sig)).astype(jnp.bfloat16)
    value_w_grad = weight_sum(wide_rows, grad_value)
    gate_w_grad = weight_sum(wide_rows, grad_gate)
    grad_normed = narrow_grad(rows_out(grad_value, value_w) + rows_out(grad_gate, gate_w))
    grad_normed, out_grad, value_w_grad, gate_w_grad = together(
        grad_normed, out_grad, value_w_grad, gate_w_grad
    )
    grad_in, gain_grad, shift_grad = norm_backward(grad_normed, standard, inverse, norm_gain)
    return (
        grad_stream + grad_in,
        (
            gain_grad,
            shift_grad,
            value_w_grad,
            gate_w_grad,
            depth_grad,
            inner_gain_grad,
            inner_shift_grad,
            out_grad,
        ),
    )


def gather_rows(shard):
    return lax.all_gather(shard, ("fsdp", "ctx"), axis=0, tiled=True)


def scatter_sum(*grads):
    joined = jnp.concatenate([grad.astype(jnp.bfloat16) for grad in grads], axis=1)
    part = lax.psum_scatter(joined, ("fsdp", "ctx"), scatter_dimension=0, tiled=True)
    return split_columns(part, grads)


def split_columns(part, grads):
    pieces = []
    start = 0
    for grad in grads:
        pieces.append(part[:, start : start + grad.shape[1]].astype(jnp.float32))
        start += grad.shape[1]
    return tuple(pieces)


def scatter_sum_all(grads, whole_parts, split_parts, own_sum):
    rows = grads[0].shape[0]
    flat = jnp.concatenate([part.reshape(-1) for part in whole_parts + split_parts])
    columns = -(-flat.shape[0] // rows)
    flat = jnp.pad(flat, (0, rows * columns - flat.shape[0])).reshape(rows, columns)
    parts = scatter_sum(*grads, jnp.pad(flat, ((0, 0), (0, -columns % 128))))
    small = parts[-1][:, :columns].reshape(-1)
    held = small.shape[0]
    sent = jnp.concatenate([small, own_sum.reshape(1)])
    sent = jnp.pad(sent, (0, -sent.shape[0] % 128)).reshape(1, -1, 128)
    tp_count = lax.axis_size("tp")
    every = lax.all_gather(sent, ("fsdp", "ctx", "tp"), axis=0, tiled=True)
    every = every.reshape(-1, tp_count, sent.size)
    by_tp = every[:, :, :held].transpose(1, 0, 2).reshape(tp_count, -1)
    total = jnp.sum(by_tp, axis=0)
    spread = by_tp
    whole = []
    start = 0
    for part in whole_parts:
        whole.append(total[start : start + part.size].reshape(part.shape))
        start += part.size
    pieces = []
    for part in split_parts:
        piece = spread[:, start : start + part.size]
        if part.ndim == 1:
            pieces.append(piece.reshape(-1))
        else:
            piece = piece.reshape((tp_count,) + part.shape)
            pieces.append(piece.transpose(1, 0, 2).reshape(part.shape[0], -1))
        start += part.size
    w, p = whole + [jnp.sum(every[:, :, held])], pieces
    return parts[:-1], (
        w[0], w[1], p[0], w[2], w[3], w[4], p[1], p[2], w[5], w[6], w[7], w[8],
        p[3], p[4], p[5], w[9], w[10], p[6], w[11], w[12], w[13], w[14],
    )


def body(
    inputs,
    teacher,
    clips_dev,
    ffn1_gain,
    ffn1_shift,
    ffn1_in,
    ffn1_in_bias,
    ffn1_out,
    ffn1_out_bias,
    attn_gain,
    attn_shift,
    query_weight,
    query_bias,
    key_weight,
    value_weight,
    value_bias,
    attn_out_weight,
    attn_out_bias,
    rel_table,
    conv_gain,
    conv_shift,
    conv_value_weight,
    conv_gate_weight,
    conv_depth,
    conv_inner_gain,
    conv_inner_shift,
    conv_out_weight,
    ffn2_gain,
    ffn2_shift,
    ffn2_in,
    ffn2_in_bias,
    ffn2_out,
    ffn2_out_bias,
    final_gain,
    final_shift,
):
    ffn1_in_all = gather_rows(ffn1_in)
    width = query_weight.shape[1]
    early = gather_rows(
        jnp.concatenate(
            [ffn1_out, query_weight, key_weight, value_weight, attn_out_weight], axis=1
        )
    )
    ffn1_out_all = early[:, : ffn1_out.shape[1]]
    attn_all = early[:, ffn1_out.shape[1] :]
    late_shard = jnp.concatenate(
        [ffn2_in, ffn2_out, conv_value_weight, conv_gate_weight, conv_out_weight], axis=1
    )
    attn_weights = (
        attn_all[:, :width],
        attn_all[:, width : 2 * width],
        attn_all[:, 2 * width : 3 * width],
        attn_all[:, 3 * width :],
    )
    tp_rank = lax.axis_index("tp")
    ctx_rank = lax.axis_index("ctx")
    hidden_local = ffn1_in.shape[1]
    width_local = width
    ffn1_bias_local = local_cut(ffn1_in_bias, tp_rank, hidden_local)
    ffn2_bias_local = local_cut(ffn2_in_bias, tp_rank, hidden_local)
    query_bias_local = local_cut(query_bias, tp_rank, width_local)
    value_bias_local = local_cut(value_bias, tp_rank, width_local)
    depth_local = local_cut(conv_depth, tp_rank, width_local)
    inner_gain_local = local_cut(conv_inner_gain, tp_rank, width_local)
    inner_shift_local = local_cut(conv_inner_shift, tp_rank, width_local)
    stream_zero = inputs.astype(jnp.float32)
    stream_one, saved_one = ffn_forward(
        stream_zero, ffn1_gain, ffn1_shift, ffn1_in_all, ffn1_bias_local, ffn1_out_all, ffn1_out_bias
    )
    stream_two, saved_two, late = attn_forward(
        stream_one,
        attn_gain,
        attn_shift,
        attn_weights,
        (query_bias_local, value_bias_local, attn_out_bias),
        rel_table,
        ctx_rank,
        late_shard,
    )
    ffn2_in_all = late[:, :hidden_local]
    ffn2_out_all = late[:, hidden_local : 2 * hidden_local]
    conv_all = late[:, 2 * hidden_local :]
    conv_weights = (
        conv_all[:, :width],
        conv_all[:, width : 2 * width],
        conv_all[:, 2 * width :],
    )
    stream_three, saved_three = conv_forward(
        stream_two,
        conv_gain,
        conv_shift,
        conv_weights,
        depth_local,
        inner_gain_local,
        inner_shift_local,
    )
    stream_four, saved_four = ffn_forward(
        stream_three,
        ffn2_gain,
        ffn2_shift,
        ffn2_in_all,
        ffn2_bias_local,
        ffn2_out_all,
        ffn2_out_bias,
    )
    final_out, final_standard, final_inverse = norm_forward(stream_four, final_gain, final_shift)
    live_slots = (
        jnp.arange(final_out.shape[0], dtype=jnp.int32) < clips_dev[lax.axis_index("fsdp")]
    ).astype(jnp.float32)
    misfit = (final_out - teacher.astype(jnp.float32)) * live_slots[:, None, None]
    sse_local = jnp.sum(misfit * misfit)
    gradient_fourth, final_gain_grad, final_shift_grad = norm_backward(
        2.0 * misfit, final_standard, final_inverse, final_gain
    )
    grad_three, ffn2_grads = ffn_backward(
        gradient_fourth, saved_four, ffn2_gain, ffn2_in_all, ffn2_out_all
    )
    grad_two, conv_grads = conv_backward(
        grad_three,
        saved_three,
        conv_gain,
        conv_weights,
        depth_local,
        inner_gain_local,
    )
    grad_one, attn_grads, inner_parts = attn_backward(
        grad_two,
        saved_two,
        attn_gain,
        attn_weights,
        rel_table,
        ctx_rank,
        (ffn2_grads[2], ffn2_grads[4], conv_grads[2], conv_grads[3], conv_grads[7]),
    )
    grad_zero, ffn1_grads = ffn_backward(
        grad_one, saved_one, ffn1_gain, ffn1_in_all, ffn1_out_all
    )
    attn_parts = scatter_sum(attn_grads[2], attn_grads[4], attn_grads[5], attn_grads[7])
    ffn1_parts, shared = scatter_sum_all(
        (ffn1_grads[2], ffn1_grads[4]),
        (
            ffn1_grads[0],
            ffn1_grads[1],
            ffn1_grads[5],
            attn_grads[0],
            attn_grads[1],
            attn_grads[8],
            attn_grads[9],
            conv_grads[0],
            conv_grads[1],
            ffn2_grads[0],
            ffn2_grads[1],
            ffn2_grads[5],
            final_gain_grad,
            final_shift_grad,
        ),
        (
            ffn1_grads[3],
            attn_grads[3],
            attn_grads[6],
            conv_grads[4],
            conv_grads[5],
            conv_grads[6],
            ffn2_grads[3],
        ),
        sse_local,
    )
    weight_parts = ffn1_parts + attn_parts + inner_parts[2:] + inner_parts[:2]
    token_count = (jnp.sum(clips_dev) * SEQ).astype(jnp.float32)
    loss = shared[21] / token_count
    return (
        final_out.astype(jnp.bfloat16),
        loss,
        grad_zero,
        shared[0],
        shared[1],
        weight_parts[0],
        shared[2],
        weight_parts[1],
        shared[3],
        shared[4],
        shared[5],
        weight_parts[2],
        shared[6],
        weight_parts[3],
        weight_parts[4],
        shared[7],
        weight_parts[5],
        shared[8],
        shared[9],
        shared[10],
        shared[11],
        weight_parts[6],
        weight_parts[7],
        shared[12],
        shared[13],
        shared[14],
        weight_parts[8],
        shared[15],
        shared[16],
        weight_parts[9],
        shared[17],
        weight_parts[10],
        shared[18],
        shared[19],
        shared[20],
    )


def solution(mesh):
    in_specs = (
        P("fsdp", ("ctx", "tp"), None),
        P("fsdp", ("ctx", "tp"), None),
        P(),
        P(),
        P(),
        P(("fsdp", "ctx"), "tp"),
        P(),
        P(("fsdp", "ctx"), "tp"),
        P(),
        P(),
        P(),
        P(("fsdp", "ctx"), "tp"),
        P(),
        P(("fsdp", "ctx"), "tp"),
        P(("fsdp", "ctx"), "tp"),
        P(),
        P(("fsdp", "ctx"), "tp"),
        P(),
        P(),
        P(),
        P(),
        P(("fsdp", "ctx"), "tp"),
        P(("fsdp", "ctx"), "tp"),
        P(),
        P(),
        P(),
        P(("fsdp", "ctx"), "tp"),
        P(),
        P(),
        P(("fsdp", "ctx"), "tp"),
        P(),
        P(("fsdp", "ctx"), "tp"),
        P(),
        P(),
        P(),
    )
    out_specs = (
        P("fsdp", ("ctx", "tp"), None),
        P(),
        P("fsdp", ("ctx", "tp"), None),
        P(),
        P(),
        P(("fsdp", "ctx"), "tp"),
        P(),
        P(("fsdp", "ctx"), "tp"),
        P(),
        P(),
        P(),
        P(("fsdp", "ctx"), "tp"),
        P(),
        P(("fsdp", "ctx"), "tp"),
        P(("fsdp", "ctx"), "tp"),
        P(),
        P(("fsdp", "ctx"), "tp"),
        P(),
        P(),
        P(),
        P(),
        P(("fsdp", "ctx"), "tp"),
        P(("fsdp", "ctx"), "tp"),
        P(),
        P(),
        P(),
        P(("fsdp", "ctx"), "tp"),
        P(),
        P(),
        P(("fsdp", "ctx"), "tp"),
        P(),
        P(("fsdp", "ctx"), "tp"),
        P(),
        P(),
        P(),
    )
    return jax.shard_map(body, mesh=mesh, in_specs=in_specs, out_specs=out_specs, check_vma=False)
```

```python
import functools
import math

import jax
import jax.numpy as jnp
from jax import lax
from jax.experimental import pallas as pl
from jax.experimental.pallas import tpu as pltpu
from jax.sharding import PartitionSpec as P

D = 1024
LEFT = 64
HEAD = 64
SEQ = 1536


epsilon = 1e-05


def from_behind(shard, axis, by):
    devices = lax.axis_size(axis)
    pairs = [(i, i + by) for i in range(devices) if 0 <= i + by < devices]
    return lax.ppermute(shard, axis, pairs)


def norm_forward(stream, norm_gain, norm_shift):
    centred = stream - jnp.mean(stream, axis=-1, keepdims=True)
    inverse = lax.rsqrt(jnp.mean(centred * centred, axis=-1, keepdims=True) + epsilon)
    standard = centred * inverse
    return (standard * norm_gain + norm_shift, standard, inverse)


def norm_backward(grad_out, standard, inverse, norm_gain):
    grad_standard = grad_out * norm_gain
    mean_first = jnp.mean(grad_standard, axis=-1, keepdims=True)
    mean_second = jnp.mean(grad_standard * standard, axis=-1, keepdims=True)
    grad_in = inverse * (grad_standard - mean_first - standard * mean_second)
    return (grad_in, jnp.sum(grad_out * standard, axis=(0, 1)), jnp.sum(grad_out, axis=(0, 1)))


def silu_slope(hidden_pre):
    gate_sig = jax.nn.sigmoid(hidden_pre)
    return gate_sig * (1.0 + hidden_pre * (1.0 - gate_sig))


def rows_in(left_reach, right_reach):
    return jnp.einsum("zub,bx->zux", left_reach, right_reach, preferred_element_type=jnp.float32)


def rows_out(left_reach, right_reach):
    return jnp.einsum("anp,op->ano", left_reach, right_reach, preferred_element_type=jnp.float32)


def weight_sum(left_reach, right_reach):
    return jnp.einsum("zbt,zbm->tm", left_reach, right_reach, preferred_element_type=jnp.float32)


def together(*values):
    return lax.optimization_barrier(values)


def widen(normed):
    return lax.all_gather(normed.astype(jnp.bfloat16), "tp", axis=1, tiled=True)


def narrow(partial_rows):
    return lax.psum_scatter(
        partial_rows.astype(jnp.bfloat16), "tp", scatter_dimension=1, tiled=True
    ).astype(jnp.float32)


def widen_grad(grad_branch):
    return lax.all_gather(grad_branch, "tp", axis=1, tiled=True)


def narrow_grad(partial_rows):
    return lax.psum_scatter(
        partial_rows.astype(jnp.bfloat16), "tp", scatter_dimension=1, tiled=True
    ).astype(jnp.float32)


def local_cut(full_array, tp_rank, size_local):
    return lax.dynamic_slice_in_dim(
        full_array, tp_rank * size_local, size_local, full_array.ndim - 1
    )


def local_put(local_array, tp_rank, full_size):
    shape_full = local_array.shape[:-1] + (full_size,)
    return lax.dynamic_update_slice_in_dim(
        jnp.zeros(shape_full, jnp.float32),
        local_array,
        tp_rank * local_array.shape[-1],
        local_array.ndim - 1,
    )


BAND = 384


def wide_table(rel_table):
    before = jnp.broadcast_to(rel_table[:1], (LEFT, HEAD))
    after = jnp.broadcast_to(rel_table[-1:], (BAND - LEFT - rel_table.shape[0], HEAD))
    return jnp.concatenate([before, rel_table, after], axis=0)


def dot_t(left, right):
    return lax.dot_general(left, right, (((1,), (1,)), ((), ())), preferred_element_type=jnp.float32)


def dot_n(left, right):
    return lax.dot_general(left, right, (((1,), (0,)), ((), ())), preferred_element_type=jnp.float32)


def scaled_scores(query_block, keys, table, place, rows_at, reach):
    rows = query_block.shape[0]
    key_count = keys.shape[0]
    near = dot_t(query_block, table)
    left, right = near[:, :1], near[:, BAND - 1 :]
    row = lax.broadcasted_iota(jnp.int32, (rows, key_count), 0)
    col = lax.broadcasted_iota(jnp.int32, (rows, key_count), 1)
    place[:, 128 : 128 + key_count] = dot_t(query_block, keys) + jnp.where(
        col < row + rows_at, left, right
    )
    rolled = pltpu.roll(near, 0, 1, stride=1, stride_axis=0)
    apart = band_distance(rows)
    band = jnp.where(apart <= -LEFT, left, jnp.where(apart >= reach, right, rolled))
    window = pl.ds(pl.multiple_of(rows_at, 128), BAND)
    place[:, window] += band - jnp.where(apart < 0, left, right)
    return place[:, 128 : 128 + key_count]


def band_distance(rows):
    row = lax.broadcasted_iota(jnp.int32, (rows, BAND), 0)
    col = lax.broadcasted_iota(jnp.int32, (rows, BAND), 1)
    return col - 128 - row


def attend_kernel(reach, start_ref, query_ref, key_ref, value_ref, table_ref, mixed_ref, total_ref, place):
    rows = query_ref.shape[1]
    rows_at = start_ref[0] + pl.program_id(2) * rows
    table = table_ref[...]
    for half in range(query_ref.shape[2] // HEAD):
        lanes = slice(half * HEAD, (half + 1) * HEAD)
        query_block = query_ref[0, :, lanes] * jnp.bfloat16(1.0 / math.sqrt(HEAD))
        scores = scaled_scores(query_block, key_ref[0, :, lanes], table, place, rows_at, reach)
        top = jnp.max(scores, axis=-1, keepdims=True)
        powers = jnp.exp(scores - top)
        row_sum = jnp.sum(powers, axis=-1, keepdims=True)
        probs = (powers * (1.0 / row_sum)).astype(jnp.bfloat16)
        mixed_ref[0, :, lanes] = dot_n(probs, value_ref[0, :, lanes]).astype(jnp.bfloat16)
        total_ref[0, :, lanes] = jnp.broadcast_to(top + jnp.log(row_sum), (rows, HEAD))


def attend_back_kernel(
    reach, start_ref, query_ref, key_ref, value_ref, table_ref, total_ref, grad_ref, groups_ref,
    query_grad_ref, pair_grad_ref, table_grad_ref, place, key_sum, value_sum,
):
    rows = query_ref.shape[1]
    key_count = key_ref.shape[1]
    block = pl.program_id(2)
    rows_at = start_ref[0] + block * rows
    table = table_ref[...]
    scale = jnp.bfloat16(1.0 / math.sqrt(HEAD))

    @pl.when(block == 0)
    def _():
        key_sum[...] = jnp.zeros_like(key_sum)
        value_sum[...] = jnp.zeros_like(value_sum)

    @pl.when((block == 0) & (pl.program_id(0) == 0) & (pl.program_id(1) == 0))
    def _():
        table_grad_ref[...] = jnp.zeros_like(table_grad_ref)

    for half in range(query_ref.shape[2] // HEAD):
        lanes = slice(half * HEAD, (half + 1) * HEAD)
        query_block = query_ref[0, :, lanes] * scale
        keys = key_ref[0, :, lanes]
        grad_block = grad_ref[0, :, lanes]
        scores = scaled_scores(query_block, keys, table, place, rows_at, reach)
        probs = jnp.exp(scores - total_ref[0, :, half * HEAD : half * HEAD + 1])
        grad_probs = dot_t(grad_block, value_ref[0, :, lanes])
        row_dot = jnp.sum(probs * grad_probs, axis=-1, keepdims=True)
        grad_scores = (probs * (grad_probs - row_dot)).astype(jnp.bfloat16)
        value_sum[lanes, :] += dot_n(grad_block.T, probs.astype(jnp.bfloat16))
        key_sum[lanes, :] += dot_n(query_block.T, grad_scores)
        wide = grad_scores.astype(jnp.float32)
        place[:, 128 : 128 + key_count] = wide
        window = place[:, pl.ds(pl.multiple_of(rows_at, 128), BAND)]
        window_col = lax.broadcasted_iota(jnp.int32, window.shape, 1) + rows_at - 128
        window = jnp.where((window_col >= 0) & (window_col < key_count), window, 0.0)
        apart = band_distance(rows)
        by_group = dot_n(grad_scores, groups_ref[...])
        past = lax.broadcasted_iota(jnp.int32, by_group.shape, 1) * 128 - rows_at
        far_left = jnp.sum(jnp.where(past < -128, by_group, 0.0), axis=-1, keepdims=True)
        far_left += jnp.sum(jnp.where(apart <= -LEFT, window, 0.0), axis=-1, keepdims=True)
        far_right = jnp.sum(jnp.where(past >= BAND - 128, by_group, 0.0), axis=-1, keepdims=True)
        far_right += jnp.sum(jnp.where(apart >= reach, window, 0.0), axis=-1, keepdims=True)
        inside = (apart > -LEFT) & (apart < reach)
        turned = jnp.where(inside, window, 0.0)
        row = lax.broadcasted_iota(jnp.int32, turned.shape, 0)
        for bit in range((rows - 1).bit_length()):
            moved = pltpu.roll(turned, BAND - (1 << bit), 1)
            turned = jnp.where(((row >> bit) & 1) == 1, moved, turned)
        lane = lax.broadcasted_iota(jnp.int32, turned.shape, 1)
        by_row = jnp.where(lane == LEFT, far_left, jnp.where(lane == 2 * LEFT + reach, far_right, turned))
        coarse = by_row.astype(jnp.bfloat16)
        fine = (by_row - coarse.astype(jnp.float32)).astype(jnp.bfloat16)
        query_grad = dot_n(grad_scores, keys) + dot_n(coarse, table) + dot_n(fine, table)
        query_grad_ref[0, :, lanes] = (query_grad * (1.0 / math.sqrt(HEAD))).astype(jnp.bfloat16)
        query_turned = query_block.T
        table_grad_ref[...] += dot_n(query_turned, coarse) + dot_n(query_turned, fine)

    @pl.when(block == pl.num_programs(2) - 1)
    def _():
        pair_grad_ref[0, 0] = key_sum[...].T.astype(jnp.bfloat16)
        pair_grad_ref[1, 0] = value_sum[...].T.astype(jnp.bfloat16)


def attend_specs(queries, keys):
    slots, rows, width = queries.shape
    lanes = 2 * HEAD
    block = 128
    grid = (slots, width // lanes, rows // block)
    by_query = pl.BlockSpec((1, block, lanes), lambda s, p, b, *_: (s, b, p))
    by_key = pl.BlockSpec((1, keys.shape[1], lanes), lambda s, p, b, *_: (s, 0, p))
    by_value = pl.BlockSpec(
        (1, keys.shape[1], lanes), lambda s, p, b, *_: (s, 0, p + width // lanes)
    )
    table = pl.BlockSpec((BAND, HEAD), lambda s, p, b, *_: (0, 0))
    place = pltpu.VMEM((block, keys.shape[1] + 256), jnp.float32)
    flops = slots * rows * keys.shape[1] * width * 4
    return grid, by_query, by_key, by_value, table, place, flops


def attend(queries, pairs, table, reach, query_start):
    grid, by_query, by_key, by_value, by_table, place, flops = attend_specs(queries, pairs)
    return pl.pallas_call(
        functools.partial(attend_kernel, reach),
        out_shape=(
            jax.ShapeDtypeStruct(queries.shape, jnp.bfloat16),
            jax.ShapeDtypeStruct(queries.shape, jnp.float32),
        ),
        grid_spec=pltpu.PrefetchScalarGridSpec(
            num_scalar_prefetch=1,
            grid=grid,
            in_specs=[by_query, by_key, by_value, by_table],
            out_specs=(by_query, by_query),
            scratch_shapes=[place],
        ),
        cost_estimate=pl.CostEstimate(flops=2 * flops, bytes_accessed=8 << 20, transcendentals=flops >> 8),
        name="attend",
    )(query_start.reshape(1), queries, pairs, pairs, table)


def attend_back(queries, pairs, table, totals, grad_mixed, reach, query_start):
    grid, by_query, by_key, by_value, by_table, place, flops = attend_specs(queries, pairs)
    slots, key_count = pairs.shape[:2]
    turned = pltpu.VMEM((2 * HEAD, key_count), jnp.float32)
    group = jnp.arange(key_count, dtype=jnp.int32)[:, None] // 128
    groups = (group == jnp.arange(128, dtype=jnp.int32)[None, :]).astype(jnp.bfloat16)
    return pl.pallas_call(
        functools.partial(attend_back_kernel, reach),
        out_shape=(
            jax.ShapeDtypeStruct(queries.shape, jnp.bfloat16),
            jax.ShapeDtypeStruct((2, slots, key_count, queries.shape[2]), jnp.bfloat16),
            jax.ShapeDtypeStruct((HEAD, BAND), jnp.float32),
        ),
        grid_spec=pltpu.PrefetchScalarGridSpec(
            num_scalar_prefetch=1,
            grid=grid,
            in_specs=[
                by_query,
                by_key,
                by_value,
                by_table,
                by_query,
                by_query,
                pl.BlockSpec((key_count, 128), lambda s, p, b, *_: (0, 0)),
            ],
            out_specs=(
                by_query,
                pl.BlockSpec((2, 1, key_count, 2 * HEAD), lambda s, p, b, *_: (0, s, 0, p)),
                pl.BlockSpec((HEAD, BAND), lambda s, p, b, *_: (0, 0)),
            ),
            scratch_shapes=[place, turned, turned],
        ),
        cost_estimate=pl.CostEstimate(flops=5 * flops, bytes_accessed=16 << 20, transcendentals=flops >> 8),
        name="attend_back",
    )(query_start.reshape(1), queries, pairs, pairs, table, totals, grad_mixed, groups)


def ffn_forward(stream, norm_gain, norm_shift, weight_in, bias_in, weight_out, bias_out):
    normed, standard, inverse = norm_forward(stream, norm_gain, norm_shift)
    wide_rows = widen(normed)
    hidden_pre = rows_in(wide_rows, weight_in) + bias_in
    active = jax.nn.silu(hidden_pre).astype(jnp.bfloat16)
    branch = narrow(rows_out(active, weight_out)) + bias_out
    return (stream + 0.5 * branch, (standard, inverse, wide_rows, hidden_pre))


def ffn_forward_first(
    stream, norm_gain, norm_shift, shard_in, bias_in, shard_out, bias_out, later_shards
):
    normed, standard, inverse = norm_forward(stream, norm_gain, norm_shift)
    normed, shard_in = together(normed.astype(jnp.bfloat16), shard_in)
    wide_rows = widen(normed)
    pieces = [
        gather_rows(shard_in[:, start : start + 256]) for start in range(0, shard_in.shape[1], 256)
    ]
    wide_rows, shard_out, *pieces = together(wide_rows, shard_out, *pieces)
    weight_out = gather_rows(shard_out)
    weight_in = jnp.concatenate(pieces, axis=1)
    hidden_pre = rows_in(wide_rows, weight_in) + bias_in
    active = jax.nn.silu(hidden_pre).astype(jnp.bfloat16)
    partial_rows = rows_out(active, weight_out).astype(jnp.bfloat16)
    partial_rows, *later_shards = together(partial_rows, *later_shards)
    later = [gather_rows(shard) for shard in later_shards]
    summed = lax.psum_scatter(partial_rows, "tp", scatter_dimension=1, tiled=True)
    summed, *later = together(summed, *later)
    branch = summed.astype(jnp.float32) + bias_out
    saved = (standard, inverse, wide_rows, hidden_pre)
    return (stream + 0.5 * branch, saved, weight_in, weight_out, later)


def ffn_backward(grad_stream, saved, norm_gain, weight_in, weight_out):
    standard, inverse, wide_rows, hidden_pre = saved
    grad_branch = (0.5 * grad_stream).astype(jnp.bfloat16)
    out_bias_grad = jnp.sum(grad_branch.astype(jnp.float32), axis=(0, 1))
    wide_grad = widen_grad(grad_branch)
    active = jax.nn.silu(hidden_pre).astype(jnp.bfloat16)
    out_grad = weight_sum(wide_grad, active)
    grad_pre = (rows_in(wide_grad, weight_out) * silu_slope(hidden_pre)).astype(jnp.bfloat16)
    in_bias_grad = jnp.sum(grad_pre.astype(jnp.float32), axis=(0, 1))
    in_grad = weight_sum(wide_rows, grad_pre)
    grad_normed = narrow_grad(rows_out(grad_pre, weight_in))
    grad_normed, in_grad, out_grad = together(grad_normed, in_grad, out_grad)
    grad_in, gain_grad, shift_grad = norm_backward(grad_normed, standard, inverse, norm_gain)
    return (
        grad_stream + grad_in,
        (gain_grad, shift_grad, in_grad, in_bias_grad, out_grad, out_bias_grad),
    )


def attn_forward(stream, norm_gain, norm_shift, weights, biases, rel_table, ctx_rank, late_shard):
    query_w, key_w, value_w, out_w = weights
    query_b, value_b, out_b = biases
    normed, standard, inverse = norm_forward(stream, norm_gain, norm_shift)
    wide_rows = widen(normed)
    queries = (rows_in(wide_rows, query_w) + query_b).astype(jnp.bfloat16)
    pair_b = jnp.concatenate([jnp.zeros_like(value_b), value_b])
    pair_w = jnp.concatenate([key_w, value_w], axis=1)
    pairs = (rows_in(wide_rows, pair_w) + pair_b).astype(jnp.bfloat16)
    pairs_all = lax.all_gather(pairs, "ctx", axis=1, tiled=True)
    pairs_all, late_shard = together(pairs_all, late_shard)
    late = gather_rows(late_shard)
    reach = rel_table.shape[0] - 1 - LEFT
    mixed_token_rows, log_total = attend(
        queries, pairs_all, wide_table(rel_table), reach, ctx_rank * queries.shape[1]
    )
    mixed_token_rows, late = together(mixed_token_rows, late)
    branch = narrow(rows_out(mixed_token_rows, out_w)) + out_b
    return (
        stream + branch,
        (standard, inverse, wide_rows, queries, pairs_all, mixed_token_rows, log_total),
        late,
    )


def attn_backward(grad_stream, saved, norm_gain, weights, rel_table, ctx_rank, inner_grads):
    query_w, key_w, value_w, out_w = weights
    standard, inverse, wide_rows, queries, pairs_all, mixed_token_rows, log_total = saved
    grad_branch = grad_stream.astype(jnp.bfloat16)
    out_bias_grad = jnp.sum(grad_branch.astype(jnp.float32), axis=(0, 1))
    inner = jnp.concatenate([grad.astype(jnp.bfloat16) for grad in inner_grads], axis=1)
    wide_grad, inner = together(widen_grad(grad_branch), inner)
    inner = lax.psum_scatter(inner, ("fsdp", "ctx"), scatter_dimension=0, tiled=True)
    grad_mixed = rows_in(wide_grad, out_w).astype(jnp.bfloat16)
    reach = rel_table.shape[0] - 1 - LEFT
    query_low, pair_terms, table_turned = attend_back(
        queries,
        pairs_all,
        wide_table(rel_table),
        log_total,
        grad_mixed,
        reach,
        ctx_rank * queries.shape[1],
    )
    query_low, pair_terms, inner = together(query_low, pair_terms, inner)
    out_grad = weight_sum(wide_grad, mixed_token_rows)
    inner_parts = split_columns(inner, inner_grads)
    table_grad = table_turned[:, LEFT : LEFT + rel_table.shape[0]].T
    pair_low = lax.psum_scatter(pair_terms, "ctx", scatter_dimension=2, tiled=True)
    key_low, value_low = pair_low[0], pair_low[1]
    query_bias_grad = jnp.sum(query_low.astype(jnp.float32), axis=(0, 1))
    value_bias_grad = jnp.sum(value_low.astype(jnp.float32), axis=(0, 1))
    query_w_grad = weight_sum(wide_rows, query_low)
    key_w_grad = weight_sum(wide_rows, key_low)
    value_w_grad = weight_sum(wide_rows, value_low)
    grad_normed = narrow_grad(
        rows_out(query_low, query_w) + rows_out(key_low, key_w) + rows_out(value_low, value_w)
    )
    grad_normed, out_grad, query_w_grad, key_w_grad, value_w_grad = together(
        grad_normed, out_grad, query_w_grad, key_w_grad, value_w_grad
    )
    grad_in, gain_grad, shift_grad = norm_backward(grad_normed, standard, inverse, norm_gain)
    return (
        grad_stream + grad_in,
        (
            gain_grad,
            shift_grad,
            query_w_grad,
            query_bias_grad,
            key_w_grad,
            value_w_grad,
            value_bias_grad,
            out_grad,
            out_bias_grad,
            table_grad,
        ),
        inner_parts,
    )


def conv_forward(stream, norm_gain, norm_shift, weights, depth_local, inner_gain, inner_offset):
    value_w, gate_w, out_w = weights
    normed, standard, inverse = norm_forward(stream, norm_gain, norm_shift)
    wide_rows = widen(normed)
    part_value = rows_in(wide_rows, value_w)
    part_gate = rows_in(wide_rows, gate_w)
    gated_rows = (part_value * jax.nn.sigmoid(part_gate)).astype(jnp.bfloat16)
    row_count = gated_rows.shape[1]
    reach_rows = depth_local.shape[0] - 1
    halo_rows = from_behind(gated_rows[:, row_count - reach_rows :, :], "ctx", 1)
    padded = jnp.concatenate([halo_rows, gated_rows], axis=1)
    padded_float = padded.astype(jnp.float32)
    convolved = depth_local[0] * padded_float[:, 0:row_count, :]
    for tap_index in range(1, depth_local.shape[0]):
        convolved = (
            convolved
            + depth_local[tap_index] * padded_float[:, tap_index : tap_index + row_count, :]
        )
    row_sums = lax.psum(
        (jnp.sum(convolved, axis=-1), jnp.sum(convolved * convolved, axis=-1)), "tp"
    )
    row_mean = (row_sums[0] / D)[..., None]
    row_var = (row_sums[1] / D)[..., None] - row_mean * row_mean
    inner_inverse = lax.rsqrt(row_var + epsilon)
    inner_standard = (convolved - row_mean) * inner_inverse
    inner_pre = inner_standard * inner_gain + inner_offset
    active = jax.nn.silu(inner_pre).astype(jnp.bfloat16)
    branch = narrow(rows_out(active, out_w))
    return (
        stream + branch,
        (
            standard,
            inverse,
            wide_rows,
            part_value,
            part_gate,
            padded,
            inner_standard,
            inner_inverse,
            inner_pre,
        ),
    )


def taps_back_kernel(depth_ref, grad_ref, padded_ref, gated_ref, depth_grad_ref, wide):
    taps = depth_ref.shape[0]
    rows, width = gated_ref.shape[1:]
    step = 64

    @pl.when(pl.program_id(0) == 0)
    def _():
        depth_grad_ref[...] = jnp.zeros_like(depth_grad_ref)

    wide[: padded_ref.shape[1], :] = padded_ref[0].astype(jnp.float32)
    for lane in range(0, width, 128):
        lanes = slice(lane, lane + 128)
        for start in range(0, rows, step):
            own = grad_ref[0, start : start + step, lanes]
            total = jnp.zeros((step, 128), jnp.float32)
            for tap in range(taps):
                first = start + taps - 1 - tap
                total += depth_ref[tap : tap + 1, lanes] * grad_ref[0, first : first + step, lanes]
                product = own * wide[start + tap : start + tap + step, lanes]
                depth_grad_ref[8 * tap : 8 * tap + 8, lanes] += jnp.sum(
                    product.reshape(step // 8, 8, 128), axis=0
                )
            gated_ref[0, start : start + step, lanes] = total


def taps_back(grad_conv, ahead, padded, depth_local):
    slots, rows, width = grad_conv.shape
    taps = depth_local.shape[0]
    spare = -(rows + taps - 1) % 8
    reach = jnp.concatenate(
        [grad_conv, ahead, jnp.zeros((slots, spare, width), jnp.float32)], axis=1
    )
    held = jnp.pad(padded, ((0, 0), (0, spare), (0, 0)))
    by_slot = lambda count: pl.BlockSpec((1, count, width), lambda s: (s, 0, 0))
    gated, depth_sums = pl.pallas_call(
        taps_back_kernel,
        out_shape=(
            jax.ShapeDtypeStruct((slots, rows, width), jnp.float32),
            jax.ShapeDtypeStruct((8 * taps, width), jnp.float32),
        ),
        grid=(slots,),
        in_specs=[
            pl.BlockSpec((taps, width), lambda s: (0, 0)),
            by_slot(reach.shape[1]),
            by_slot(held.shape[1]),
        ],
        out_specs=(by_slot(rows), pl.BlockSpec((8 * taps, width), lambda s: (0, 0))),
        scratch_shapes=[pltpu.VMEM((held.shape[1], width), jnp.float32)],
        cost_estimate=pl.CostEstimate(
            flops=4 * taps * slots * rows * width, bytes_accessed=4 << 20, transcendentals=0
        ),
        name="taps_back",
    )(depth_local, reach, held)
    return gated, jnp.sum(depth_sums.reshape(taps, 8, width), axis=1)


def conv_backward(grad_stream, saved, norm_gain, weights, depth_local, inner_gain):
    value_w, gate_w, out_w = weights
    (
        standard,
        inverse,
        wide_rows,
        part_value,
        part_gate,
        padded,
        inner_standard,
        inner_inverse,
        inner_pre,
    ) = saved
    grad_branch = grad_stream.astype(jnp.bfloat16)
    wide_grad = widen_grad(grad_branch)
    active = jax.nn.silu(inner_pre).astype(jnp.bfloat16)
    out_grad = weight_sum(wide_grad, active)
    grad_inner = rows_in(wide_grad, out_w) * silu_slope(inner_pre)
    inner_gain_grad = jnp.sum(grad_inner * inner_standard, axis=(0, 1))
    inner_shift_grad = jnp.sum(grad_inner, axis=(0, 1))
    grad_standard = grad_inner * inner_gain
    row_sums = lax.psum(
        (jnp.sum(grad_standard, axis=-1), jnp.sum(grad_standard * inner_standard, axis=-1)), "tp"
    )
    grad_conv = inner_inverse * (
        grad_standard - (row_sums[0] / D)[..., None] - inner_standard * (row_sums[1] / D)[..., None]
    )
    row_count = grad_conv.shape[1]
    tap_count = depth_local.shape[0]
    reach_rows = tap_count - 1
    ahead = from_behind(grad_conv[:, :reach_rows, :].astype(jnp.bfloat16), "ctx", -1)
    grad_gated, depth_grad = taps_back(grad_conv, ahead.astype(jnp.float32), padded, depth_local)
    gate_sig = jax.nn.sigmoid(part_gate)
    grad_value = (grad_gated * gate_sig).astype(jnp.bfloat16)
    grad_gate = (grad_gated * part_value * gate_sig * (1.0 - gate_sig)).astype(jnp.bfloat16)
    value_w_grad = weight_sum(wide_rows, grad_value)
    gate_w_grad = weight_sum(wide_rows, grad_gate)
    grad_normed = narrow_grad(rows_out(grad_value, value_w) + rows_out(grad_gate, gate_w))
    grad_normed, out_grad, value_w_grad, gate_w_grad = together(
        grad_normed, out_grad, value_w_grad, gate_w_grad
    )
    grad_in, gain_grad, shift_grad = norm_backward(grad_normed, standard, inverse, norm_gain)
    return (
        grad_stream + grad_in,
        (
            gain_grad,
            shift_grad,
            value_w_grad,
            gate_w_grad,
            depth_grad,
            inner_gain_grad,
            inner_shift_grad,
            out_grad,
        ),
    )


def gather_rows(shard):
    return lax.all_gather(shard, ("fsdp", "ctx"), axis=0, tiled=True)


def scatter_sum(*grads):
    joined = jnp.concatenate([grad.astype(jnp.bfloat16) for grad in grads], axis=1)
    part = lax.psum_scatter(joined, ("fsdp", "ctx"), scatter_dimension=0, tiled=True)
    return split_columns(part, grads)


def split_columns(part, grads):
    pieces = []
    start = 0
    for grad in grads:
        pieces.append(part[:, start : start + grad.shape[1]].astype(jnp.float32))
        start += grad.shape[1]
    return tuple(pieces)


def scatter_sum_all(grads, whole_parts, split_parts, own_parts):
    rows = grads[0].shape[0]
    flat = jnp.concatenate([part.reshape(-1) for part in whole_parts + split_parts])
    columns = -(-flat.shape[0] // rows)
    flat = jnp.pad(flat, (0, rows * columns - flat.shape[0])).reshape(rows, columns)
    parts = scatter_sum(*grads, jnp.pad(flat, ((0, 0), (0, -columns % 128))))
    small = parts[-1][:, :columns].reshape(-1)
    held = small.shape[0]
    sent = jnp.concatenate([small] + [part.reshape(-1) for part in own_parts])
    sent = jnp.pad(sent, (0, -sent.shape[0] % 128)).reshape(1, -1, 128)
    tp_count = lax.axis_size("tp")
    every = lax.all_gather(sent, "tp", axis=0, tiled=True)
    every = lax.all_gather(every, ("fsdp", "ctx"), axis=0, tiled=True)
    every = every.reshape(-1, tp_count, sent.size)
    by_tp = every[:, :, :held].transpose(1, 0, 2).reshape(tp_count, -1)
    total = jnp.sum(by_tp, axis=0)
    spread = by_tp
    whole = []
    start = 0
    for part in whole_parts:
        whole.append(total[start : start + part.size].reshape(part.shape))
        start += part.size
    pieces = []
    for part in split_parts:
        piece = spread[:, start : start + part.size]
        if part.ndim == 1:
            pieces.append(piece.reshape(-1))
        else:
            piece = piece.reshape((tp_count,) + part.shape)
            pieces.append(piece.transpose(1, 0, 2).reshape(part.shape[0], -1))
        start += part.size
    own = jnp.sum(every[:, :, held:], axis=(0, 1))
    start = 0
    owned = []
    for part in own_parts:
        owned.append(own[start : start + part.size].reshape(part.shape))
        start += part.size
    w, p = owned[:2] + whole + owned[2:], pieces
    return parts[:-1], (
        w[0], w[1], p[0], w[2], w[3], w[4], p[1], p[2], w[5], w[6], w[7], w[8],
        p[3], p[4], p[5], w[9], w[10], p[6], w[11], w[12], w[13], w[14],
    )


def body(
    inputs,
    teacher,
    clips_dev,
    ffn1_gain,
    ffn1_shift,
    ffn1_in,
    ffn1_in_bias,
    ffn1_out,
    ffn1_out_bias,
    attn_gain,
    attn_shift,
    query_weight,
    query_bias,
    key_weight,
    value_weight,
    value_bias,
    attn_out_weight,
    attn_out_bias,
    rel_table,
    conv_gain,
    conv_shift,
    conv_value_weight,
    conv_gate_weight,
    conv_depth,
    conv_inner_gain,
    conv_inner_shift,
    conv_out_weight,
    ffn2_gain,
    ffn2_shift,
    ffn2_in,
    ffn2_in_bias,
    ffn2_out,
    ffn2_out_bias,
    final_gain,
    final_shift,
):
    width = query_weight.shape[1]
    late_shard = jnp.concatenate(
        [ffn2_in, ffn2_out, conv_value_weight, conv_gate_weight, conv_out_weight], axis=1
    )
    tp_rank = lax.axis_index("tp")
    ctx_rank = lax.axis_index("ctx")
    hidden_local = ffn1_in.shape[1]
    width_local = width
    ffn1_bias_local = local_cut(ffn1_in_bias, tp_rank, hidden_local)
    ffn2_bias_local = local_cut(ffn2_in_bias, tp_rank, hidden_local)
    query_bias_local = local_cut(query_bias, tp_rank, width_local)
    value_bias_local = local_cut(value_bias, tp_rank, width_local)
    depth_local = local_cut(conv_depth, tp_rank, width_local)
    inner_gain_local = local_cut(conv_inner_gain, tp_rank, width_local)
    inner_shift_local = local_cut(conv_inner_shift, tp_rank, width_local)
    stream_zero = inputs.astype(jnp.float32)
    stream_one, saved_one, ffn1_in_all, ffn1_out_all, attn_weights = ffn_forward_first(
        stream_zero,
        ffn1_gain,
        ffn1_shift,
        ffn1_in,
        ffn1_bias_local,
        ffn1_out,
        ffn1_out_bias,
        (query_weight, key_weight, value_weight, attn_out_weight),
    )
    stream_two, saved_two, late = attn_forward(
        stream_one,
        attn_gain,
        attn_shift,
        attn_weights,
        (query_bias_local, value_bias_local, attn_out_bias),
        rel_table,
        ctx_rank,
        late_shard,
    )
    ffn2_in_all = late[:, :hidden_local]
    ffn2_out_all = late[:, hidden_local : 2 * hidden_local]
    conv_all = late[:, 2 * hidden_local :]
    conv_weights = (
        conv_all[:, :width],
        conv_all[:, width : 2 * width],
        conv_all[:, 2 * width :],
    )
    stream_three, saved_three = conv_forward(
        stream_two,
        conv_gain,
        conv_shift,
        conv_weights,
        depth_local,
        inner_gain_local,
        inner_shift_local,
    )
    stream_four, saved_four = ffn_forward(
        stream_three,
        ffn2_gain,
        ffn2_shift,
        ffn2_in_all,
        ffn2_bias_local,
        ffn2_out_all,
        ffn2_out_bias,
    )
    final_out, final_standard, final_inverse = norm_forward(stream_four, final_gain, final_shift)
    live_slots = (
        jnp.arange(final_out.shape[0], dtype=jnp.int32) < clips_dev[lax.axis_index("fsdp")]
    ).astype(jnp.float32)
    misfit = (final_out - teacher.astype(jnp.float32)) * live_slots[:, None, None]
    sse_local = jnp.sum(misfit * misfit)
    gradient_fourth, final_gain_grad, final_shift_grad = norm_backward(
        2.0 * misfit, final_standard, final_inverse, final_gain
    )
    grad_three, ffn2_grads = ffn_backward(
        gradient_fourth, saved_four, ffn2_gain, ffn2_in_all, ffn2_out_all
    )
    grad_two, conv_grads = conv_backward(
        grad_three,
        saved_three,
        conv_gain,
        conv_weights,
        depth_local,
        inner_gain_local,
    )
    grad_one, attn_grads, inner_parts = attn_backward(
        grad_two,
        saved_two,
        attn_gain,
        attn_weights,
        rel_table,
        ctx_rank,
        (ffn2_grads[2], ffn2_grads[4], conv_grads[2], conv_grads[3], conv_grads[7]),
    )
    grad_zero, ffn1_grads = ffn_backward(
        grad_one, saved_one, ffn1_gain, ffn1_in_all, ffn1_out_all
    )
    attn_parts = scatter_sum(attn_grads[2], attn_grads[4], attn_grads[5], attn_grads[7])
    ffn1_parts, shared = scatter_sum_all(
        (ffn1_grads[2], ffn1_grads[4]),
        (
            ffn1_grads[5],
            attn_grads[0],
            attn_grads[1],
            attn_grads[8],
            attn_grads[9],
            conv_grads[0],
            conv_grads[1],
            ffn2_grads[0],
            ffn2_grads[1],
            ffn2_grads[5],
            final_gain_grad,
            final_shift_grad,
        ),
        (
            ffn1_grads[3],
            attn_grads[3],
            attn_grads[6],
            conv_grads[4],
            conv_grads[5],
            conv_grads[6],
            ffn2_grads[3],
        ),
        (ffn1_grads[0], ffn1_grads[1], sse_local),
    )
    weight_parts = ffn1_parts + attn_parts + inner_parts[2:] + inner_parts[:2]
    token_count = (jnp.sum(clips_dev) * SEQ).astype(jnp.float32)
    loss = shared[21] / token_count
    return (
        final_out.astype(jnp.bfloat16),
        loss,
        grad_zero,
        shared[0],
        shared[1],
        weight_parts[0],
        shared[2],
        weight_parts[1],
        shared[3],
        shared[4],
        shared[5],
        weight_parts[2],
        shared[6],
        weight_parts[3],
        weight_parts[4],
        shared[7],
        weight_parts[5],
        shared[8],
        shared[9],
        shared[10],
        shared[11],
        weight_parts[6],
        weight_parts[7],
        shared[12],
        shared[13],
        shared[14],
        weight_parts[8],
        shared[15],
        shared[16],
        weight_parts[9],
        shared[17],
        weight_parts[10],
        shared[18],
        shared[19],
        shared[20],
    )


def solution(mesh):
    in_specs = (
        P("fsdp", ("ctx", "tp"), None),
        P("fsdp", ("ctx", "tp"), None),
        P(),
        P(),
        P(),
        P(("fsdp", "ctx"), "tp"),
        P(),
        P(("fsdp", "ctx"), "tp"),
        P(),
        P(),
        P(),
        P(("fsdp", "ctx"), "tp"),
        P(),
        P(("fsdp", "ctx"), "tp"),
        P(("fsdp", "ctx"), "tp"),
        P(),
        P(("fsdp", "ctx"), "tp"),
        P(),
        P(),
        P(),
        P(),
        P(("fsdp", "ctx"), "tp"),
        P(("fsdp", "ctx"), "tp"),
        P(),
        P(),
        P(),
        P(("fsdp", "ctx"), "tp"),
        P(),
        P(),
        P(("fsdp", "ctx"), "tp"),
        P(),
        P(("fsdp", "ctx"), "tp"),
        P(),
        P(),
        P(),
    )
    out_specs = (
        P("fsdp", ("ctx", "tp"), None),
        P(),
        P("fsdp", ("ctx", "tp"), None),
        P(),
        P(),
        P(("fsdp", "ctx"), "tp"),
        P(),
        P(("fsdp", "ctx"), "tp"),
        P(),
        P(),
        P(),
        P(("fsdp", "ctx"), "tp"),
        P(),
        P(("fsdp", "ctx"), "tp"),
        P(("fsdp", "ctx"), "tp"),
        P(),
        P(("fsdp", "ctx"), "tp"),
        P(),
        P(),
        P(),
        P(),
        P(("fsdp", "ctx"), "tp"),
        P(("fsdp", "ctx"), "tp"),
        P(),
        P(),
        P(),
        P(("fsdp", "ctx"), "tp"),
        P(),
        P(),
        P(("fsdp", "ctx"), "tp"),
        P(),
        P(("fsdp", "ctx"), "tp"),
        P(),
        P(),
        P(),
    )
    return jax.shard_map(body, mesh=mesh, in_specs=in_specs, out_specs=out_specs, check_vma=False)
```

```python
import functools
import math

import jax
import jax.numpy as jnp
from jax import lax
from jax.experimental import pallas as pl
from jax.experimental.pallas import tpu as pltpu
from jax.sharding import PartitionSpec as P

D = 1024
LEFT = 64
HEAD = 64
SEQ = 1536


epsilon = 1e-05


def from_behind(shard, axis, by):
    devices = lax.axis_size(axis)
    pairs = [(i, i + by) for i in range(devices) if 0 <= i + by < devices]
    return lax.ppermute(shard, axis, pairs)


def norm_forward(stream, norm_gain, norm_shift):
    centred = stream - jnp.mean(stream, axis=-1, keepdims=True)
    inverse = lax.rsqrt(jnp.mean(centred * centred, axis=-1, keepdims=True) + epsilon)
    standard = centred * inverse
    return (standard * norm_gain + norm_shift, standard, inverse)


def norm_backward(grad_out, standard, inverse, norm_gain):
    grad_standard = grad_out * norm_gain
    mean_first = jnp.mean(grad_standard, axis=-1, keepdims=True)
    mean_second = jnp.mean(grad_standard * standard, axis=-1, keepdims=True)
    grad_in = inverse * (grad_standard - mean_first - standard * mean_second)
    return (grad_in, jnp.sum(grad_out * standard, axis=(0, 1)), jnp.sum(grad_out, axis=(0, 1)))


def silu_slope(hidden_pre):
    gate_sig = jax.nn.sigmoid(hidden_pre)
    return gate_sig * (1.0 + hidden_pre * (1.0 - gate_sig))


def rows_in(left_reach, right_reach):
    return jnp.einsum("zub,bx->zux", left_reach, right_reach, preferred_element_type=jnp.float32)


def rows_out(left_reach, right_reach):
    return jnp.einsum("anp,op->ano", left_reach, right_reach, preferred_element_type=jnp.float32)


def weight_sum(left_reach, right_reach):
    return jnp.einsum("zbt,zbm->tm", left_reach, right_reach, preferred_element_type=jnp.float32)


def together(*values):
    return lax.optimization_barrier(values)


def widen(normed):
    return lax.all_gather(normed.astype(jnp.bfloat16), "tp", axis=1, tiled=True)


def widen_ctx(normed):
    return lax.all_gather(normed.astype(jnp.bfloat16), "ctx", axis=1, tiled=True)


def narrow_ctx(partial_rows):
    return lax.psum_scatter(
        partial_rows.astype(jnp.bfloat16), "ctx", scatter_dimension=1, tiled=True
    )


def narrow(partial_rows):
    return lax.psum_scatter(
        partial_rows.astype(jnp.bfloat16), "tp", scatter_dimension=1, tiled=True
    ).astype(jnp.float32)


def widen_grad(grad_branch):
    return lax.all_gather(grad_branch, "tp", axis=1, tiled=True)


def narrow_grad(partial_rows):
    return lax.psum_scatter(
        partial_rows.astype(jnp.bfloat16), "tp", scatter_dimension=1, tiled=True
    ).astype(jnp.float32)


def local_cut(full_array, tp_rank, size_local):
    return lax.dynamic_slice_in_dim(
        full_array, tp_rank * size_local, size_local, full_array.ndim - 1
    )


def local_put(local_array, tp_rank, full_size):
    shape_full = local_array.shape[:-1] + (full_size,)
    return lax.dynamic_update_slice_in_dim(
        jnp.zeros(shape_full, jnp.float32),
        local_array,
        tp_rank * local_array.shape[-1],
        local_array.ndim - 1,
    )


BAND = 384


def wide_table(rel_table):
    before = jnp.broadcast_to(rel_table[:1], (LEFT, HEAD))
    after = jnp.broadcast_to(rel_table[-1:], (BAND - LEFT - rel_table.shape[0], HEAD))
    return jnp.concatenate([before, rel_table, after], axis=0)


def dot_t(left, right):
    return lax.dot_general(left, right, (((1,), (1,)), ((), ())), preferred_element_type=jnp.float32)


def dot_n(left, right):
    return lax.dot_general(left, right, (((1,), (0,)), ((), ())), preferred_element_type=jnp.float32)


def scaled_scores(query_block, keys, table, place, rows_at, reach):
    rows = query_block.shape[0]
    key_count = keys.shape[0]
    near = dot_t(query_block, table)
    left, right = near[:, :1], near[:, BAND - 1 :]
    row = lax.broadcasted_iota(jnp.int32, (rows, key_count), 0)
    col = lax.broadcasted_iota(jnp.int32, (rows, key_count), 1)
    place[:, 128 : 128 + key_count] = dot_t(query_block, keys) + jnp.where(
        col < row + rows_at, left, right
    )
    rolled = pltpu.roll(near, 0, 1, stride=1, stride_axis=0)
    apart = band_distance(rows)
    band = jnp.where(apart <= -LEFT, left, jnp.where(apart >= reach, right, rolled))
    window = pl.ds(pl.multiple_of(rows_at, 128), BAND)
    place[:, window] += band - jnp.where(apart < 0, left, right)
    return place[:, 128 : 128 + key_count]


def band_distance(rows):
    row = lax.broadcasted_iota(jnp.int32, (rows, BAND), 0)
    col = lax.broadcasted_iota(jnp.int32, (rows, BAND), 1)
    return col - 128 - row


def attend_kernel(reach, start_ref, query_ref, key_ref, value_ref, table_ref, mixed_ref, total_ref, place):
    rows = query_ref.shape[1]
    rows_at = start_ref[0] + pl.program_id(2) * rows
    table = table_ref[...]
    for half in range(query_ref.shape[2] // HEAD):
        lanes = slice(half * HEAD, (half + 1) * HEAD)
        query_block = query_ref[0, :, lanes] * jnp.bfloat16(1.0 / math.sqrt(HEAD))
        scores = scaled_scores(query_block, key_ref[0, :, lanes], table, place, rows_at, reach)
        top = jnp.max(scores, axis=-1, keepdims=True)
        powers = jnp.exp(scores - top)
        row_sum = jnp.sum(powers, axis=-1, keepdims=True)
        probs = (powers * (1.0 / row_sum)).astype(jnp.bfloat16)
        mixed_ref[0, :, lanes] = dot_n(probs, value_ref[0, :, lanes]).astype(jnp.bfloat16)
        total_ref[0, :, lanes] = jnp.broadcast_to(top + jnp.log(row_sum), (rows, HEAD))


def attend_back_kernel(
    reach, start_ref, query_ref, key_ref, value_ref, table_ref, total_ref, grad_ref, groups_ref,
    query_grad_ref, pair_grad_ref, table_grad_ref, place, key_sum, value_sum,
):
    rows = query_ref.shape[1]
    key_count = key_ref.shape[1]
    block = pl.program_id(2)
    rows_at = start_ref[0] + block * rows
    table = table_ref[...]
    scale = jnp.bfloat16(1.0 / math.sqrt(HEAD))

    @pl.when(block == 0)
    def _():
        key_sum[...] = jnp.zeros_like(key_sum)
        value_sum[...] = jnp.zeros_like(value_sum)

    @pl.when((block == 0) & (pl.program_id(0) == 0) & (pl.program_id(1) == 0))
    def _():
        table_grad_ref[...] = jnp.zeros_like(table_grad_ref)

    for half in range(query_ref.shape[2] // HEAD):
        lanes = slice(half * HEAD, (half + 1) * HEAD)
        query_block = query_ref[0, :, lanes] * scale
        keys = key_ref[0, :, lanes]
        grad_block = grad_ref[0, :, lanes]
        scores = scaled_scores(query_block, keys, table, place, rows_at, reach)
        probs = jnp.exp(scores - total_ref[0, :, half * HEAD : half * HEAD + 1])
        grad_probs = dot_t(grad_block, value_ref[0, :, lanes])
        row_dot = jnp.sum(probs * grad_probs, axis=-1, keepdims=True)
        grad_scores = (probs * (grad_probs - row_dot)).astype(jnp.bfloat16)
        value_sum[lanes, :] += dot_n(grad_block.T, probs.astype(jnp.bfloat16))
        key_sum[lanes, :] += dot_n(query_block.T, grad_scores)
        wide = grad_scores.astype(jnp.float32)
        place[:, 128 : 128 + key_count] = wide
        window = place[:, pl.ds(pl.multiple_of(rows_at, 128), BAND)]
        window_col = lax.broadcasted_iota(jnp.int32, window.shape, 1) + rows_at - 128
        window = jnp.where((window_col >= 0) & (window_col < key_count), window, 0.0)
        apart = band_distance(rows)
        by_group = dot_n(grad_scores, groups_ref[...])
        past = lax.broadcasted_iota(jnp.int32, by_group.shape, 1) * 128 - rows_at
        far_left = jnp.sum(jnp.where(past < -128, by_group, 0.0), axis=-1, keepdims=True)
        far_left += jnp.sum(jnp.where(apart <= -LEFT, window, 0.0), axis=-1, keepdims=True)
        far_right = jnp.sum(jnp.where(past >= BAND - 128, by_group, 0.0), axis=-1, keepdims=True)
        far_right += jnp.sum(jnp.where(apart >= reach, window, 0.0), axis=-1, keepdims=True)
        inside = (apart > -LEFT) & (apart < reach)
        turned = jnp.where(inside, window, 0.0)
        row = lax.broadcasted_iota(jnp.int32, turned.shape, 0)
        for bit in range((rows - 1).bit_length()):
            moved = pltpu.roll(turned, BAND - (1 << bit), 1)
            turned = jnp.where(((row >> bit) & 1) == 1, moved, turned)
        lane = lax.broadcasted_iota(jnp.int32, turned.shape, 1)
        by_row = jnp.where(lane == LEFT, far_left, jnp.where(lane == 2 * LEFT + reach, far_right, turned))
        coarse = by_row.astype(jnp.bfloat16)
        fine = (by_row - coarse.astype(jnp.float32)).astype(jnp.bfloat16)
        query_grad = dot_n(grad_scores, keys) + dot_n(coarse, table) + dot_n(fine, table)
        query_grad_ref[0, :, lanes] = (query_grad * (1.0 / math.sqrt(HEAD))).astype(jnp.bfloat16)
        query_turned = query_block.T
        table_grad_ref[...] += dot_n(query_turned, coarse) + dot_n(query_turned, fine)

    @pl.when(block == pl.num_programs(2) - 1)
    def _():
        pair_grad_ref[0, 0] = key_sum[...].T.astype(jnp.bfloat16)
        pair_grad_ref[1, 0] = value_sum[...].T.astype(jnp.bfloat16)


def attend_specs(queries, keys):
    slots, rows, width = queries.shape
    lanes = 2 * HEAD
    block = 128
    grid = (slots, width // lanes, rows // block)
    by_query = pl.BlockSpec((1, block, lanes), lambda s, p, b, *_: (s, b, p))
    by_key = pl.BlockSpec((1, keys.shape[1], lanes), lambda s, p, b, *_: (s, 0, p))
    by_value = pl.BlockSpec(
        (1, keys.shape[1], lanes), lambda s, p, b, *_: (s, 0, p + width // lanes)
    )
    table = pl.BlockSpec((BAND, HEAD), lambda s, p, b, *_: (0, 0))
    place = pltpu.VMEM((block, keys.shape[1] + 256), jnp.float32)
    flops = slots * rows * keys.shape[1] * width * 4
    return grid, by_query, by_key, by_value, table, place, flops


def attend(queries, pairs, table, reach, query_start):
    grid, by_query, by_key, by_value, by_table, place, flops = attend_specs(queries, pairs)
    return pl.pallas_call(
        functools.partial(attend_kernel, reach),
        out_shape=(
            jax.ShapeDtypeStruct(queries.shape, jnp.bfloat16),
            jax.ShapeDtypeStruct(queries.shape, jnp.float32),
        ),
        grid_spec=pltpu.PrefetchScalarGridSpec(
            num_scalar_prefetch=1,
            grid=grid,
            in_specs=[by_query, by_key, by_value, by_table],
            out_specs=(by_query, by_query),
            scratch_shapes=[place],
        ),
        cost_estimate=pl.CostEstimate(flops=2 * flops, bytes_accessed=8 << 20, transcendentals=flops >> 8),
        name="attend",
    )(query_start.reshape(1), queries, pairs, pairs, table)


def attend_back(queries, pairs, table, totals, grad_mixed, reach, query_start):
    grid, by_query, by_key, by_value, by_table, place, flops = attend_specs(queries, pairs)
    slots, key_count = pairs.shape[:2]
    turned = pltpu.VMEM((2 * HEAD, key_count), jnp.float32)
    group = jnp.arange(key_count, dtype=jnp.int32)[:, None] // 128
    groups = (group == jnp.arange(128, dtype=jnp.int32)[None, :]).astype(jnp.bfloat16)
    return pl.pallas_call(
        functools.partial(attend_back_kernel, reach),
        out_shape=(
            jax.ShapeDtypeStruct(queries.shape, jnp.bfloat16),
            jax.ShapeDtypeStruct((2, slots, key_count, queries.shape[2]), jnp.bfloat16),
            jax.ShapeDtypeStruct((HEAD, BAND), jnp.float32),
        ),
        grid_spec=pltpu.PrefetchScalarGridSpec(
            num_scalar_prefetch=1,
            grid=grid,
            in_specs=[
                by_query,
                by_key,
                by_value,
                by_table,
                by_query,
                by_query,
                pl.BlockSpec((key_count, 128), lambda s, p, b, *_: (0, 0)),
            ],
            out_specs=(
                by_query,
                pl.BlockSpec((2, 1, key_count, 2 * HEAD), lambda s, p, b, *_: (0, s, 0, p)),
                pl.BlockSpec((HEAD, BAND), lambda s, p, b, *_: (0, 0)),
            ),
            scratch_shapes=[place, turned, turned],
        ),
        cost_estimate=pl.CostEstimate(flops=5 * flops, bytes_accessed=16 << 20, transcendentals=flops >> 8),
        name="attend_back",
    )(query_start.reshape(1), queries, pairs, pairs, table, totals, grad_mixed, groups)


def ffn_forward(stream, norm_gain, norm_shift, weight_in, bias_in, weight_out, bias_out):
    normed, standard, inverse = norm_forward(stream, norm_gain, norm_shift)
    wide_rows = widen_ctx(normed)
    hidden_pre = rows_in(wide_rows, weight_in) + bias_in
    active = jax.nn.silu(hidden_pre).astype(jnp.bfloat16)
    branch = narrow_ctx(rows_out(active, weight_out)).astype(jnp.float32) + bias_out
    return (stream + 0.5 * branch, (standard, inverse, wide_rows, hidden_pre))


def ffn_forward_first(
    stream, norm_gain, norm_shift, shard_in, bias_in, shard_out, bias_out, later_shards
):
    normed, standard, inverse = norm_forward(stream, norm_gain, norm_shift)
    normed, shard_in, shard_out = together(normed.astype(jnp.bfloat16), shard_in, shard_out)
    wide_rows = widen_ctx(normed)
    mine_in, mine_out = across(shard_in), across(shard_out)
    piece = -(-mine_in.shape[0] // 4)
    pieces = [
        gather_panels(mine_in[start : start + piece])
        for start in range(0, mine_in.shape[0], piece)
    ]
    weight_out = gather_panels(mine_out)
    weight_in = join_panels(jnp.concatenate(pieces, axis=1))
    wide_rows, weight_in, weight_out = together(wide_rows, weight_in, weight_out)
    weight_out = join_panels(weight_out)
    hidden_pre = rows_in(wide_rows, weight_in) + bias_in
    active = jax.nn.silu(hidden_pre).astype(jnp.bfloat16)
    partial_rows = rows_out(active, weight_out).astype(jnp.bfloat16)
    partial_rows, *later_shards = together(partial_rows, *later_shards)
    later = [gather_rows(shard) for shard in later_shards]
    summed = narrow_ctx(partial_rows)
    summed, *later = together(summed, *later)
    branch = summed.astype(jnp.float32) + bias_out
    saved = (standard, inverse, wide_rows, hidden_pre)
    return (stream + 0.5 * branch, saved, weight_in, weight_out, later)


def ffn_backward(grad_stream, saved, norm_gain, weight_in, weight_out, beside=None):
    standard, inverse, wide_rows, hidden_pre = saved
    grad_branch = (0.5 * grad_stream).astype(jnp.bfloat16)
    out_bias_grad = jnp.sum(grad_branch.astype(jnp.float32), axis=(0, 1))
    wide_grad = widen_ctx(grad_branch)
    if beside is not None:
        wide_grad, beside = together(wide_grad, beside)
        beside = lax.psum_scatter(beside, ("fsdp", "ctx"), scatter_dimension=0, tiled=True)
    active = jax.nn.silu(hidden_pre).astype(jnp.bfloat16)
    out_grad = weight_sum(wide_grad, active)
    grad_pre = (rows_in(wide_grad, weight_out) * silu_slope(hidden_pre)).astype(jnp.bfloat16)
    in_bias_grad = jnp.sum(grad_pre.astype(jnp.float32), axis=(0, 1))
    in_grad = weight_sum(wide_rows, grad_pre)
    partial_rows = rows_out(grad_pre, weight_in).astype(jnp.bfloat16)
    if beside is not None:
        partial_rows, beside = together(partial_rows, beside)
    grad_normed = narrow_ctx(partial_rows)
    grad_normed, in_grad, out_grad = together(grad_normed, in_grad, out_grad)
    grad_normed = grad_normed.astype(jnp.float32)
    grad_in, gain_grad, shift_grad = norm_backward(grad_normed, standard, inverse, norm_gain)
    return (
        grad_stream + grad_in,
        (gain_grad, shift_grad, in_grad, in_bias_grad, out_grad, out_bias_grad),
        beside,
    )


def attn_forward(stream, norm_gain, norm_shift, weights, biases, rel_table, ctx_rank, late_shard, panel_shards):
    query_w, key_w, value_w, out_w = weights
    query_b, value_b, out_b = biases
    normed, standard, inverse = norm_forward(stream, norm_gain, norm_shift)
    normed, *panel_shards = together(normed.astype(jnp.bfloat16), *panel_shards)
    mine = jnp.concatenate([across(shard) for shard in panel_shards], axis=1)
    wide_rows, mine = together(widen(normed), mine)
    queries = (rows_in(wide_rows, query_w) + query_b).astype(jnp.bfloat16)
    pair_b = jnp.concatenate([jnp.zeros_like(value_b), value_b])
    pair_w = jnp.concatenate([key_w, value_w], axis=1)
    pairs = (rows_in(wide_rows, pair_w) + pair_b).astype(jnp.bfloat16)
    pairs_all = lax.all_gather(pairs, "ctx", axis=1, tiled=True)
    pairs_all, late_shard, mine = together(pairs_all, late_shard, mine)
    late = (gather_panels(mine), gather_rows(late_shard))
    reach = rel_table.shape[0] - 1 - LEFT
    mixed_token_rows, log_total = attend(
        queries, pairs_all, wide_table(rel_table), reach, ctx_rank * queries.shape[1]
    )
    mixed_token_rows, *late = together(mixed_token_rows, *late)
    branch = narrow(rows_out(mixed_token_rows, out_w)) + out_b
    return (
        stream + branch,
        (standard, inverse, wide_rows, queries, pairs_all, mixed_token_rows, log_total),
        late,
    )


def attn_backward(grad_stream, saved, norm_gain, weights, rel_table, ctx_rank, inner_grads):
    query_w, key_w, value_w, out_w = weights
    standard, inverse, wide_rows, queries, pairs_all, mixed_token_rows, log_total = saved
    grad_branch = grad_stream.astype(jnp.bfloat16)
    out_bias_grad = jnp.sum(grad_branch.astype(jnp.float32), axis=(0, 1))
    inner = jnp.concatenate([grad.astype(jnp.bfloat16) for grad in inner_grads[2:]], axis=1)
    panels = split_panels(*inner_grads[:2])
    wide_grad, inner, panels = together(widen_grad(grad_branch), inner, panels)
    inner = lax.psum_scatter(inner, ("fsdp", "ctx"), scatter_dimension=0, tiled=True)
    panels = scatter_panels(panels)
    grad_mixed = rows_in(wide_grad, out_w).astype(jnp.bfloat16)
    reach = rel_table.shape[0] - 1 - LEFT
    query_low, pair_terms, table_turned = attend_back(
        queries,
        pairs_all,
        wide_table(rel_table),
        log_total,
        grad_mixed,
        reach,
        ctx_rank * queries.shape[1],
    )
    query_low, pair_terms, inner, panels = together(query_low, pair_terms, inner, panels)
    out_grad = weight_sum(wide_grad, mixed_token_rows)
    inner_parts = split_columns(inner, inner_grads[2:])
    table_grad = table_turned[:, LEFT : LEFT + rel_table.shape[0]].T
    pair_low = lax.psum_scatter(pair_terms, "ctx", scatter_dimension=2, tiled=True)
    half = panels.shape[1] // 2
    pair_low, first_part, second_part = together(
        pair_low, across_back(panels[:, :half]), across_back(panels[:, half:])
    )
    inner_parts = (
        first_part.astype(jnp.float32),
        second_part.astype(jnp.float32),
    ) + inner_parts
    key_low, value_low = pair_low[0], pair_low[1]
    query_bias_grad = jnp.sum(query_low.astype(jnp.float32), axis=(0, 1))
    value_bias_grad = jnp.sum(value_low.astype(jnp.float32), axis=(0, 1))
    query_w_grad = weight_sum(wide_rows, query_low)
    key_w_grad = weight_sum(wide_rows, key_low)
    value_w_grad = weight_sum(wide_rows, value_low)
    grad_normed = narrow_grad(
        rows_out(query_low, query_w) + rows_out(key_low, key_w) + rows_out(value_low, value_w)
    )
    grad_normed, out_grad, query_w_grad, key_w_grad, value_w_grad = together(
        grad_normed, out_grad, query_w_grad, key_w_grad, value_w_grad
    )
    grad_in, gain_grad, shift_grad = norm_backward(grad_normed, standard, inverse, norm_gain)
    return (
        grad_stream + grad_in,
        (
            gain_grad,
            shift_grad,
            query_w_grad,
            query_bias_grad,
            key_w_grad,
            value_w_grad,
            value_bias_grad,
            out_grad,
            out_bias_grad,
            table_grad,
        ),
        inner_parts,
    )


def conv_forward(stream, norm_gain, norm_shift, weights, depth_local, inner_gain, inner_offset):
    value_w, gate_w, out_w = weights
    normed, standard, inverse = norm_forward(stream, norm_gain, norm_shift)
    wide_rows = widen(normed)
    part_value = rows_in(wide_rows, value_w)
    part_gate = rows_in(wide_rows, gate_w)
    gated_rows = (part_value * jax.nn.sigmoid(part_gate)).astype(jnp.bfloat16)
    row_count = gated_rows.shape[1]
    reach_rows = depth_local.shape[0] - 1
    halo_rows = from_behind(gated_rows[:, row_count - reach_rows :, :], "ctx", 1)
    padded = jnp.concatenate([halo_rows, gated_rows], axis=1)
    padded_float = padded.astype(jnp.float32)
    convolved = depth_local[0] * padded_float[:, 0:row_count, :]
    for tap_index in range(1, depth_local.shape[0]):
        convolved = (
            convolved
            + depth_local[tap_index] * padded_float[:, tap_index : tap_index + row_count, :]
        )
    row_sums = lax.psum(
        (jnp.sum(convolved, axis=-1), jnp.sum(convolved * convolved, axis=-1)), "tp"
    )
    row_mean = (row_sums[0] / D)[..., None]
    row_var = (row_sums[1] / D)[..., None] - row_mean * row_mean
    inner_inverse = lax.rsqrt(row_var + epsilon)
    inner_standard = (convolved - row_mean) * inner_inverse
    inner_pre = inner_standard * inner_gain + inner_offset
    active = jax.nn.silu(inner_pre).astype(jnp.bfloat16)
    branch = narrow(rows_out(active, out_w))
    return (
        stream + branch,
        (
            standard,
            inverse,
            wide_rows,
            part_value,
            part_gate,
            padded,
            inner_standard,
            inner_inverse,
            inner_pre,
        ),
    )


def taps_back_kernel(depth_ref, grad_ref, padded_ref, gated_ref, depth_grad_ref, wide):
    taps = depth_ref.shape[0]
    rows, width = gated_ref.shape[1:]
    step = 64

    @pl.when(pl.program_id(0) == 0)
    def _():
        depth_grad_ref[...] = jnp.zeros_like(depth_grad_ref)

    wide[: padded_ref.shape[1], :] = padded_ref[0].astype(jnp.float32)
    for lane in range(0, width, 128):
        lanes = slice(lane, lane + 128)
        for start in range(0, rows, step):
            own = grad_ref[0, start : start + step, lanes]
            total = jnp.zeros((step, 128), jnp.float32)
            for tap in range(taps):
                first = start + taps - 1 - tap
                total += depth_ref[tap : tap + 1, lanes] * grad_ref[0, first : first + step, lanes]
                product = own * wide[start + tap : start + tap + step, lanes]
                depth_grad_ref[8 * tap : 8 * tap + 8, lanes] += jnp.sum(
                    product.reshape(step // 8, 8, 128), axis=0
                )
            gated_ref[0, start : start + step, lanes] = total


def taps_back(grad_conv, ahead, padded, depth_local):
    slots, rows, width = grad_conv.shape
    taps = depth_local.shape[0]
    spare = -(rows + taps - 1) % 8
    reach = jnp.concatenate(
        [grad_conv, ahead, jnp.zeros((slots, spare, width), jnp.float32)], axis=1
    )
    held = jnp.pad(padded, ((0, 0), (0, spare), (0, 0)))
    by_slot = lambda count: pl.BlockSpec((1, count, width), lambda s: (s, 0, 0))
    gated, depth_sums = pl.pallas_call(
        taps_back_kernel,
        out_shape=(
            jax.ShapeDtypeStruct((slots, rows, width), jnp.float32),
            jax.ShapeDtypeStruct((8 * taps, width), jnp.float32),
        ),
        grid=(slots,),
        in_specs=[
            pl.BlockSpec((taps, width), lambda s: (0, 0)),
            by_slot(reach.shape[1]),
            by_slot(held.shape[1]),
        ],
        out_specs=(by_slot(rows), pl.BlockSpec((8 * taps, width), lambda s: (0, 0))),
        scratch_shapes=[pltpu.VMEM((held.shape[1], width), jnp.float32)],
        cost_estimate=pl.CostEstimate(
            flops=4 * taps * slots * rows * width, bytes_accessed=4 << 20, transcendentals=0
        ),
        name="taps_back",
    )(depth_local, reach, held)
    return gated, jnp.sum(depth_sums.reshape(taps, 8, width), axis=1)


def conv_backward(grad_stream, saved, norm_gain, weights, depth_local, inner_gain):
    value_w, gate_w, out_w = weights
    (
        standard,
        inverse,
        wide_rows,
        part_value,
        part_gate,
        padded,
        inner_standard,
        inner_inverse,
        inner_pre,
    ) = saved
    grad_branch = grad_stream.astype(jnp.bfloat16)
    wide_grad = widen_grad(grad_branch)
    active = jax.nn.silu(inner_pre).astype(jnp.bfloat16)
    out_grad = weight_sum(wide_grad, active)
    grad_inner = rows_in(wide_grad, out_w) * silu_slope(inner_pre)
    inner_gain_grad = jnp.sum(grad_inner * inner_standard, axis=(0, 1))
    inner_shift_grad = jnp.sum(grad_inner, axis=(0, 1))
    grad_standard = grad_inner * inner_gain
    row_sums = lax.psum(
        (jnp.sum(grad_standard, axis=-1), jnp.sum(grad_standard * inner_standard, axis=-1)), "tp"
    )
    grad_conv = inner_inverse * (
        grad_standard - (row_sums[0] / D)[..., None] - inner_standard * (row_sums[1] / D)[..., None]
    )
    row_count = grad_conv.shape[1]
    tap_count = depth_local.shape[0]
    reach_rows = tap_count - 1
    ahead = from_behind(grad_conv[:, :reach_rows, :].astype(jnp.bfloat16), "ctx", -1)
    grad_gated, depth_grad = taps_back(grad_conv, ahead.astype(jnp.float32), padded, depth_local)
    gate_sig = jax.nn.sigmoid(part_gate)
    grad_value = (grad_gated * gate_sig).astype(jnp.bfloat16)
    grad_gate = (grad_gated * part_value * gate_sig * (1.0 - gate_sig)).astype(jnp.bfloat16)
    value_w_grad = weight_sum(wide_rows, grad_value)
    gate_w_grad = weight_sum(wide_rows, grad_gate)
    grad_normed = narrow_grad(rows_out(grad_value, value_w) + rows_out(grad_gate, gate_w))
    grad_normed, out_grad, value_w_grad, gate_w_grad = together(
        grad_normed, out_grad, value_w_grad, gate_w_grad
    )
    grad_in, gain_grad, shift_grad = norm_backward(grad_normed, standard, inverse, norm_gain)
    return (
        grad_stream + grad_in,
        (
            gain_grad,
            shift_grad,
            value_w_grad,
            gate_w_grad,
            depth_grad,
            inner_gain_grad,
            inner_shift_grad,
            out_grad,
        ),
    )


def across(shard):
    return lax.all_to_all(shard, "ctx", split_axis=1, concat_axis=0, tiled=True)


def across_back(shard):
    return lax.all_to_all(shard, "ctx", split_axis=0, concat_axis=1, tiled=True)


def gather_panels(mine):
    return lax.all_gather(mine, ("tp", "fsdp"), axis=0, tiled=False)


def join_panels(panels):
    count, rows, columns = panels.shape
    tp_count = lax.axis_size("tp")
    panels = panels.reshape(tp_count, count // tp_count * rows, columns)
    return panels.transpose(1, 0, 2).reshape(panels.shape[1], tp_count * columns)


def split_panels(*grads):
    tp_count = lax.axis_size("tp")
    parts = []
    for grad in grads:
        part = grad.astype(jnp.bfloat16).reshape(grad.shape[0], tp_count, -1)
        parts.append(part.transpose(1, 0, 2).reshape(tp_count * grad.shape[0], -1))
    return jnp.concatenate(parts, axis=1)


def scatter_panels(joined):
    return lax.psum_scatter(joined, ("tp", "fsdp"), scatter_dimension=0, tiled=True)


def gather_rows(shard):
    return lax.all_gather(shard, ("fsdp", "ctx"), axis=0, tiled=True)


def scatter_sum(*grads):
    joined = jnp.concatenate([grad.astype(jnp.bfloat16) for grad in grads], axis=1)
    part = lax.psum_scatter(joined, ("fsdp", "ctx"), scatter_dimension=0, tiled=True)
    return split_columns(part, grads)


def split_columns(part, grads):
    pieces = []
    start = 0
    for grad in grads:
        pieces.append(part[:, start : start + grad.shape[1]].astype(jnp.float32))
        start += grad.shape[1]
    return tuple(pieces)


def small_columns(whole_parts, split_parts, rows):
    flat = jnp.concatenate([part.reshape(-1) for part in whole_parts + split_parts])
    columns = -(-flat.shape[0] // rows)
    flat = jnp.pad(flat, (0, rows * columns - flat.shape[0])).reshape(rows, columns)
    return jnp.pad(flat, ((0, 0), (0, -columns % 128)))


def finish_small(small, whole_parts, split_parts, own_parts, hidden_part):
    rows = small.shape[0] * lax.axis_size(("fsdp", "ctx"))
    count = sum(part.size for part in whole_parts + split_parts)
    small = small[:, : -(-count // rows)].astype(jnp.float32).reshape(-1)
    held = small.shape[0]
    sent = jnp.concatenate(
        [small] + [part.reshape(-1) for part in own_parts] + [hidden_part.reshape(-1)]
    )
    sent = jnp.pad(sent, (0, -sent.shape[0] % 128)).reshape(1, -1, 128)
    tp_count = lax.axis_size("tp")
    ctx_count = lax.axis_size("ctx")
    every = lax.all_gather(sent, "tp", axis=0, tiled=True)
    every = lax.all_gather(every, ("fsdp", "ctx"), axis=0, tiled=True)
    every = every.reshape(-1, tp_count, sent.size)
    by_tp = every[:, :, :held].transpose(1, 0, 2).reshape(tp_count, -1)
    total = jnp.sum(by_tp, axis=0)
    spread = by_tp
    whole = []
    start = 0
    for part in whole_parts:
        whole.append(total[start : start + part.size].reshape(part.shape))
        start += part.size
    pieces = []
    for part in split_parts:
        piece = spread[:, start : start + part.size]
        if part.ndim == 1:
            pieces.append(piece.reshape(-1))
        else:
            piece = piece.reshape((tp_count,) + part.shape)
            pieces.append(piece.transpose(1, 0, 2).reshape(part.shape[0], -1))
        start += part.size
    own = jnp.sum(every[:, :, held:], axis=(0, 1))
    start = 0
    owned = []
    for part in own_parts:
        owned.append(own[start : start + part.size].reshape(part.shape))
        start += part.size
    first = held + start
    hidden = every[:, :, first : first + hidden_part.size]
    hidden = hidden.reshape(-1, ctx_count, tp_count, hidden_part.size).sum(axis=(0, 2))
    hidden = hidden_order(hidden)
    w, p = whole, pieces
    return (
        owned[0], owned[1], hidden, owned[2], w[0], w[1], p[0], p[1], w[2], w[3], w[4], w[5],
        p[2], p[3], p[4], w[6], w[7], w[8], w[9], w[10], w[11], owned[3],
    )


def hidden_order(by_ctx):
    ctx_count = by_ctx.shape[0]
    parts = by_ctx.reshape(ctx_count, lax.axis_size("tp"), -1)
    return parts.transpose(1, 0, 2).reshape(-1)


def hidden_local(full, ctx_rank):
    parts = full.reshape(lax.axis_size("tp"), lax.axis_size("ctx"), -1)
    return lax.dynamic_slice_in_dim(parts, ctx_rank, 1, 1).reshape(-1)


def hidden_put(local, ctx_rank):
    parts = local.reshape(lax.axis_size("tp"), 1, -1)
    full = jnp.zeros((parts.shape[0], lax.axis_size("ctx"), parts.shape[2]), jnp.float32)
    return lax.dynamic_update_slice_in_dim(full, parts, ctx_rank, 1).reshape(-1)


def body(
    inputs,
    teacher,
    clips_dev,
    ffn1_gain,
    ffn1_shift,
    ffn1_in,
    ffn1_in_bias,
    ffn1_out,
    ffn1_out_bias,
    attn_gain,
    attn_shift,
    query_weight,
    query_bias,
    key_weight,
    value_weight,
    value_bias,
    attn_out_weight,
    attn_out_bias,
    rel_table,
    conv_gain,
    conv_shift,
    conv_value_weight,
    conv_gate_weight,
    conv_depth,
    conv_inner_gain,
    conv_inner_shift,
    conv_out_weight,
    ffn2_gain,
    ffn2_shift,
    ffn2_in,
    ffn2_in_bias,
    ffn2_out,
    ffn2_out_bias,
    final_gain,
    final_shift,
):
    width = query_weight.shape[1]
    late_shard = jnp.concatenate(
        [conv_value_weight, conv_gate_weight, conv_out_weight], axis=1
    )
    tp_rank = lax.axis_index("tp")
    ctx_rank = lax.axis_index("ctx")
    width_local = width
    ffn1_bias_local = hidden_local(ffn1_in_bias, ctx_rank)
    ffn2_bias_local = hidden_local(ffn2_in_bias, ctx_rank)
    query_bias_local = local_cut(query_bias, tp_rank, width_local)
    value_bias_local = local_cut(value_bias, tp_rank, width_local)
    depth_local = local_cut(conv_depth, tp_rank, width_local)
    inner_gain_local = local_cut(conv_inner_gain, tp_rank, width_local)
    inner_shift_local = local_cut(conv_inner_shift, tp_rank, width_local)
    stream_zero = inputs.astype(jnp.float32)
    stream_one, saved_one, ffn1_in_all, ffn1_out_all, attn_weights = ffn_forward_first(
        stream_zero,
        ffn1_gain,
        ffn1_shift,
        ffn1_in,
        ffn1_bias_local,
        ffn1_out,
        ffn1_out_bias,
        (query_weight, key_weight, value_weight, attn_out_weight),
    )
    stream_two, saved_two, late = attn_forward(
        stream_one,
        attn_gain,
        attn_shift,
        attn_weights,
        (query_bias_local, value_bias_local, attn_out_bias),
        rel_table,
        ctx_rank,
        late_shard,
        (ffn2_in, ffn2_out),
    )
    half = late[0].shape[2] // 2
    ffn2_in_all = join_panels(late[0][:, :, :half])
    ffn2_out_all = join_panels(late[0][:, :, half:])
    conv_all = late[1]
    conv_weights = (
        conv_all[:, :width],
        conv_all[:, width : 2 * width],
        conv_all[:, 2 * width :],
    )
    stream_three, saved_three = conv_forward(
        stream_two,
        conv_gain,
        conv_shift,
        conv_weights,
        depth_local,
        inner_gain_local,
        inner_shift_local,
    )
    stream_four, saved_four = ffn_forward(
        stream_three,
        ffn2_gain,
        ffn2_shift,
        ffn2_in_all,
        ffn2_bias_local,
        ffn2_out_all,
        ffn2_out_bias,
    )
    final_out, final_standard, final_inverse = norm_forward(stream_four, final_gain, final_shift)
    live_slots = (
        jnp.arange(final_out.shape[0], dtype=jnp.int32) < clips_dev[lax.axis_index("fsdp")]
    ).astype(jnp.float32)
    misfit = (final_out - teacher.astype(jnp.float32)) * live_slots[:, None, None]
    sse_local = jnp.sum(misfit * misfit)
    gradient_fourth, final_gain_grad, final_shift_grad = norm_backward(
        2.0 * misfit, final_standard, final_inverse, final_gain
    )
    grad_three, ffn2_grads, _ = ffn_backward(
        gradient_fourth, saved_four, ffn2_gain, ffn2_in_all, ffn2_out_all
    )
    grad_two, conv_grads = conv_backward(
        grad_three,
        saved_three,
        conv_gain,
        conv_weights,
        depth_local,
        inner_gain_local,
    )
    grad_one, attn_grads, inner_parts = attn_backward(
        grad_two,
        saved_two,
        attn_gain,
        attn_weights,
        rel_table,
        ctx_rank,
        (ffn2_grads[2], ffn2_grads[4], conv_grads[2], conv_grads[3], conv_grads[7]),
    )
    attn_mats = (attn_grads[2], attn_grads[4], attn_grads[5], attn_grads[7])
    whole_parts = (
        attn_grads[0],
        attn_grads[1],
        attn_grads[8],
        attn_grads[9],
        conv_grads[0],
        conv_grads[1],
        ffn2_grads[0],
        ffn2_grads[1],
        hidden_put(ffn2_grads[3], ctx_rank),
        ffn2_grads[5],
        final_gain_grad,
        final_shift_grad,
    )
    split_parts = (
        attn_grads[3],
        attn_grads[6],
        conv_grads[4],
        conv_grads[5],
        conv_grads[6],
    )
    columns = small_columns(whole_parts, split_parts, attn_mats[0].shape[0])
    beside_mats = attn_mats + (columns,)
    beside = jnp.concatenate([part.astype(jnp.bfloat16) for part in beside_mats], axis=1)
    grad_zero, ffn1_grads, beside = ffn_backward(
        grad_one, saved_one, ffn1_gain, ffn1_in_all, ffn1_out_all, beside
    )
    attn_parts = split_columns(beside, beside_mats)
    panels = scatter_panels(split_panels(ffn1_grads[2], ffn1_grads[4]))
    half = panels.shape[1] // 2
    ffn1_parts = (
        across_back(panels[:, :half]).astype(jnp.float32),
        across_back(panels[:, half:]).astype(jnp.float32),
    )
    shared = finish_small(
        attn_parts[-1],
        whole_parts,
        split_parts,
        (ffn1_grads[0], ffn1_grads[1], ffn1_grads[5], sse_local),
        ffn1_grads[3],
    )
    attn_parts = attn_parts[:-1]
    weight_parts = ffn1_parts + attn_parts + inner_parts[2:] + inner_parts[:2]
    token_count = (jnp.sum(clips_dev) * SEQ).astype(jnp.float32)
    loss = shared[21] / token_count
    return (
        final_out.astype(jnp.bfloat16),
        loss,
        grad_zero,
        shared[0],
        shared[1],
        weight_parts[0],
        shared[2],
        weight_parts[1],
        shared[3],
        shared[4],
        shared[5],
        weight_parts[2],
        shared[6],
        weight_parts[3],
        weight_parts[4],
        shared[7],
        weight_parts[5],
        shared[8],
        shared[9],
        shared[10],
        shared[11],
        weight_parts[6],
        weight_parts[7],
        shared[12],
        shared[13],
        shared[14],
        weight_parts[8],
        shared[15],
        shared[16],
        weight_parts[9],
        shared[17],
        weight_parts[10],
        shared[18],
        shared[19],
        shared[20],
    )


def solution(mesh):
    in_specs = (
        P("fsdp", ("ctx", "tp"), None),
        P("fsdp", ("ctx", "tp"), None),
        P(),
        P(),
        P(),
        P(("fsdp", "ctx"), "tp"),
        P(),
        P(("fsdp", "ctx"), "tp"),
        P(),
        P(),
        P(),
        P(("fsdp", "ctx"), "tp"),
        P(),
        P(("fsdp", "ctx"), "tp"),
        P(("fsdp", "ctx"), "tp"),
        P(),
        P(("fsdp", "ctx"), "tp"),
        P(),
        P(),
        P(),
        P(),
        P(("fsdp", "ctx"), "tp"),
        P(("fsdp", "ctx"), "tp"),
        P(),
        P(),
        P(),
        P(("fsdp", "ctx"), "tp"),
        P(),
        P(),
        P(("fsdp", "ctx"), "tp"),
        P(),
        P(("fsdp", "ctx"), "tp"),
        P(),
        P(),
        P(),
    )
    out_specs = (
        P("fsdp", ("ctx", "tp"), None),
        P(),
        P("fsdp", ("ctx", "tp"), None),
        P(),
        P(),
        P(("fsdp", "ctx"), "tp"),
        P(),
        P(("fsdp", "ctx"), "tp"),
        P(),
        P(),
        P(),
        P(("fsdp", "ctx"), "tp"),
        P(),
        P(("fsdp", "ctx"), "tp"),
        P(("fsdp", "ctx"), "tp"),
        P(),
        P(("fsdp", "ctx"), "tp"),
        P(),
        P(),
        P(),
        P(),
        P(("fsdp", "ctx"), "tp"),
        P(("fsdp", "ctx"), "tp"),
        P(),
        P(),
        P(),
        P(("fsdp", "ctx"), "tp"),
        P(),
        P(),
        P(("fsdp", "ctx"), "tp"),
        P(),
        P(("fsdp", "ctx"), "tp"),
        P(),
        P(),
        P(),
    )
    return jax.shard_map(body, mesh=mesh, in_specs=in_specs, out_specs=out_specs, check_vma=False)
```

```python
import functools
import math

import jax
import jax.numpy as jnp
from jax import lax
from jax.experimental import pallas as pl
from jax.experimental.pallas import tpu as pltpu
from jax.sharding import PartitionSpec as P

D = 1024
LEFT = 64
HEAD = 64
SEQ = 1536


epsilon = 1e-05


def from_behind(shard, axis, by):
    devices = lax.axis_size(axis)
    pairs = [(i, i + by) for i in range(devices) if 0 <= i + by < devices]
    return lax.ppermute(shard, axis, pairs)


def norm_forward(stream, norm_gain, norm_shift):
    centred = stream - jnp.mean(stream, axis=-1, keepdims=True)
    inverse = lax.rsqrt(jnp.mean(centred * centred, axis=-1, keepdims=True) + epsilon)
    standard = centred * inverse
    return (standard * norm_gain + norm_shift, standard, inverse)


def norm_backward(grad_out, standard, inverse, norm_gain):
    grad_standard = grad_out * norm_gain
    mean_first = jnp.mean(grad_standard, axis=-1, keepdims=True)
    mean_second = jnp.mean(grad_standard * standard, axis=-1, keepdims=True)
    grad_in = inverse * (grad_standard - mean_first - standard * mean_second)
    return (grad_in, jnp.sum(grad_out * standard, axis=(0, 1)), jnp.sum(grad_out, axis=(0, 1)))


def silu_slope(hidden_pre):
    gate_sig = jax.nn.sigmoid(hidden_pre)
    return gate_sig * (1.0 + hidden_pre * (1.0 - gate_sig))


def rows_in(left_reach, right_reach):
    return jnp.einsum("zub,bx->zux", left_reach, right_reach, preferred_element_type=jnp.float32)


def rows_out(left_reach, right_reach):
    return jnp.einsum("anp,op->ano", left_reach, right_reach, preferred_element_type=jnp.float32)


def weight_sum(left_reach, right_reach):
    return jnp.einsum("zbt,zbm->tm", left_reach, right_reach, preferred_element_type=jnp.float32)


def together(*values):
    return lax.optimization_barrier(values)


def widen(normed):
    return lax.all_gather(normed.astype(jnp.bfloat16), "tp", axis=1, tiled=True)


def narrow(partial_rows):
    return lax.psum_scatter(
        partial_rows.astype(jnp.bfloat16), "tp", scatter_dimension=1, tiled=True
    ).astype(jnp.float32)


def widen_grad(grad_branch):
    return lax.all_gather(grad_branch, "tp", axis=1, tiled=True)


def narrow_grad(partial_rows):
    return lax.psum_scatter(
        partial_rows.astype(jnp.bfloat16), "tp", scatter_dimension=1, tiled=True
    ).astype(jnp.float32)


def local_cut(full_array, tp_rank, size_local):
    return lax.dynamic_slice_in_dim(
        full_array, tp_rank * size_local, size_local, full_array.ndim - 1
    )


def local_put(local_array, tp_rank, full_size):
    shape_full = local_array.shape[:-1] + (full_size,)
    return lax.dynamic_update_slice_in_dim(
        jnp.zeros(shape_full, jnp.float32),
        local_array,
        tp_rank * local_array.shape[-1],
        local_array.ndim - 1,
    )


BAND = 384


def wide_table(rel_table):
    before = jnp.broadcast_to(rel_table[:1], (LEFT, HEAD))
    after = jnp.broadcast_to(rel_table[-1:], (BAND - LEFT - rel_table.shape[0], HEAD))
    return jnp.concatenate([before, rel_table, after], axis=0)


def dot_t(left, right):
    return lax.dot_general(left, right, (((1,), (1,)), ((), ())), preferred_element_type=jnp.float32)


def dot_n(left, right):
    return lax.dot_general(left, right, (((1,), (0,)), ((), ())), preferred_element_type=jnp.float32)


def scaled_scores(query_block, keys, table, place, rows_at, reach):
    rows = query_block.shape[0]
    key_count = keys.shape[0]
    near = dot_t(query_block, table)
    left, right = near[:, :1], near[:, BAND - 1 :]
    row = lax.broadcasted_iota(jnp.int32, (rows, key_count), 0)
    col = lax.broadcasted_iota(jnp.int32, (rows, key_count), 1)
    place[:, 128 : 128 + key_count] = dot_t(query_block, keys) + jnp.where(
        col < row + rows_at, left, right
    )
    rolled = pltpu.roll(near, 0, 1, stride=1, stride_axis=0)
    apart = band_distance(rows)
    band = jnp.where(apart <= -LEFT, left, jnp.where(apart >= reach, right, rolled))
    window = pl.ds(pl.multiple_of(rows_at, 128), BAND)
    place[:, window] += band - jnp.where(apart < 0, left, right)
    return place[:, 128 : 128 + key_count]


def band_distance(rows):
    row = lax.broadcasted_iota(jnp.int32, (rows, BAND), 0)
    col = lax.broadcasted_iota(jnp.int32, (rows, BAND), 1)
    return col - 128 - row


def attend_kernel(reach, start_ref, query_ref, key_ref, value_ref, table_ref, mixed_ref, probs_ref, place):
    rows = query_ref.shape[1]
    rows_at = start_ref[0] + pl.program_id(2) * rows
    table = table_ref[...]
    for half in range(query_ref.shape[2] // HEAD):
        lanes = slice(half * HEAD, (half + 1) * HEAD)
        query_block = query_ref[0, :, lanes] * jnp.bfloat16(1.0 / math.sqrt(HEAD))
        scores = scaled_scores(query_block, key_ref[0, :, lanes], table, place, rows_at, reach)
        top = jnp.max(scores, axis=-1, keepdims=True)
        powers = jnp.exp(scores - top)
        row_sum = jnp.sum(powers, axis=-1, keepdims=True)
        probs = (powers * (1.0 / row_sum)).astype(jnp.bfloat16)
        mixed_ref[0, :, lanes] = dot_n(probs, value_ref[0, :, lanes]).astype(jnp.bfloat16)
        probs_ref[0, half] = probs


def attend_back_kernel(
    reach, start_ref, query_ref, key_ref, value_ref, table_ref, probs_ref, grad_ref, groups_ref,
    query_grad_ref, pair_grad_ref, table_grad_ref, place, key_sum, value_sum,
):
    rows = query_ref.shape[1]
    key_count = key_ref.shape[1]
    block = pl.program_id(2)
    rows_at = start_ref[0] + block * rows
    table = table_ref[...]
    scale = jnp.bfloat16(1.0 / math.sqrt(HEAD))

    @pl.when(block == 0)
    def _():
        key_sum[...] = jnp.zeros_like(key_sum)
        value_sum[...] = jnp.zeros_like(value_sum)

    @pl.when((block == 0) & (pl.program_id(0) == 0) & (pl.program_id(1) == 0))
    def _():
        table_grad_ref[...] = jnp.zeros_like(table_grad_ref)

    for half in range(query_ref.shape[2] // HEAD):
        lanes = slice(half * HEAD, (half + 1) * HEAD)
        query_block = query_ref[0, :, lanes] * scale
        keys = key_ref[0, :, lanes]
        grad_block = grad_ref[0, :, lanes]
        probs_low = probs_ref[0, half]
        probs = probs_low.astype(jnp.float32)
        grad_probs = dot_t(grad_block, value_ref[0, :, lanes])
        row_dot = jnp.sum(probs * grad_probs, axis=-1, keepdims=True)
        grad_scores = (probs * (grad_probs - row_dot)).astype(jnp.bfloat16)
        value_sum[lanes, :] += dot_n(grad_block.T, probs_low)
        key_sum[lanes, :] += dot_n(query_block.T, grad_scores)
        wide = grad_scores.astype(jnp.float32)
        place[:, 128 : 128 + key_count] = wide
        window = place[:, pl.ds(pl.multiple_of(rows_at, 128), BAND)]
        window_col = lax.broadcasted_iota(jnp.int32, window.shape, 1) + rows_at - 128
        window = jnp.where((window_col >= 0) & (window_col < key_count), window, 0.0)
        apart = band_distance(rows)
        by_group = dot_n(grad_scores, groups_ref[...])
        past = lax.broadcasted_iota(jnp.int32, by_group.shape, 1) * 128 - rows_at
        far_left = jnp.sum(jnp.where(past < -128, by_group, 0.0), axis=-1, keepdims=True)
        far_left += jnp.sum(jnp.where(apart <= -LEFT, window, 0.0), axis=-1, keepdims=True)
        far_right = jnp.sum(jnp.where(past >= BAND - 128, by_group, 0.0), axis=-1, keepdims=True)
        far_right += jnp.sum(jnp.where(apart >= reach, window, 0.0), axis=-1, keepdims=True)
        inside = (apart > -LEFT) & (apart < reach)
        turned = jnp.where(inside, window, 0.0)
        row = lax.broadcasted_iota(jnp.int32, turned.shape, 0)
        for bit in range((rows - 1).bit_length()):
            moved = pltpu.roll(turned, BAND - (1 << bit), 1)
            turned = jnp.where(((row >> bit) & 1) == 1, moved, turned)
        lane = lax.broadcasted_iota(jnp.int32, turned.shape, 1)
        by_row = jnp.where(lane == LEFT, far_left, jnp.where(lane == 2 * LEFT + reach, far_right, turned))
        coarse = by_row.astype(jnp.bfloat16)
        fine = (by_row - coarse.astype(jnp.float32)).astype(jnp.bfloat16)
        query_grad = dot_n(grad_scores, keys) + dot_n(coarse, table) + dot_n(fine, table)
        query_grad_ref[0, :, lanes] = (query_grad * (1.0 / math.sqrt(HEAD))).astype(jnp.bfloat16)
        query_turned = query_block.T
        table_grad_ref[...] += dot_n(query_turned, coarse) + dot_n(query_turned, fine)

    @pl.when(block == pl.num_programs(2) - 1)
    def _():
        pair_grad_ref[0, 0] = key_sum[...].T.astype(jnp.bfloat16)
        pair_grad_ref[1, 0] = value_sum[...].T.astype(jnp.bfloat16)


def attend_specs(queries, keys):
    slots, rows, width = queries.shape
    lanes = 2 * HEAD
    block = 128
    grid = (slots, width // lanes, rows // block)
    by_query = pl.BlockSpec((1, block, lanes), lambda s, p, b, *_: (s, b, p))
    by_key = pl.BlockSpec((1, keys.shape[1], lanes), lambda s, p, b, *_: (s, 0, p))
    by_value = pl.BlockSpec(
        (1, keys.shape[1], lanes), lambda s, p, b, *_: (s, 0, p + width // lanes)
    )
    table = pl.BlockSpec((BAND, HEAD), lambda s, p, b, *_: (0, 0))
    place = pltpu.VMEM((block, keys.shape[1] + 256), jnp.float32)
    flops = slots * rows * keys.shape[1] * width * 4
    by_prob = pl.BlockSpec((1, 2, block, keys.shape[1]), lambda s, p, b, *_: (s, p, b, 0))
    return grid, by_query, by_key, by_value, by_prob, table, place, flops


def attend(queries, pairs, table, reach, query_start):
    grid, by_query, by_key, by_value, by_prob, by_table, place, flops = attend_specs(queries, pairs)
    return pl.pallas_call(
        functools.partial(attend_kernel, reach),
        out_shape=(
            jax.ShapeDtypeStruct(queries.shape, jnp.bfloat16),
            jax.ShapeDtypeStruct(
                queries.shape[:1] + (queries.shape[2] // HEAD, queries.shape[1], pairs.shape[1]),
                jnp.bfloat16,
            ),
        ),
        grid_spec=pltpu.PrefetchScalarGridSpec(
            num_scalar_prefetch=1,
            grid=grid,
            in_specs=[by_query, by_key, by_value, by_table],
            out_specs=(by_query, by_prob),
            scratch_shapes=[place],
        ),
        cost_estimate=pl.CostEstimate(flops=2 * flops, bytes_accessed=8 << 20, transcendentals=flops >> 8),
        name="attend",
    )(query_start.reshape(1), queries, pairs, pairs, table)


def attend_back(queries, pairs, table, totals, grad_mixed, reach, query_start):
    grid, by_query, by_key, by_value, by_prob, by_table, place, flops = attend_specs(queries, pairs)
    slots, key_count = pairs.shape[:2]
    turned = pltpu.VMEM((2 * HEAD, key_count), jnp.float32)
    group = jnp.arange(key_count, dtype=jnp.int32)[:, None] // 128
    groups = (group == jnp.arange(128, dtype=jnp.int32)[None, :]).astype(jnp.bfloat16)
    return pl.pallas_call(
        functools.partial(attend_back_kernel, reach),
        out_shape=(
            jax.ShapeDtypeStruct(queries.shape, jnp.bfloat16),
            jax.ShapeDtypeStruct((2, slots, key_count, queries.shape[2]), jnp.bfloat16),
            jax.ShapeDtypeStruct((HEAD, BAND), jnp.float32),
        ),
        grid_spec=pltpu.PrefetchScalarGridSpec(
            num_scalar_prefetch=1,
            grid=grid,
            in_specs=[
                by_query,
                by_key,
                by_value,
                by_table,
                by_prob,
                by_query,
                pl.BlockSpec((key_count, 128), lambda s, p, b, *_: (0, 0)),
            ],
            out_specs=(
                by_query,
                pl.BlockSpec((2, 1, key_count, 2 * HEAD), lambda s, p, b, *_: (0, s, 0, p)),
                pl.BlockSpec((HEAD, BAND), lambda s, p, b, *_: (0, 0)),
            ),
            scratch_shapes=[place, turned, turned],
        ),
        cost_estimate=pl.CostEstimate(flops=5 * flops, bytes_accessed=16 << 20, transcendentals=flops >> 8),
        name="attend_back",
    )(query_start.reshape(1), queries, pairs, pairs, table, totals, grad_mixed, groups)


def ffn_forward(stream, norm_gain, norm_shift, weight_in, bias_in, weight_out, bias_out):
    normed, standard, inverse = norm_forward(stream, norm_gain, norm_shift)
    wide_rows = widen(normed)
    hidden_pre = rows_in(wide_rows, weight_in) + bias_in
    active = jax.nn.silu(hidden_pre).astype(jnp.bfloat16)
    branch = narrow(rows_out(active, weight_out)) + bias_out
    return (stream + 0.5 * branch, (standard, inverse, wide_rows, hidden_pre))


def ffn_forward_first(
    stream, norm_gain, norm_shift, shard_in, bias_in, shard_out, bias_out, later_shards
):
    normed, standard, inverse = norm_forward(stream, norm_gain, norm_shift)
    normed, shard_in = together(normed.astype(jnp.bfloat16), shard_in)
    wide_rows = widen(normed)
    pieces = [
        gather_rows(shard_in[:, start : start + 256]) for start in range(0, shard_in.shape[1], 256)
    ]
    wide_rows, shard_out, *pieces = together(wide_rows, shard_out, *pieces)
    weight_out = gather_rows(shard_out)
    weight_in = jnp.concatenate(pieces, axis=1)
    hidden_pre = rows_in(wide_rows, weight_in) + bias_in
    active = jax.nn.silu(hidden_pre).astype(jnp.bfloat16)
    partial_rows = rows_out(active, weight_out).astype(jnp.bfloat16)
    partial_rows, *later_shards = together(partial_rows, *later_shards)
    later = [gather_rows(shard) for shard in later_shards]
    summed = lax.psum_scatter(partial_rows, "tp", scatter_dimension=1, tiled=True)
    summed, *later = together(summed, *later)
    branch = summed.astype(jnp.float32) + bias_out
    saved = (standard, inverse, wide_rows, hidden_pre)
    return (stream + 0.5 * branch, saved, weight_in, weight_out, later)


def ffn_backward(grad_stream, saved, norm_gain, weight_in, weight_out, beside=None):
    standard, inverse, wide_rows, hidden_pre = saved
    grad_branch = (0.5 * grad_stream).astype(jnp.bfloat16)
    out_bias_grad = jnp.sum(grad_branch.astype(jnp.float32), axis=(0, 1))
    wide_grad = widen_grad(grad_branch)
    if beside is not None:
        wide_grad, beside = together(wide_grad, beside)
        beside = lax.psum_scatter(beside, ("fsdp", "ctx"), scatter_dimension=0, tiled=True)
    active = jax.nn.silu(hidden_pre).astype(jnp.bfloat16)
    out_grad = weight_sum(wide_grad, active)
    grad_pre = (rows_in(wide_grad, weight_out) * silu_slope(hidden_pre)).astype(jnp.bfloat16)
    in_bias_grad = jnp.sum(grad_pre.astype(jnp.float32), axis=(0, 1))
    in_grad = weight_sum(wide_rows, grad_pre)
    partial_rows = rows_out(grad_pre, weight_in).astype(jnp.bfloat16)
    if beside is not None:
        partial_rows, beside = together(partial_rows, beside)
    grad_normed = narrow_grad(partial_rows)
    grad_normed, in_grad, out_grad = together(grad_normed, in_grad, out_grad)
    grad_in, gain_grad, shift_grad = norm_backward(grad_normed, standard, inverse, norm_gain)
    return (
        grad_stream + grad_in,
        (gain_grad, shift_grad, in_grad, in_bias_grad, out_grad, out_bias_grad),
        beside,
    )


def attn_forward(stream, norm_gain, norm_shift, weights, biases, rel_table, ctx_rank, late_shard):
    query_w, key_w, value_w, out_w = weights
    query_b, value_b, out_b = biases
    normed, standard, inverse = norm_forward(stream, norm_gain, norm_shift)
    wide_rows = widen(normed)
    queries = (rows_in(wide_rows, query_w) + query_b).astype(jnp.bfloat16)
    pair_b = jnp.concatenate([jnp.zeros_like(value_b), value_b])
    pair_w = jnp.concatenate([key_w, value_w], axis=1)
    pairs = (rows_in(wide_rows, pair_w) + pair_b).astype(jnp.bfloat16)
    pairs_all = lax.all_gather(pairs, "ctx", axis=1, tiled=True)
    pairs_all, late_shard = together(pairs_all, late_shard)
    late = gather_rows(late_shard)
    reach = rel_table.shape[0] - 1 - LEFT
    mixed_token_rows, log_total = attend(
        queries, pairs_all, wide_table(rel_table), reach, ctx_rank * queries.shape[1]
    )
    mixed_token_rows, late = together(mixed_token_rows, late)
    branch = narrow(rows_out(mixed_token_rows, out_w)) + out_b
    return (
        stream + branch,
        (standard, inverse, wide_rows, queries, pairs_all, mixed_token_rows, log_total),
        late,
    )


def attn_backward(grad_stream, saved, norm_gain, weights, rel_table, ctx_rank, inner_grads):
    query_w, key_w, value_w, out_w = weights
    standard, inverse, wide_rows, queries, pairs_all, mixed_token_rows, log_total = saved
    grad_branch = grad_stream.astype(jnp.bfloat16)
    out_bias_grad = jnp.sum(grad_branch.astype(jnp.float32), axis=(0, 1))
    inner = jnp.concatenate([grad.astype(jnp.bfloat16) for grad in inner_grads], axis=1)
    wide_grad, inner = together(widen_grad(grad_branch), inner)
    inner = lax.psum_scatter(inner, ("fsdp", "ctx"), scatter_dimension=0, tiled=True)
    grad_mixed = rows_in(wide_grad, out_w).astype(jnp.bfloat16)
    reach = rel_table.shape[0] - 1 - LEFT
    query_low, pair_terms, table_turned = attend_back(
        queries,
        pairs_all,
        wide_table(rel_table),
        log_total,
        grad_mixed,
        reach,
        ctx_rank * queries.shape[1],
    )
    query_low, pair_terms, inner = together(query_low, pair_terms, inner)
    out_grad = weight_sum(wide_grad, mixed_token_rows)
    inner_parts = split_columns(inner, inner_grads)
    table_grad = table_turned[:, LEFT : LEFT + rel_table.shape[0]].T
    pair_low = lax.psum_scatter(pair_terms, "ctx", scatter_dimension=2, tiled=True)
    key_low, value_low = pair_low[0], pair_low[1]
    query_bias_grad = jnp.sum(query_low.astype(jnp.float32), axis=(0, 1))
    value_bias_grad = jnp.sum(value_low.astype(jnp.float32), axis=(0, 1))
    query_w_grad = weight_sum(wide_rows, query_low)
    key_w_grad = weight_sum(wide_rows, key_low)
    value_w_grad = weight_sum(wide_rows, value_low)
    grad_normed = narrow_grad(
        rows_out(query_low, query_w) + rows_out(key_low, key_w) + rows_out(value_low, value_w)
    )
    grad_normed, out_grad, query_w_grad, key_w_grad, value_w_grad = together(
        grad_normed, out_grad, query_w_grad, key_w_grad, value_w_grad
    )
    grad_in, gain_grad, shift_grad = norm_backward(grad_normed, standard, inverse, norm_gain)
    return (
        grad_stream + grad_in,
        (
            gain_grad,
            shift_grad,
            query_w_grad,
            query_bias_grad,
            key_w_grad,
            value_w_grad,
            value_bias_grad,
            out_grad,
            out_bias_grad,
            table_grad,
        ),
        inner_parts,
    )


def sum_rows(first, second):
    every = lax.all_gather(jnp.stack([first, second]), "tp", axis=0, tiled=False)
    return jnp.sum(every, axis=0)


def conv_forward(stream, norm_gain, norm_shift, weights, depth_local, inner_gain, inner_offset):
    value_w, gate_w, out_w = weights
    normed, standard, inverse = norm_forward(stream, norm_gain, norm_shift)
    wide_rows = widen(normed)
    part_value = rows_in(wide_rows, value_w)
    part_gate = rows_in(wide_rows, gate_w)
    gated_rows = (part_value * jax.nn.sigmoid(part_gate)).astype(jnp.bfloat16)
    row_count = gated_rows.shape[1]
    reach_rows = depth_local.shape[0] - 1
    halo_rows = from_behind(gated_rows[:, row_count - reach_rows :, :], "ctx", 1)
    padded = jnp.concatenate([halo_rows, gated_rows], axis=1)
    padded_float = padded.astype(jnp.float32)
    convolved = depth_local[0] * padded_float[:, 0:row_count, :]
    for tap_index in range(1, depth_local.shape[0]):
        convolved = (
            convolved
            + depth_local[tap_index] * padded_float[:, tap_index : tap_index + row_count, :]
        )
    row_sums = sum_rows(jnp.sum(convolved, axis=-1), jnp.sum(convolved * convolved, axis=-1))
    row_mean = (row_sums[0] / D)[..., None]
    row_var = (row_sums[1] / D)[..., None] - row_mean * row_mean
    inner_inverse = lax.rsqrt(row_var + epsilon)
    inner_standard = (convolved - row_mean) * inner_inverse
    inner_pre = inner_standard * inner_gain + inner_offset
    active = jax.nn.silu(inner_pre).astype(jnp.bfloat16)
    branch = narrow(rows_out(active, out_w))
    return (
        stream + branch,
        (
            standard,
            inverse,
            wide_rows,
            part_value,
            part_gate,
            padded,
            inner_standard,
            inner_inverse,
            inner_pre,
        ),
    )


def taps_back_kernel(depth_ref, grad_ref, padded_ref, gated_ref, depth_grad_ref, wide):
    taps = depth_ref.shape[0]
    rows, width = gated_ref.shape[1:]
    step = 64

    @pl.when(pl.program_id(0) == 0)
    def _():
        depth_grad_ref[...] = jnp.zeros_like(depth_grad_ref)

    wide[: padded_ref.shape[1], :] = padded_ref[0].astype(jnp.float32)
    for lane in range(0, width, 128):
        lanes = slice(lane, lane + 128)
        for start in range(0, rows, step):
            own = grad_ref[0, start : start + step, lanes]
            total = jnp.zeros((step, 128), jnp.float32)
            for tap in range(taps):
                first = start + taps - 1 - tap
                total += depth_ref[tap : tap + 1, lanes] * grad_ref[0, first : first + step, lanes]
                product = own * wide[start + tap : start + tap + step, lanes]
                depth_grad_ref[8 * tap : 8 * tap + 8, lanes] += jnp.sum(
                    product.reshape(step // 8, 8, 128), axis=0
                )
            gated_ref[0, start : start + step, lanes] = total


def taps_back(grad_conv, ahead, padded, depth_local):
    slots, rows, width = grad_conv.shape
    taps = depth_local.shape[0]
    spare = -(rows + taps - 1) % 8
    reach = jnp.concatenate(
        [grad_conv, ahead, jnp.zeros((slots, spare, width), jnp.float32)], axis=1
    )
    held = jnp.pad(padded, ((0, 0), (0, spare), (0, 0)))
    by_slot = lambda count: pl.BlockSpec((1, count, width), lambda s: (s, 0, 0))
    gated, depth_sums = pl.pallas_call(
        taps_back_kernel,
        out_shape=(
            jax.ShapeDtypeStruct((slots, rows, width), jnp.float32),
            jax.ShapeDtypeStruct((8 * taps, width), jnp.float32),
        ),
        grid=(slots,),
        in_specs=[
            pl.BlockSpec((taps, width), lambda s: (0, 0)),
            by_slot(reach.shape[1]),
            by_slot(held.shape[1]),
        ],
        out_specs=(by_slot(rows), pl.BlockSpec((8 * taps, width), lambda s: (0, 0))),
        scratch_shapes=[pltpu.VMEM((held.shape[1], width), jnp.float32)],
        cost_estimate=pl.CostEstimate(
            flops=4 * taps * slots * rows * width, bytes_accessed=4 << 20, transcendentals=0
        ),
        name="taps_back",
    )(depth_local, reach, held)
    return gated, jnp.sum(depth_sums.reshape(taps, 8, width), axis=1)


def conv_backward(grad_stream, saved, norm_gain, weights, depth_local, inner_gain):
    value_w, gate_w, out_w = weights
    (
        standard,
        inverse,
        wide_rows,
        part_value,
        part_gate,
        padded,
        inner_standard,
        inner_inverse,
        inner_pre,
    ) = saved
    grad_branch = grad_stream.astype(jnp.bfloat16)
    wide_grad = widen_grad(grad_branch)
    active = jax.nn.silu(inner_pre).astype(jnp.bfloat16)
    out_grad = weight_sum(wide_grad, active)
    grad_inner = rows_in(wide_grad, out_w) * silu_slope(inner_pre)
    inner_gain_grad = jnp.sum(grad_inner * inner_standard, axis=(0, 1))
    inner_shift_grad = jnp.sum(grad_inner, axis=(0, 1))
    grad_standard = grad_inner * inner_gain
    row_sums = sum_rows(
        jnp.sum(grad_standard, axis=-1), jnp.sum(grad_standard * inner_standard, axis=-1)
    )
    grad_conv = inner_inverse * (
        grad_standard - (row_sums[0] / D)[..., None] - inner_standard * (row_sums[1] / D)[..., None]
    )
    row_count = grad_conv.shape[1]
    tap_count = depth_local.shape[0]
    reach_rows = tap_count - 1
    ahead = from_behind(grad_conv[:, :reach_rows, :].astype(jnp.bfloat16), "ctx", -1)
    grad_gated, depth_grad = taps_back(grad_conv, ahead.astype(jnp.float32), padded, depth_local)
    gate_sig = jax.nn.sigmoid(part_gate)
    grad_value = (grad_gated * gate_sig).astype(jnp.bfloat16)
    grad_gate = (grad_gated * part_value * gate_sig * (1.0 - gate_sig)).astype(jnp.bfloat16)
    value_w_grad = weight_sum(wide_rows, grad_value)
    gate_w_grad = weight_sum(wide_rows, grad_gate)
    grad_normed = narrow_grad(rows_out(grad_value, value_w) + rows_out(grad_gate, gate_w))
    grad_normed, out_grad, value_w_grad, gate_w_grad = together(
        grad_normed, out_grad, value_w_grad, gate_w_grad
    )
    grad_in, gain_grad, shift_grad = norm_backward(grad_normed, standard, inverse, norm_gain)
    return (
        grad_stream + grad_in,
        (
            gain_grad,
            shift_grad,
            value_w_grad,
            gate_w_grad,
            depth_grad,
            inner_gain_grad,
            inner_shift_grad,
            out_grad,
        ),
    )


def gather_rows(shard):
    return lax.all_gather(shard, ("fsdp", "ctx"), axis=0, tiled=True)


def scatter_sum(*grads):
    joined = jnp.concatenate([grad.astype(jnp.bfloat16) for grad in grads], axis=1)
    part = lax.psum_scatter(joined, ("fsdp", "ctx"), scatter_dimension=0, tiled=True)
    return split_columns(part, grads)


def split_columns(part, grads):
    pieces = []
    start = 0
    for grad in grads:
        pieces.append(part[:, start : start + grad.shape[1]].astype(jnp.float32))
        start += grad.shape[1]
    return tuple(pieces)


def small_columns(whole_parts, split_parts, rows):
    flat = jnp.concatenate([part.reshape(-1) for part in whole_parts + split_parts])
    columns = -(-flat.shape[0] // rows)
    flat = jnp.pad(flat, (0, rows * columns - flat.shape[0])).reshape(rows, columns)
    return jnp.pad(flat, ((0, 0), (0, -columns % 128)))


def finish_small(small, whole_parts, split_parts, own_parts, hidden_part):
    rows = small.shape[0] * lax.axis_size(("fsdp", "ctx"))
    count = sum(part.size for part in whole_parts + split_parts)
    small = small[:, : -(-count // rows)].astype(jnp.float32).reshape(-1)
    held = small.shape[0]
    sent = jnp.concatenate(
        [small] + [part.reshape(-1) for part in own_parts] + [hidden_part.reshape(-1)]
    )
    sent = jnp.pad(sent, (0, -sent.shape[0] % 128)).reshape(1, -1, 128)
    tp_count = lax.axis_size("tp")
    every = lax.all_gather(sent, "tp", axis=0, tiled=True)
    every = lax.all_gather(every, ("fsdp", "ctx"), axis=0, tiled=True)
    every = every.reshape(-1, tp_count, sent.size)
    by_tp = every[:, :, :held].transpose(1, 0, 2).reshape(tp_count, -1)
    total = jnp.sum(by_tp, axis=0)
    spread = by_tp
    whole = []
    start = 0
    for part in whole_parts:
        whole.append(total[start : start + part.size].reshape(part.shape))
        start += part.size
    pieces = []
    for part in split_parts:
        piece = spread[:, start : start + part.size]
        if part.ndim == 1:
            pieces.append(piece.reshape(-1))
        else:
            piece = piece.reshape((tp_count,) + part.shape)
            pieces.append(piece.transpose(1, 0, 2).reshape(part.shape[0], -1))
        start += part.size
    own = jnp.sum(every[:, :, held:], axis=0)
    owned = []
    start = 0
    for part in own_parts:
        owned.append(jnp.sum(own[:, start : start + part.size], axis=0).reshape(part.shape))
        start += part.size
    hidden = own[:, start : start + hidden_part.size].reshape(-1)
    w, p = whole, pieces
    return (
        owned[0], owned[1], hidden, owned[2], w[0], w[1], p[0], p[1], w[2], w[3], w[4], w[5],
        p[2], p[3], p[4], w[6], w[7], p[5], w[8], w[9], w[10], owned[3],
    )


def body(
    inputs,
    teacher,
    clips_dev,
    ffn1_gain,
    ffn1_shift,
    ffn1_in,
    ffn1_in_bias,
    ffn1_out,
    ffn1_out_bias,
    attn_gain,
    attn_shift,
    query_weight,
    query_bias,
    key_weight,
    value_weight,
    value_bias,
    attn_out_weight,
    attn_out_bias,
    rel_table,
    conv_gain,
    conv_shift,
    conv_value_weight,
    conv_gate_weight,
    conv_depth,
    conv_inner_gain,
    conv_inner_shift,
    conv_out_weight,
    ffn2_gain,
    ffn2_shift,
    ffn2_in,
    ffn2_in_bias,
    ffn2_out,
    ffn2_out_bias,
    final_gain,
    final_shift,
):
    width = query_weight.shape[1]
    late_shard = jnp.concatenate(
        [ffn2_in, ffn2_out, conv_value_weight, conv_gate_weight, conv_out_weight], axis=1
    )
    tp_rank = lax.axis_index("tp")
    ctx_rank = lax.axis_index("ctx")
    hidden_local = ffn1_in.shape[1]
    width_local = width
    ffn1_bias_local = local_cut(ffn1_in_bias, tp_rank, hidden_local)
    ffn2_bias_local = local_cut(ffn2_in_bias, tp_rank, hidden_local)
    query_bias_local = local_cut(query_bias, tp_rank, width_local)
    value_bias_local = local_cut(value_bias, tp_rank, width_local)
    depth_local = local_cut(conv_depth, tp_rank, width_local)
    inner_gain_local = local_cut(conv_inner_gain, tp_rank, width_local)
    inner_shift_local = local_cut(conv_inner_shift, tp_rank, width_local)
    stream_zero = inputs.astype(jnp.float32)
    stream_one, saved_one, ffn1_in_all, ffn1_out_all, attn_weights = ffn_forward_first(
        stream_zero,
        ffn1_gain,
        ffn1_shift,
        ffn1_in,
        ffn1_bias_local,
        ffn1_out,
        ffn1_out_bias,
        (query_weight, key_weight, value_weight, attn_out_weight),
    )
    stream_two, saved_two, late = attn_forward(
        stream_one,
        attn_gain,
        attn_shift,
        attn_weights,
        (query_bias_local, value_bias_local, attn_out_bias),
        rel_table,
        ctx_rank,
        late_shard,
    )
    ffn2_in_all = late[:, :hidden_local]
    ffn2_out_all = late[:, hidden_local : 2 * hidden_local]
    conv_all = late[:, 2 * hidden_local :]
    conv_weights = (
        conv_all[:, :width],
        conv_all[:, width : 2 * width],
        conv_all[:, 2 * width :],
    )
    stream_three, saved_three = conv_forward(
        stream_two,
        conv_gain,
        conv_shift,
        conv_weights,
        depth_local,
        inner_gain_local,
        inner_shift_local,
    )
    stream_four, saved_four = ffn_forward(
        stream_three,
        ffn2_gain,
        ffn2_shift,
        ffn2_in_all,
        ffn2_bias_local,
        ffn2_out_all,
        ffn2_out_bias,
    )
    final_out, final_standard, final_inverse = norm_forward(stream_four, final_gain, final_shift)
    live_slots = (
        jnp.arange(final_out.shape[0], dtype=jnp.int32) < clips_dev[lax.axis_index("fsdp")]
    ).astype(jnp.float32)
    misfit = (final_out - teacher.astype(jnp.float32)) * live_slots[:, None, None]
    sse_local = jnp.sum(misfit * misfit)
    gradient_fourth, final_gain_grad, final_shift_grad = norm_backward(
        2.0 * misfit, final_standard, final_inverse, final_gain
    )
    grad_three, ffn2_grads, _ = ffn_backward(
        gradient_fourth, saved_four, ffn2_gain, ffn2_in_all, ffn2_out_all
    )
    grad_two, conv_grads = conv_backward(
        grad_three,
        saved_three,
        conv_gain,
        conv_weights,
        depth_local,
        inner_gain_local,
    )
    grad_one, attn_grads, inner_parts = attn_backward(
        grad_two,
        saved_two,
        attn_gain,
        attn_weights,
        rel_table,
        ctx_rank,
        (ffn2_grads[2], ffn2_grads[4], conv_grads[2], conv_grads[3], conv_grads[7]),
    )
    attn_mats = (attn_grads[2], attn_grads[4], attn_grads[5], attn_grads[7])
    whole_parts = (
        attn_grads[0],
        attn_grads[1],
        attn_grads[8],
        attn_grads[9],
        conv_grads[0],
        conv_grads[1],
        ffn2_grads[0],
        ffn2_grads[1],
        ffn2_grads[5],
        final_gain_grad,
        final_shift_grad,
    )
    split_parts = (
        attn_grads[3],
        attn_grads[6],
        conv_grads[4],
        conv_grads[5],
        conv_grads[6],
        ffn2_grads[3],
    )
    columns = small_columns(whole_parts, split_parts, attn_mats[0].shape[0])
    beside_mats = attn_mats + (columns,)
    beside = jnp.concatenate([part.astype(jnp.bfloat16) for part in beside_mats], axis=1)
    grad_zero, ffn1_grads, beside = ffn_backward(
        grad_one, saved_one, ffn1_gain, ffn1_in_all, ffn1_out_all, beside
    )
    attn_parts = split_columns(beside, beside_mats)
    ffn1_parts = scatter_sum(ffn1_grads[2], ffn1_grads[4])
    shared = finish_small(
        attn_parts[-1],
        whole_parts,
        split_parts,
        (ffn1_grads[0], ffn1_grads[1], ffn1_grads[5], sse_local),
        ffn1_grads[3],
    )
    attn_parts = attn_parts[:-1]
    weight_parts = ffn1_parts + attn_parts + inner_parts[2:] + inner_parts[:2]
    token_count = (jnp.sum(clips_dev) * SEQ).astype(jnp.float32)
    loss = shared[21] / token_count
    return (
        final_out.astype(jnp.bfloat16),
        loss,
        grad_zero,
        shared[0],
        shared[1],
        weight_parts[0],
        shared[2],
        weight_parts[1],
        shared[3],
        shared[4],
        shared[5],
        weight_parts[2],
        shared[6],
        weight_parts[3],
        weight_parts[4],
        shared[7],
        weight_parts[5],
        shared[8],
        shared[9],
        shared[10],
        shared[11],
        weight_parts[6],
        weight_parts[7],
        shared[12],
        shared[13],
        shared[14],
        weight_parts[8],
        shared[15],
        shared[16],
        weight_parts[9],
        shared[17],
        weight_parts[10],
        shared[18],
        shared[19],
        shared[20],
    )


def solution(mesh):
    in_specs = (
        P("fsdp", ("ctx", "tp"), None),
        P("fsdp", ("ctx", "tp"), None),
        P(),
        P(),
        P(),
        P(("fsdp", "ctx"), "tp"),
        P(),
        P(("fsdp", "ctx"), "tp"),
        P(),
        P(),
        P(),
        P(("fsdp", "ctx"), "tp"),
        P(),
        P(("fsdp", "ctx"), "tp"),
        P(("fsdp", "ctx"), "tp"),
        P(),
        P(("fsdp", "ctx"), "tp"),
        P(),
        P(),
        P(),
        P(),
        P(("fsdp", "ctx"), "tp"),
        P(("fsdp", "ctx"), "tp"),
        P(),
        P(),
        P(),
        P(("fsdp", "ctx"), "tp"),
        P(),
        P(),
        P(("fsdp", "ctx"), "tp"),
        P(),
        P(("fsdp", "ctx"), "tp"),
        P(),
        P(),
        P(),
    )
    out_specs = (
        P("fsdp", ("ctx", "tp"), None),
        P(),
        P("fsdp", ("ctx", "tp"), None),
        P(),
        P(),
        P(("fsdp", "ctx"), "tp"),
        P(),
        P(("fsdp", "ctx"), "tp"),
        P(),
        P(),
        P(),
        P(("fsdp", "ctx"), "tp"),
        P(),
        P(("fsdp", "ctx"), "tp"),
        P(("fsdp", "ctx"), "tp"),
        P(),
        P(("fsdp", "ctx"), "tp"),
        P(),
        P(),
        P(),
        P(),
        P(("fsdp", "ctx"), "tp"),
        P(("fsdp", "ctx"), "tp"),
        P(),
        P(),
        P(),
        P(("fsdp", "ctx"), "tp"),
        P(),
        P(),
        P(("fsdp", "ctx"), "tp"),
        P(),
        P(("fsdp", "ctx"), "tp"),
        P(),
        P(),
        P(),
    )
    return jax.shard_map(body, mesh=mesh, in_specs=in_specs, out_specs=out_specs, check_vma=False)
```

```python
import functools
import math

import jax
import jax.numpy as jnp
from jax import lax
from jax.experimental import pallas as pl
from jax.experimental.pallas import tpu as pltpu
from jax.sharding import PartitionSpec as P

D = 1024
LEFT = 64
HEAD = 64
SEQ = 1536


epsilon = 1e-05


def from_behind(shard, axis, by):
    devices = lax.axis_size(axis)
    pairs = [(i, i + by) for i in range(devices) if 0 <= i + by < devices]
    return lax.ppermute(shard, axis, pairs)


def norm_forward(stream, norm_gain, norm_shift):
    centred = stream - jnp.mean(stream, axis=-1, keepdims=True)
    inverse = lax.rsqrt(jnp.mean(centred * centred, axis=-1, keepdims=True) + epsilon)
    standard = centred * inverse
    return (standard * norm_gain + norm_shift, standard, inverse)


def norm_backward(grad_out, standard, inverse, norm_gain):
    grad_standard = grad_out * norm_gain
    mean_first = jnp.mean(grad_standard, axis=-1, keepdims=True)
    mean_second = jnp.mean(grad_standard * standard, axis=-1, keepdims=True)
    grad_in = inverse * (grad_standard - mean_first - standard * mean_second)
    return (grad_in, jnp.sum(grad_out * standard, axis=(0, 1)), jnp.sum(grad_out, axis=(0, 1)))


def silu_slope(hidden_pre):
    gate_sig = jax.nn.sigmoid(hidden_pre)
    return gate_sig * (1.0 + hidden_pre * (1.0 - gate_sig))


def rows_in(left_reach, right_reach):
    return jnp.einsum("zub,bx->zux", left_reach, right_reach, preferred_element_type=jnp.float32)


def rows_out(left_reach, right_reach):
    return jnp.einsum("anp,op->ano", left_reach, right_reach, preferred_element_type=jnp.float32)


def weight_sum(left_reach, right_reach):
    return jnp.einsum("zbt,zbm->tm", left_reach, right_reach, preferred_element_type=jnp.float32)


def together(*values):
    return lax.optimization_barrier(values)


def widen(normed):
    return lax.all_gather(normed.astype(jnp.bfloat16), "tp", axis=1, tiled=True)


def narrow(partial_rows):
    return lax.psum_scatter(
        partial_rows.astype(jnp.bfloat16), "tp", scatter_dimension=1, tiled=True
    ).astype(jnp.float32)


def widen_grad(grad_branch):
    return lax.all_gather(grad_branch, "tp", axis=1, tiled=True)


def narrow_grad(partial_rows):
    return lax.psum_scatter(
        partial_rows.astype(jnp.bfloat16), "tp", scatter_dimension=1, tiled=True
    ).astype(jnp.float32)


def local_cut(full_array, tp_rank, size_local):
    return lax.dynamic_slice_in_dim(
        full_array, tp_rank * size_local, size_local, full_array.ndim - 1
    )


def local_put(local_array, tp_rank, full_size):
    shape_full = local_array.shape[:-1] + (full_size,)
    return lax.dynamic_update_slice_in_dim(
        jnp.zeros(shape_full, jnp.float32),
        local_array,
        tp_rank * local_array.shape[-1],
        local_array.ndim - 1,
    )


BAND = 384


def wide_table(rel_table):
    before = jnp.broadcast_to(rel_table[:1], (LEFT, HEAD))
    after = jnp.broadcast_to(rel_table[-1:], (BAND - LEFT - rel_table.shape[0], HEAD))
    return jnp.concatenate([before, rel_table, after], axis=0)


def dot_t(left, right):
    return lax.dot_general(left, right, (((1,), (1,)), ((), ())), preferred_element_type=jnp.float32)


def dot_n(left, right):
    return lax.dot_general(left, right, (((1,), (0,)), ((), ())), preferred_element_type=jnp.float32)


def scaled_scores(query_block, keys, table, place, rows_at, reach):
    rows = query_block.shape[0]
    key_count = keys.shape[0]
    near = dot_t(query_block, table)
    left, right = near[:, :1], near[:, BAND - 1 :]
    row = lax.broadcasted_iota(jnp.int32, (rows, key_count), 0)
    col = lax.broadcasted_iota(jnp.int32, (rows, key_count), 1)
    place[:, 128 : 128 + key_count] = dot_t(query_block, keys) + jnp.where(
        col < row + rows_at, left, right
    )
    rolled = pltpu.roll(near, 0, 1, stride=1, stride_axis=0)
    apart = band_distance(rows)
    band = jnp.where(apart <= -LEFT, left, jnp.where(apart >= reach, right, rolled))
    window = pl.ds(pl.multiple_of(rows_at, 128), BAND)
    place[:, window] += band - jnp.where(apart < 0, left, right)
    return place[:, 128 : 128 + key_count]


def band_distance(rows):
    row = lax.broadcasted_iota(jnp.int32, (rows, BAND), 0)
    col = lax.broadcasted_iota(jnp.int32, (rows, BAND), 1)
    return col - 128 - row


def attend_kernel(reach, start_ref, query_ref, key_ref, value_ref, table_ref, mixed_ref, probs_ref, place):
    rows = query_ref.shape[1]
    rows_at = start_ref[0] + pl.program_id(2) * rows
    table = table_ref[...]
    for half in range(query_ref.shape[2] // HEAD):
        lanes = slice(half * HEAD, (half + 1) * HEAD)
        query_block = query_ref[0, :, lanes] * jnp.bfloat16(1.0 / math.sqrt(HEAD))
        scores = scaled_scores(query_block, key_ref[0, :, lanes], table, place, rows_at, reach)
        top = jnp.max(scores, axis=-1, keepdims=True)
        powers = jnp.exp(scores - top)
        row_sum = jnp.sum(powers, axis=-1, keepdims=True)
        probs = (powers * (1.0 / row_sum)).astype(jnp.bfloat16)
        mixed_ref[0, :, lanes] = dot_n(probs, value_ref[0, :, lanes]).astype(jnp.bfloat16)
        probs_ref[0, half] = probs


def attend_back_kernel(
    reach, start_ref, query_ref, key_ref, value_ref, table_ref, probs_ref, grad_ref, groups_ref,
    query_grad_ref, pair_grad_ref, table_grad_ref, place, key_sum, value_sum,
):
    rows = query_ref.shape[1]
    key_count = key_ref.shape[1]
    block = pl.program_id(2)
    rows_at = start_ref[0] + block * rows
    table = table_ref[...]
    scale = jnp.bfloat16(1.0 / math.sqrt(HEAD))

    @pl.when(block == 0)
    def _():
        key_sum[...] = jnp.zeros_like(key_sum)
        value_sum[...] = jnp.zeros_like(value_sum)

    @pl.when((block == 0) & (pl.program_id(0) == 0) & (pl.program_id(1) == 0))
    def _():
        table_grad_ref[...] = jnp.zeros_like(table_grad_ref)

    for half in range(query_ref.shape[2] // HEAD):
        lanes = slice(half * HEAD, (half + 1) * HEAD)
        query_block = query_ref[0, :, lanes] * scale
        keys = key_ref[0, :, lanes]
        grad_block = grad_ref[0, :, lanes]
        probs_low = probs_ref[0, half]
        probs = probs_low.astype(jnp.float32)
        grad_probs = dot_t(grad_block, value_ref[0, :, lanes])
        row_dot = jnp.sum(probs * grad_probs, axis=-1, keepdims=True)
        grad_scores = (probs * (grad_probs - row_dot)).astype(jnp.bfloat16)
        value_sum[lanes, :] += dot_n(grad_block.T, probs_low)
        key_sum[lanes, :] += dot_n(query_block.T, grad_scores)
        wide = grad_scores.astype(jnp.float32)
        place[:, 128 : 128 + key_count] = wide
        window = place[:, pl.ds(pl.multiple_of(rows_at, 128), BAND)]
        window_col = lax.broadcasted_iota(jnp.int32, window.shape, 1) + rows_at - 128
        window = jnp.where((window_col >= 0) & (window_col < key_count), window, 0.0)
        apart = band_distance(rows)
        by_group = dot_n(grad_scores, groups_ref[...])
        past = lax.broadcasted_iota(jnp.int32, by_group.shape, 1) * 128 - rows_at
        far_left = jnp.sum(jnp.where(past < -128, by_group, 0.0), axis=-1, keepdims=True)
        far_left += jnp.sum(jnp.where(apart <= -LEFT, window, 0.0), axis=-1, keepdims=True)
        far_right = jnp.sum(jnp.where(past >= BAND - 128, by_group, 0.0), axis=-1, keepdims=True)
        far_right += jnp.sum(jnp.where(apart >= reach, window, 0.0), axis=-1, keepdims=True)
        inside = (apart > -LEFT) & (apart < reach)
        turned = jnp.where(inside, window, 0.0)
        row = lax.broadcasted_iota(jnp.int32, turned.shape, 0)
        for bit in range((rows - 1).bit_length()):
            moved = pltpu.roll(turned, BAND - (1 << bit), 1)
            turned = jnp.where(((row >> bit) & 1) == 1, moved, turned)
        lane = lax.broadcasted_iota(jnp.int32, turned.shape, 1)
        by_row = jnp.where(lane == LEFT, far_left, jnp.where(lane == 2 * LEFT + reach, far_right, turned))
        coarse = by_row.astype(jnp.bfloat16)
        fine = (by_row - coarse.astype(jnp.float32)).astype(jnp.bfloat16)
        query_grad = dot_n(grad_scores, keys) + dot_n(coarse, table) + dot_n(fine, table)
        query_grad_ref[0, :, lanes] = (query_grad * (1.0 / math.sqrt(HEAD))).astype(jnp.bfloat16)
        query_turned = query_block.T
        table_grad_ref[...] += dot_n(query_turned, coarse) + dot_n(query_turned, fine)

    @pl.when(block == pl.num_programs(2) - 1)
    def _():
        pair_grad_ref[0, 0] = key_sum[...].T.astype(jnp.bfloat16)
        pair_grad_ref[1, 0] = value_sum[...].T.astype(jnp.bfloat16)


def attend_specs(queries, keys):
    slots, rows, width = queries.shape
    lanes = 2 * HEAD
    block = 128
    grid = (slots, width // lanes, rows // block)
    by_query = pl.BlockSpec((1, block, lanes), lambda s, p, b, *_: (s, b, p))
    by_key = pl.BlockSpec((1, keys.shape[1], lanes), lambda s, p, b, *_: (s, 0, p))
    by_value = pl.BlockSpec(
        (1, keys.shape[1], lanes), lambda s, p, b, *_: (s, 0, p + width // lanes)
    )
    table = pl.BlockSpec((BAND, HEAD), lambda s, p, b, *_: (0, 0))
    place = pltpu.VMEM((block, keys.shape[1] + 256), jnp.float32)
    flops = slots * rows * keys.shape[1] * width * 4
    by_prob = pl.BlockSpec((1, 2, block, keys.shape[1]), lambda s, p, b, *_: (s, p, b, 0))
    return grid, by_query, by_key, by_value, by_prob, table, place, flops


def attend(queries, pairs, table, reach, query_start):
    grid, by_query, by_key, by_value, by_prob, by_table, place, flops = attend_specs(queries, pairs)
    return pl.pallas_call(
        functools.partial(attend_kernel, reach),
        out_shape=(
            jax.ShapeDtypeStruct(queries.shape, jnp.bfloat16),
            jax.ShapeDtypeStruct(
                queries.shape[:1] + (queries.shape[2] // HEAD, queries.shape[1], pairs.shape[1]),
                jnp.bfloat16,
            ),
        ),
        grid_spec=pltpu.PrefetchScalarGridSpec(
            num_scalar_prefetch=1,
            grid=grid,
            in_specs=[by_query, by_key, by_value, by_table],
            out_specs=(by_query, by_prob),
            scratch_shapes=[place],
        ),
        cost_estimate=pl.CostEstimate(flops=2 * flops, bytes_accessed=8 << 20, transcendentals=flops >> 8),
        name="attend",
    )(query_start.reshape(1), queries, pairs, pairs, table)


def attend_back(queries, pairs, table, totals, grad_mixed, reach, query_start):
    grid, by_query, by_key, by_value, by_prob, by_table, place, flops = attend_specs(queries, pairs)
    slots, key_count = pairs.shape[:2]
    turned = pltpu.VMEM((2 * HEAD, key_count), jnp.float32)
    group = jnp.arange(key_count, dtype=jnp.int32)[:, None] // 128
    groups = (group == jnp.arange(128, dtype=jnp.int32)[None, :]).astype(jnp.bfloat16)
    return pl.pallas_call(
        functools.partial(attend_back_kernel, reach),
        out_shape=(
            jax.ShapeDtypeStruct(queries.shape, jnp.bfloat16),
            jax.ShapeDtypeStruct((2, slots, key_count, queries.shape[2]), jnp.bfloat16),
            jax.ShapeDtypeStruct((HEAD, BAND), jnp.float32),
        ),
        grid_spec=pltpu.PrefetchScalarGridSpec(
            num_scalar_prefetch=1,
            grid=grid,
            in_specs=[
                by_query,
                by_key,
                by_value,
                by_table,
                by_prob,
                by_query,
                pl.BlockSpec((key_count, 128), lambda s, p, b, *_: (0, 0)),
            ],
            out_specs=(
                by_query,
                pl.BlockSpec((2, 1, key_count, 2 * HEAD), lambda s, p, b, *_: (0, s, 0, p)),
                pl.BlockSpec((HEAD, BAND), lambda s, p, b, *_: (0, 0)),
            ),
            scratch_shapes=[place, turned, turned],
        ),
        cost_estimate=pl.CostEstimate(flops=5 * flops, bytes_accessed=16 << 20, transcendentals=flops >> 8),
        name="attend_back",
    )(query_start.reshape(1), queries, pairs, pairs, table, totals, grad_mixed, groups)


def ffn_forward(stream, norm_gain, norm_shift, weight_in, bias_in, weight_out, bias_out):
    normed, standard, inverse = norm_forward(stream, norm_gain, norm_shift)
    wide_rows = widen(normed)
    hidden_pre = rows_in(wide_rows, weight_in) + bias_in
    active = jax.nn.silu(hidden_pre).astype(jnp.bfloat16)
    branch = narrow(rows_out(active, weight_out)) + bias_out
    return (stream + 0.5 * branch, (standard, inverse, wide_rows, hidden_pre))


def ffn_forward_first(
    stream, norm_gain, norm_shift, shard_in, bias_in, shard_out, bias_out, later_shards
):
    normed, standard, inverse = norm_forward(stream, norm_gain, norm_shift)
    normed, shard_in = together(normed.astype(jnp.bfloat16), shard_in)
    wide_rows = widen(normed)
    pieces = [
        gather_rows(shard_in[:, start : start + 256]) for start in range(0, shard_in.shape[1], 256)
    ]
    wide_rows, shard_out, *pieces = together(wide_rows, shard_out, *pieces)
    weight_out = gather_rows(shard_out)
    weight_in = jnp.concatenate(pieces, axis=1)
    hidden_pre = rows_in(wide_rows, weight_in) + bias_in
    active = jax.nn.silu(hidden_pre).astype(jnp.bfloat16)
    partial_rows = rows_out(active, weight_out).astype(jnp.bfloat16)
    partial_rows, *later_shards = together(partial_rows, *later_shards)
    later = [gather_rows(shard) for shard in later_shards]
    summed = lax.psum_scatter(partial_rows, "tp", scatter_dimension=1, tiled=True)
    summed, *later = together(summed, *later)
    branch = summed.astype(jnp.float32) + bias_out
    saved = (standard, inverse, wide_rows, hidden_pre)
    return (stream + 0.5 * branch, saved, weight_in, weight_out, later)


def ffn_backward(grad_stream, saved, norm_gain, weight_in, weight_out, beside=None):
    standard, inverse, wide_rows, hidden_pre = saved
    grad_branch = (0.5 * grad_stream).astype(jnp.bfloat16)
    out_bias_grad = jnp.sum(grad_branch.astype(jnp.float32), axis=(0, 1))
    wide_grad = widen_grad(grad_branch)
    if beside is not None:
        wide_grad, beside = together(wide_grad, exchange(beside, ("fsdp", "ctx")))
        beside = add_up(beside)
    active = jax.nn.silu(hidden_pre).astype(jnp.bfloat16)
    out_grad = weight_sum(wide_grad, active)
    grad_pre = (rows_in(wide_grad, weight_out) * silu_slope(hidden_pre)).astype(jnp.bfloat16)
    in_bias_grad = jnp.sum(grad_pre.astype(jnp.float32), axis=(0, 1))
    in_grad = weight_sum(wide_rows, grad_pre)
    partial_rows = rows_out(grad_pre, weight_in).astype(jnp.bfloat16)
    grad_normed = narrow_grad(partial_rows)
    if beside is not None:
        in_grad = exchange(in_grad.astype(jnp.bfloat16), ("fsdp", "ctx"))
        out_grad = exchange(out_grad.astype(jnp.bfloat16), ("fsdp", "ctx"))
    grad_normed, in_grad, out_grad = together(grad_normed, in_grad, out_grad)
    if beside is not None:
        in_grad, out_grad = add_up(in_grad), add_up(out_grad)
    grad_in, gain_grad, shift_grad = norm_backward(grad_normed, standard, inverse, norm_gain)
    return (
        grad_stream + grad_in,
        (gain_grad, shift_grad, in_grad, in_bias_grad, out_grad, out_bias_grad),
        beside,
    )


def attn_forward(stream, norm_gain, norm_shift, weights, biases, rel_table, ctx_rank, late_shard):
    query_w, key_w, value_w, out_w = weights
    query_b, value_b, out_b = biases
    normed, standard, inverse = norm_forward(stream, norm_gain, norm_shift)
    wide_rows = widen(normed)
    queries = (rows_in(wide_rows, query_w) + query_b).astype(jnp.bfloat16)
    pair_b = jnp.concatenate([jnp.zeros_like(value_b), value_b])
    pair_w = jnp.concatenate([key_w, value_w], axis=1)
    pairs = (rows_in(wide_rows, pair_w) + pair_b).astype(jnp.bfloat16)
    pairs_all = lax.all_gather(pairs, "ctx", axis=1, tiled=True)
    pairs_all, late_shard = together(pairs_all, late_shard)
    late = gather_rows(late_shard)
    reach = rel_table.shape[0] - 1 - LEFT
    mixed_token_rows, log_total = attend(
        queries, pairs_all, wide_table(rel_table), reach, ctx_rank * queries.shape[1]
    )
    mixed_token_rows, late = together(mixed_token_rows, late)
    branch = narrow(rows_out(mixed_token_rows, out_w)) + out_b
    return (
        stream + branch,
        (standard, inverse, wide_rows, queries, pairs_all, mixed_token_rows, log_total),
        late,
    )


def attn_backward(grad_stream, saved, norm_gain, weights, rel_table, ctx_rank, inner_grads):
    query_w, key_w, value_w, out_w = weights
    standard, inverse, wide_rows, queries, pairs_all, mixed_token_rows, log_total = saved
    grad_branch = grad_stream.astype(jnp.bfloat16)
    out_bias_grad = jnp.sum(grad_branch.astype(jnp.float32), axis=(0, 1))
    inner = jnp.concatenate([grad.astype(jnp.bfloat16) for grad in inner_grads], axis=1)
    wide_grad, inner = together(widen_grad(grad_branch), inner)
    inner = lax.psum_scatter(inner, ("fsdp", "ctx"), scatter_dimension=0, tiled=True)
    grad_mixed = rows_in(wide_grad, out_w).astype(jnp.bfloat16)
    reach = rel_table.shape[0] - 1 - LEFT
    query_low, pair_terms, table_turned = attend_back(
        queries,
        pairs_all,
        wide_table(rel_table),
        log_total,
        grad_mixed,
        reach,
        ctx_rank * queries.shape[1],
    )
    query_low, pair_terms, inner = together(query_low, pair_terms, inner)
    out_grad = weight_sum(wide_grad, mixed_token_rows)
    inner_parts = split_columns(inner, inner_grads)
    table_grad = table_turned[:, LEFT : LEFT + rel_table.shape[0]].T
    pair_low = add_up(exchange(pair_terms, "ctx", 2)).astype(jnp.bfloat16)
    key_low, value_low = pair_low[0], pair_low[1]
    query_bias_grad = jnp.sum(query_low.astype(jnp.float32), axis=(0, 1))
    value_bias_grad = jnp.sum(value_low.astype(jnp.float32), axis=(0, 1))
    query_w_grad = weight_sum(wide_rows, query_low)
    key_w_grad = weight_sum(wide_rows, key_low)
    value_w_grad = weight_sum(wide_rows, value_low)
    grad_normed = narrow_grad(
        rows_out(query_low, query_w) + rows_out(key_low, key_w) + rows_out(value_low, value_w)
    )
    grad_normed, out_grad, query_w_grad, key_w_grad, value_w_grad = together(
        grad_normed, out_grad, query_w_grad, key_w_grad, value_w_grad
    )
    grad_in, gain_grad, shift_grad = norm_backward(grad_normed, standard, inverse, norm_gain)
    return (
        grad_stream + grad_in,
        (
            gain_grad,
            shift_grad,
            query_w_grad,
            query_bias_grad,
            key_w_grad,
            value_w_grad,
            value_bias_grad,
            out_grad,
            out_bias_grad,
            table_grad,
        ),
        inner_parts,
    )


def sum_rows(first, second):
    every = lax.all_gather(jnp.stack([first, second]), "tp", axis=0, tiled=False)
    return jnp.sum(every, axis=0)


def conv_forward(stream, norm_gain, norm_shift, weights, depth_local, inner_gain, inner_offset):
    value_w, gate_w, out_w = weights
    normed, standard, inverse = norm_forward(stream, norm_gain, norm_shift)
    wide_rows = widen(normed)
    part_value = rows_in(wide_rows, value_w)
    part_gate = rows_in(wide_rows, gate_w)
    gated_rows = (part_value * jax.nn.sigmoid(part_gate)).astype(jnp.bfloat16)
    row_count = gated_rows.shape[1]
    reach_rows = depth_local.shape[0] - 1
    halo_rows = from_behind(gated_rows[:, row_count - reach_rows :, :], "ctx", 1)
    padded = jnp.concatenate([halo_rows, gated_rows], axis=1)
    padded_float = padded.astype(jnp.float32)
    convolved = depth_local[0] * padded_float[:, 0:row_count, :]
    for tap_index in range(1, depth_local.shape[0]):
        convolved = (
            convolved
            + depth_local[tap_index] * padded_float[:, tap_index : tap_index + row_count, :]
        )
    row_sums = sum_rows(jnp.sum(convolved, axis=-1), jnp.sum(convolved * convolved, axis=-1))
    row_mean = (row_sums[0] / D)[..., None]
    row_var = (row_sums[1] / D)[..., None] - row_mean * row_mean
    inner_inverse = lax.rsqrt(row_var + epsilon)
    inner_standard = (convolved - row_mean) * inner_inverse
    inner_pre = inner_standard * inner_gain + inner_offset
    active = jax.nn.silu(inner_pre).astype(jnp.bfloat16)
    branch = narrow(rows_out(active, out_w))
    return (
        stream + branch,
        (
            standard,
            inverse,
            wide_rows,
            part_value,
            part_gate,
            padded,
            inner_standard,
            inner_inverse,
            inner_pre,
        ),
    )


def taps_back_kernel(depth_ref, grad_ref, padded_ref, gated_ref, depth_grad_ref, wide):
    taps = depth_ref.shape[0]
    rows, width = gated_ref.shape[1:]
    step = 64

    @pl.when(pl.program_id(0) == 0)
    def _():
        depth_grad_ref[...] = jnp.zeros_like(depth_grad_ref)

    wide[: padded_ref.shape[1], :] = padded_ref[0].astype(jnp.float32)
    for lane in range(0, width, 128):
        lanes = slice(lane, lane + 128)
        for start in range(0, rows, step):
            own = grad_ref[0, start : start + step, lanes]
            total = jnp.zeros((step, 128), jnp.float32)
            for tap in range(taps):
                first = start + taps - 1 - tap
                total += depth_ref[tap : tap + 1, lanes] * grad_ref[0, first : first + step, lanes]
                product = own * wide[start + tap : start + tap + step, lanes]
                depth_grad_ref[8 * tap : 8 * tap + 8, lanes] += jnp.sum(
                    product.reshape(step // 8, 8, 128), axis=0
                )
            gated_ref[0, start : start + step, lanes] = total


def taps_back(grad_conv, ahead, padded, depth_local):
    slots, rows, width = grad_conv.shape
    taps = depth_local.shape[0]
    spare = -(rows + taps - 1) % 8
    reach = jnp.concatenate(
        [grad_conv, ahead, jnp.zeros((slots, spare, width), jnp.float32)], axis=1
    )
    held = jnp.pad(padded, ((0, 0), (0, spare), (0, 0)))
    by_slot = lambda count: pl.BlockSpec((1, count, width), lambda s: (s, 0, 0))
    gated, depth_sums = pl.pallas_call(
        taps_back_kernel,
        out_shape=(
            jax.ShapeDtypeStruct((slots, rows, width), jnp.float32),
            jax.ShapeDtypeStruct((8 * taps, width), jnp.float32),
        ),
        grid=(slots,),
        in_specs=[
            pl.BlockSpec((taps, width), lambda s: (0, 0)),
            by_slot(reach.shape[1]),
            by_slot(held.shape[1]),
        ],
        out_specs=(by_slot(rows), pl.BlockSpec((8 * taps, width), lambda s: (0, 0))),
        scratch_shapes=[pltpu.VMEM((held.shape[1], width), jnp.float32)],
        cost_estimate=pl.CostEstimate(
            flops=4 * taps * slots * rows * width, bytes_accessed=4 << 20, transcendentals=0
        ),
        name="taps_back",
    )(depth_local, reach, held)
    return gated, jnp.sum(depth_sums.reshape(taps, 8, width), axis=1)


def conv_backward(grad_stream, saved, norm_gain, weights, depth_local, inner_gain):
    value_w, gate_w, out_w = weights
    (
        standard,
        inverse,
        wide_rows,
        part_value,
        part_gate,
        padded,
        inner_standard,
        inner_inverse,
        inner_pre,
    ) = saved
    grad_branch = grad_stream.astype(jnp.bfloat16)
    wide_grad = widen_grad(grad_branch)
    active = jax.nn.silu(inner_pre).astype(jnp.bfloat16)
    out_grad = weight_sum(wide_grad, active)
    grad_inner = rows_in(wide_grad, out_w) * silu_slope(inner_pre)
    inner_gain_grad = jnp.sum(grad_inner * inner_standard, axis=(0, 1))
    inner_shift_grad = jnp.sum(grad_inner, axis=(0, 1))
    grad_standard = grad_inner * inner_gain
    row_sums = sum_rows(
        jnp.sum(grad_standard, axis=-1), jnp.sum(grad_standard * inner_standard, axis=-1)
    )
    grad_conv = inner_inverse * (
        grad_standard - (row_sums[0] / D)[..., None] - inner_standard * (row_sums[1] / D)[..., None]
    )
    row_count = grad_conv.shape[1]
    tap_count = depth_local.shape[0]
    reach_rows = tap_count - 1
    ahead = from_behind(grad_conv[:, :reach_rows, :].astype(jnp.bfloat16), "ctx", -1)
    grad_gated, depth_grad = taps_back(grad_conv, ahead.astype(jnp.float32), padded, depth_local)
    gate_sig = jax.nn.sigmoid(part_gate)
    grad_value = (grad_gated * gate_sig).astype(jnp.bfloat16)
    grad_gate = (grad_gated * part_value * gate_sig * (1.0 - gate_sig)).astype(jnp.bfloat16)
    value_w_grad = weight_sum(wide_rows, grad_value)
    gate_w_grad = weight_sum(wide_rows, grad_gate)
    grad_normed = narrow_grad(rows_out(grad_value, value_w) + rows_out(grad_gate, gate_w))
    grad_normed, out_grad, value_w_grad, gate_w_grad = together(
        grad_normed, out_grad, value_w_grad, gate_w_grad
    )
    grad_in, gain_grad, shift_grad = norm_backward(grad_normed, standard, inverse, norm_gain)
    return (
        grad_stream + grad_in,
        (
            gain_grad,
            shift_grad,
            value_w_grad,
            gate_w_grad,
            depth_grad,
            inner_gain_grad,
            inner_shift_grad,
            out_grad,
        ),
    )


def gather_rows(shard):
    return lax.all_gather(shard, ("fsdp", "ctx"), axis=0, tiled=True)


def exchange(joined, axes, dim=0):
    count = lax.axis_size(axes)
    shape = joined.shape
    parts = joined.reshape(shape[:dim] + (count, shape[dim] // count) + shape[dim + 1 :])
    parts = jnp.moveaxis(parts, dim, 0)
    return lax.all_to_all(parts, axes, split_axis=0, concat_axis=0, tiled=True)


def add_up(received):
    return jnp.sum(received.astype(jnp.float32), axis=0)


def split_columns(part, grads):
    pieces = []
    start = 0
    for grad in grads:
        pieces.append(part[:, start : start + grad.shape[1]].astype(jnp.float32))
        start += grad.shape[1]
    return tuple(pieces)


def small_columns(whole_parts, split_parts, rows):
    flat = jnp.concatenate([part.reshape(-1) for part in whole_parts + split_parts])
    columns = -(-flat.shape[0] // rows)
    flat = jnp.pad(flat, (0, rows * columns - flat.shape[0])).reshape(rows, columns)
    return jnp.pad(flat, ((0, 0), (0, -columns % 128)))


def finish_small(small, whole_parts, split_parts, own_parts, hidden_part):
    rows = small.shape[0] * lax.axis_size(("fsdp", "ctx"))
    count = sum(part.size for part in whole_parts + split_parts)
    small = small[:, : -(-count // rows)].astype(jnp.float32).reshape(-1)
    held = small.shape[0]
    sent = jnp.concatenate(
        [small] + [part.reshape(-1) for part in own_parts] + [hidden_part.reshape(-1)]
    )
    sent = jnp.pad(sent, (0, -sent.shape[0] % 128)).reshape(1, -1, 128)
    tp_count = lax.axis_size("tp")
    every = lax.all_gather(sent, "tp", axis=0, tiled=True)
    every = lax.all_gather(every, ("fsdp", "ctx"), axis=0, tiled=True)
    every = every.reshape(-1, tp_count, sent.size)
    by_tp = every[:, :, :held].transpose(1, 0, 2).reshape(tp_count, -1)
    total = jnp.sum(by_tp, axis=0)
    spread = by_tp
    whole = []
    start = 0
    for part in whole_parts:
        whole.append(total[start : start + part.size].reshape(part.shape))
        start += part.size
    pieces = []
    for part in split_parts:
        piece = spread[:, start : start + part.size]
        if part.ndim == 1:
            pieces.append(piece.reshape(-1))
        else:
            piece = piece.reshape((tp_count,) + part.shape)
            pieces.append(piece.transpose(1, 0, 2).reshape(part.shape[0], -1))
        start += part.size
    own = jnp.sum(every[:, :, held:], axis=0)
    owned = []
    start = 0
    for part in own_parts:
        owned.append(jnp.sum(own[:, start : start + part.size], axis=0).reshape(part.shape))
        start += part.size
    hidden = own[:, start : start + hidden_part.size].reshape(-1)
    w, p = whole, pieces
    return (
        owned[0], owned[1], hidden, owned[2], w[0], w[1], p[0], p[1], w[2], w[3], w[4], w[5],
        p[2], p[3], p[4], w[6], w[7], p[5], w[8], w[9], w[10], owned[3],
    )


def body(
    inputs,
    teacher,
    clips_dev,
    ffn1_gain,
    ffn1_shift,
    ffn1_in,
    ffn1_in_bias,
    ffn1_out,
    ffn1_out_bias,
    attn_gain,
    attn_shift,
    query_weight,
    query_bias,
    key_weight,
    value_weight,
    value_bias,
    attn_out_weight,
    attn_out_bias,
    rel_table,
    conv_gain,
    conv_shift,
    conv_value_weight,
    conv_gate_weight,
    conv_depth,
    conv_inner_gain,
    conv_inner_shift,
    conv_out_weight,
    ffn2_gain,
    ffn2_shift,
    ffn2_in,
    ffn2_in_bias,
    ffn2_out,
    ffn2_out_bias,
    final_gain,
    final_shift,
):
    width = query_weight.shape[1]
    late_shard = jnp.concatenate(
        [ffn2_in, ffn2_out, conv_value_weight, conv_gate_weight, conv_out_weight], axis=1
    )
    tp_rank = lax.axis_index("tp")
    ctx_rank = lax.axis_index("ctx")
    hidden_local = ffn1_in.shape[1]
    width_local = width
    ffn1_bias_local = local_cut(ffn1_in_bias, tp_rank, hidden_local)
    ffn2_bias_local = local_cut(ffn2_in_bias, tp_rank, hidden_local)
    query_bias_local = local_cut(query_bias, tp_rank, width_local)
    value_bias_local = local_cut(value_bias, tp_rank, width_local)
    depth_local = local_cut(conv_depth, tp_rank, width_local)
    inner_gain_local = local_cut(conv_inner_gain, tp_rank, width_local)
    inner_shift_local = local_cut(conv_inner_shift, tp_rank, width_local)
    stream_zero = inputs.astype(jnp.float32)
    stream_one, saved_one, ffn1_in_all, ffn1_out_all, attn_weights = ffn_forward_first(
        stream_zero,
        ffn1_gain,
        ffn1_shift,
        ffn1_in,
        ffn1_bias_local,
        ffn1_out,
        ffn1_out_bias,
        (query_weight, key_weight, value_weight, attn_out_weight),
    )
    stream_two, saved_two, late = attn_forward(
        stream_one,
        attn_gain,
        attn_shift,
        attn_weights,
        (query_bias_local, value_bias_local, attn_out_bias),
        rel_table,
        ctx_rank,
        late_shard,
    )
    ffn2_in_all = late[:, :hidden_local]
    ffn2_out_all = late[:, hidden_local : 2 * hidden_local]
    conv_all = late[:, 2 * hidden_local :]
    conv_weights = (
        conv_all[:, :width],
        conv_all[:, width : 2 * width],
        conv_all[:, 2 * width :],
    )
    stream_three, saved_three = conv_forward(
        stream_two,
        conv_gain,
        conv_shift,
        conv_weights,
        depth_local,
        inner_gain_local,
        inner_shift_local,
    )
    stream_four, saved_four = ffn_forward(
        stream_three,
        ffn2_gain,
        ffn2_shift,
        ffn2_in_all,
        ffn2_bias_local,
        ffn2_out_all,
        ffn2_out_bias,
    )
    final_out, final_standard, final_inverse = norm_forward(stream_four, final_gain, final_shift)
    live_slots = (
        jnp.arange(final_out.shape[0], dtype=jnp.int32) < clips_dev[lax.axis_index("fsdp")]
    ).astype(jnp.float32)
    misfit = (final_out - teacher.astype(jnp.float32)) * live_slots[:, None, None]
    sse_local = jnp.sum(misfit * misfit)
    gradient_fourth, final_gain_grad, final_shift_grad = norm_backward(
        2.0 * misfit, final_standard, final_inverse, final_gain
    )
    grad_three, ffn2_grads, _ = ffn_backward(
        gradient_fourth, saved_four, ffn2_gain, ffn2_in_all, ffn2_out_all
    )
    grad_two, conv_grads = conv_backward(
        grad_three,
        saved_three,
        conv_gain,
        conv_weights,
        depth_local,
        inner_gain_local,
    )
    grad_one, attn_grads, inner_parts = attn_backward(
        grad_two,
        saved_two,
        attn_gain,
        attn_weights,
        rel_table,
        ctx_rank,
        (ffn2_grads[2], ffn2_grads[4], conv_grads[2], conv_grads[3], conv_grads[7]),
    )
    attn_mats = (attn_grads[2], attn_grads[4], attn_grads[5], attn_grads[7])
    whole_parts = (
        attn_grads[0],
        attn_grads[1],
        attn_grads[8],
        attn_grads[9],
        conv_grads[0],
        conv_grads[1],
        ffn2_grads[0],
        ffn2_grads[1],
        ffn2_grads[5],
        final_gain_grad,
        final_shift_grad,
    )
    split_parts = (
        attn_grads[3],
        attn_grads[6],
        conv_grads[4],
        conv_grads[5],
        conv_grads[6],
        ffn2_grads[3],
    )
    columns = small_columns(whole_parts, split_parts, attn_mats[0].shape[0])
    beside_mats = attn_mats + (columns,)
    beside = jnp.concatenate([part.astype(jnp.bfloat16) for part in beside_mats], axis=1)
    grad_zero, ffn1_grads, beside = ffn_backward(
        grad_one, saved_one, ffn1_gain, ffn1_in_all, ffn1_out_all, beside
    )
    attn_parts = split_columns(beside, beside_mats)
    ffn1_parts = (ffn1_grads[2], ffn1_grads[4])
    shared = finish_small(
        attn_parts[-1],
        whole_parts,
        split_parts,
        (ffn1_grads[0], ffn1_grads[1], ffn1_grads[5], sse_local),
        ffn1_grads[3],
    )
    attn_parts = attn_parts[:-1]
    weight_parts = ffn1_parts + attn_parts + inner_parts[2:] + inner_parts[:2]
    token_count = (jnp.sum(clips_dev) * SEQ).astype(jnp.float32)
    loss = shared[21] / token_count
    return (
        final_out.astype(jnp.bfloat16),
        loss,
        grad_zero,
        shared[0],
        shared[1],
        weight_parts[0],
        shared[2],
        weight_parts[1],
        shared[3],
        shared[4],
        shared[5],
        weight_parts[2],
        shared[6],
        weight_parts[3],
        weight_parts[4],
        shared[7],
        weight_parts[5],
        shared[8],
        shared[9],
        shared[10],
        shared[11],
        weight_parts[6],
        weight_parts[7],
        shared[12],
        shared[13],
        shared[14],
        weight_parts[8],
        shared[15],
        shared[16],
        weight_parts[9],
        shared[17],
        weight_parts[10],
        shared[18],
        shared[19],
        shared[20],
    )


def solution(mesh):
    in_specs = (
        P("fsdp", ("ctx", "tp"), None),
        P("fsdp", ("ctx", "tp"), None),
        P(),
        P(),
        P(),
        P(("fsdp", "ctx"), "tp"),
        P(),
        P(("fsdp", "ctx"), "tp"),
        P(),
        P(),
        P(),
        P(("fsdp", "ctx"), "tp"),
        P(),
        P(("fsdp", "ctx"), "tp"),
        P(("fsdp", "ctx"), "tp"),
        P(),
        P(("fsdp", "ctx"), "tp"),
        P(),
        P(),
        P(),
        P(),
        P(("fsdp", "ctx"), "tp"),
        P(("fsdp", "ctx"), "tp"),
        P(),
        P(),
        P(),
        P(("fsdp", "ctx"), "tp"),
        P(),
        P(),
        P(("fsdp", "ctx"), "tp"),
        P(),
        P(("fsdp", "ctx"), "tp"),
        P(),
        P(),
        P(),
    )
    out_specs = (
        P("fsdp", ("ctx", "tp"), None),
        P(),
        P("fsdp", ("ctx", "tp"), None),
        P(),
        P(),
        P(("fsdp", "ctx"), "tp"),
        P(),
        P(("fsdp", "ctx"), "tp"),
        P(),
        P(),
        P(),
        P(("fsdp", "ctx"), "tp"),
        P(),
        P(("fsdp", "ctx"), "tp"),
        P(("fsdp", "ctx"), "tp"),
        P(),
        P(("fsdp", "ctx"), "tp"),
        P(),
        P(),
        P(),
        P(),
        P(("fsdp", "ctx"), "tp"),
        P(("fsdp", "ctx"), "tp"),
        P(),
        P(),
        P(),
        P(("fsdp", "ctx"), "tp"),
        P(),
        P(),
        P(("fsdp", "ctx"), "tp"),
        P(),
        P(("fsdp", "ctx"), "tp"),
        P(),
        P(),
        P(),
    )
    return jax.shard_map(body, mesh=mesh, in_specs=in_specs, out_specs=out_specs, check_vma=False)
```
